32 devices in a mesh: gz: 8 (over z, y), ga: 4 (over x, core).
Axes of the slice: x: 2, y: 2, z: 4, core: 2. Of those that a mesh axis runs over, the one named last changes fastest.
Arguments:
- solution: float32 [64, 256, 256], P(('gz', 'ga')), may hold values from -6 to 6
- residual: float32 [64, 256, 256], P(('gz', 'ga')), may hold values from -40 to 40
- direction: float32 [64, 256, 256], P(('gz', 'ga')), may hold values from -40 to 40
Outputs:
- solution_out: float32 [64, 256, 256], P(('gz', 'ga'))
- residual_out: float32 [64, 256, 256], P(('gz', 'ga'))
- direction_out: float32 [64, 256, 256], P(('gz', 'ga'))
The draws below stay inside these ranges and needn't reach their ends.
All inputs are finite; a program needn't handle non-finite values.
Results may differ from the reference program's by a relative error of at most 0.0003.
Values sent between devices are 32-bit elements; how exact they have to be, the bound alone decides.
A program may use at most 128 MiB of HBM per device.

```python
import math
import jax
import jax.numpy as jnp
import numpy as np
from jax import lax

NX = 256
NY = 256
S = 8
NZ = 64


def base_noise(key):
    return jnp.clip(jax.random.normal(key, (NZ, NX, NY), jnp.float32), -3.0, 3.0)


def box_filter(field):
    padded = jnp.pad(field, ((0, 0), (1, 1), (1, 1)))
    total = jnp.zeros_like(field)
    for shift_x in range(3):
        for shift_y in range(3):
            total = total + padded[:, shift_x:shift_x + NX, shift_y:shift_y + NY]
    return total / 3.0


def checker_sign():
    plane_ids = jnp.arange(NZ, dtype=jnp.int32)[:, None, None]
    column_ids = jnp.arange(NX, dtype=jnp.int32)[None, :, None]
    row_ids = jnp.arange(NY, dtype=jnp.int32)[None, None, :]
    parity = (plane_ids + column_ids + row_ids) % 2
    return 1.0 - 2.0 * parity.astype(jnp.float32)


def block_table(key, low, high, width):
    count = (NZ + width - 1) // width
    plane_ids = jnp.arange(NZ, dtype=jnp.int32)
    values = jax.random.uniform(key, (count,), jnp.float32, low, high)
    return values[plane_ids // width]


def mixed_field(key, salt):
    white = base_noise(jax.random.fold_in(key, salt + 1))
    smooth = box_filter(base_noise(jax.random.fold_in(key, salt + 2)))
    rough = checker_sign() * box_filter(base_noise(jax.random.fold_in(key, salt + 3)))
    mixing = block_table(jax.random.fold_in(key, salt + 4), -1.2, 1.2, 8)
    mixing = mixing + block_table(jax.random.fold_in(key, salt + 5), -0.5, 0.5, 2)
    upward = jnp.maximum(mixing, 0.0)[:, None, None]
    downward = jnp.maximum(-mixing, 0.0)[:, None, None]
    field = white + upward * smooth + downward * rough
    amplitude = jnp.exp(block_table(jax.random.fold_in(key, salt + 6), 0.0, math.log(10.0), 8))
    return (field, amplitude)


def paired_fields(key):
    depth = jnp.arange(NZ, dtype=jnp.float32) / max(NZ - 1, 1)
    direction_base, direction_amp = mixed_field(key, 100)
    residual_base, residual_amp = mixed_field(key, 200)
    coupling = block_table(jax.random.fold_in(key, 301), -1.0, 1.0, 8)
    coupling = coupling + block_table(jax.random.fold_in(key, 302), -0.3, 0.3, 2)
    trend = 3.0 ** depth
    direction = (0.2 * trend * direction_amp)[:, None, None] * direction_base
    residual = (0.2 * trend * residual_amp)[:, None, None] * (residual_base + coupling[:, None, None] * direction_base)
    return (jnp.clip(residual, -39.0, 39.0), jnp.clip(direction, -39.0, 39.0))


def draw_residual(key, part):
    return paired_fields(key)[0]


def draw_direction(key, part):
    return paired_fields(key)[1]


def shard_levels(own_key, dims, pieces, least, largest):
    factor_of = 1.0
    for dim, parts in pieces:
        steps = jax.random.uniform(jax.random.fold_in(jax.random.fold_in(own_key, 6), dim), (parts,), jnp.float32, least / len(pieces), largest / len(pieces))
        factor_of = factor_of * jnp.repeat(jnp.exp(steps), dims[dim] // parts).reshape((-1,) + (1,) * (len(dims) - 1 - dim))
    return factor_of


def scatter_about(stream_key, extent, spread, reach, cuts=(), kind=jnp.bfloat16):
    drawn = spread * jax.random.normal(stream_key, extent, jnp.float32)
    if cuts:
        drawn = drawn * shard_levels(stream_key, extent, cuts, -0.22, 0.18)
    return jnp.clip(drawn, -reach, reach).astype(kind)


def setup_inputs(seed: int = 0) -> dict:
    arg_keys = jax.random.split(jax.random.key(seed), 4)
    solution = scatter_about(arg_keys[0], (NZ, NX, NY), 1.0, 6.0, ((0, 32),), jnp.float32)
    residual = draw_residual(jax.random.fold_in(arg_keys[3], 71), 0)
    direction = draw_direction(jax.random.fold_in(arg_keys[3], 71), 0)
    return dict(solution=solution, residual=residual, direction=direction)


precise = lax.Precision.HIGHEST
first_scale = -1.0 / 6.0
next_scale = -1.0 / 3.0


def neighbours_padded(extended):
    centre = extended[:, 1:-1]
    total = extended[:, 2:] + extended[:, :-2]
    padded = jnp.pad(centre, ((0, 0), (0, 0), (1, 1), (1, 1)))
    total = total + padded[:, :, 2:, 1:-1] + padded[:, :, :-2, 1:-1]
    total = total + padded[:, :, 1:-1, 2:] + padded[:, :, 1:-1, :-2]
    return total


def change_matrix(steps):
    count = 2 * steps + 1
    table = np.zeros((count, count), np.float32)
    for offset, length in ((0, steps + 1), (steps + 1, steps)):
        for power in range(length - 1):
            column = offset + power
            table[column, column] = 6.0
            if power == 0:
                table[column + 1, column] = 6.0
            else:
                table[column + 1, column] = 3.0
                table[column - 1, column] = 3.0
    return table


def quadratic(left, gram, right):
    return jnp.dot(left, jnp.dot(gram, right, precision=precise), precision=precise)


def inner_steps(gram, steps):
    table = jnp.asarray(change_matrix(steps), jnp.float32)
    count = 2 * steps + 1
    unit_rows = jnp.eye(count, dtype=jnp.float32)
    search = unit_rows[0]
    remain = unit_rows[steps + 1]
    iterate = jnp.zeros((count,), jnp.float32)
    current = quadratic(remain, gram, remain)
    for step in range(steps):
        moved = jnp.dot(table, search, precision=precise)
        alpha = current / quadratic(search, gram, moved)
        iterate = iterate + alpha * search
        remain = remain - alpha * moved
        updated = quadratic(remain, gram, remain)
        search = remain + (updated / current) * search
        current = updated
    return jnp.stack([iterate, remain, search])


def reference(solution, residual, direction):
    current = jnp.stack([direction, residual])
    earlier = current
    search_chain = [direction]
    residual_chain = [residual]
    for power in range(1, S + 1):
        active = current if power < S else current[0:1]
        beside = neighbours_padded(jnp.pad(active, ((0, 0), (1, 1), (0, 0), (0, 0))))
        if power == 1:
            following = beside * first_scale
        else:
            following = beside * next_scale - earlier[:active.shape[0]]
        earlier = active
        current = following
        search_chain.append(following[0])
        if power < S:
            residual_chain.append(following[1])
    basis = jnp.stack(search_chain + residual_chain)
    flat = basis.reshape(basis.shape[0], -1)
    gram = jnp.dot(flat, flat.T, precision=precise, preferred_element_type=jnp.float32)
    coefs = inner_steps(gram, S)
    combined = jnp.dot(coefs, flat, precision=precise, preferred_element_type=jnp.float32)
    shape = solution.shape
    return (solution + combined[0].reshape(shape), combined[1].reshape(shape), combined[2].reshape(shape))
```

```python
import functools

import jax
import jax.numpy as jnp
import numpy as np
from jax import lax
from jax.experimental import pallas as pl
from jax.experimental.pallas import tpu as pltpu
from jax.sharding import PartitionSpec as P

S = 8
MESH = pl.DeviceIdType.MESH
first_scale = -1.0 / 6.0
next_scale = -1.0 / 3.0
SIDE = 24
LANES = 128
HALVES = S // 2
UNROLL = 4
PIECES = 4
VMEM_LIMIT = 32 * 2 ** 20


def change_matrix(steps):
    count = 2 * steps + 1
    table = np.zeros((count, count), np.float64)
    for offset, length in ((0, steps + 1), (steps + 1, steps)):
        for power in range(length - 1):
            column = offset + power
            table[column, column] = 6.0
            if power == 0:
                table[column + 1, column] = 6.0
            else:
                table[column + 1, column] = 3.0
                table[column - 1, column] = 3.0
    return table


def dd(power, odd):
    return 2 * power + odd


def rr(power, odd):
    return 2 * S + 1 + 2 * power + odd


def dr(power, odd):
    return 4 * S + 2 * power + odd


COUNT = 6 * S


def gram_tables():
    def moment(kind, order):
        half, odd = order // 2, order % 2
        row = np.zeros(COUNT)
        row[kind(half, odd)] += 2.0
        row[kind(0, odd)] -= 1.0
        return row

    size = 2 * S + 1
    table = np.zeros((COUNT, size, size))
    for i in range(size):
        for j in range(size):
            a, b = (i if i <= S else i - S - 1), (j if j <= S else j - S - 1)
            kind = dd if (i <= S and j <= S) else rr if (i > S and j > S) else dr
            table[:, i, j] = 0.5 * (moment(kind, a + b) + moment(kind, abs(a - b)))
    moved = table @ change_matrix(S)

    def padded(t):
        out = np.zeros((t.shape[0], SIDE, LANES), np.float32)
        out[:, :size, :size] = t
        return out

    change = np.stack([change_matrix(S), change_matrix(S).T])
    return padded(table), padded(moved), padded(change)


def flipped(p, bits, group):
    if group & (group - 1):
        return (p + bits) % group
    out, step = p, 1
    while step < group:
        if bits & step:
            out = out + step * (1 - 2 * ((p // step) % 2))
        step *= 2
    return out


def send_order(group):
    if group & (group - 1):
        return list(range(1, group))
    first = [j for j in range(2, group) if (j // 2) & (j // 2 - 1) == 0]
    first = first[::2] + first[1::2]
    return first + [j for j in range(2, group) if j not in first] + [1]


def kernel(gz_count, ga, res_ref, dir_ref, gram_hbm, moved_hbm, change_hbm,
           dx, last, beta_ref,
           X, halo, stage, edge, edge_in, accs, red, coef, out_dx, out_q, held, gram_tab, moved_tab, change_tab,
           in_send, in_recv, own_sem, z_send, z_recv, r_send, r_recv, e_send, e_recv,
           a_send, a_recv, o_send, o_recv, q_send, q_recv, f_send, f_recv, load_sem):
    group = 2 * ga
    groups = gz_count // 2
    count = gz_count * ga
    planes, width, depth = res_ref.shape
    tall = planes * group
    rows = width // group
    iz, ia = lax.axis_index("gz"), lax.axis_index("ga")
    me = iz * ga + ia
    g = iz // 2
    p = (iz % 2) * ga + ia
    order = send_order(group)

    def place(position):
        upper = position // ga
        return upper * (3 * ga - 1 - position) + (1 - upper) * position

    b = place(p)

    def device(which, position):
        return (which * 2 + position // ga, position % ga)

    def block_rows(block):
        return pl.ds(pl.multiple_of(block * rows, rows), rows)

    loads = [pltpu.make_async_copy(source, target, load_sem.at[i]) for i, (source, target) in enumerate((
        (dir_ref, held.at[0]), (res_ref, held.at[1]), (gram_hbm, gram_tab), (moved_hbm, moved_tab),
        (change_hbm, change_tab)))]
    for load in loads:
        load.start()

    below, above = g > 0, g < groups - 1
    before, after = b > 0, b < group - 1
    z_there, r_there = (below, above), (before, after)

    barrier = pltpu.get_barrier_semaphore()

    def greet(target):
        pl.semaphore_signal(barrier, inc=1, device_id=target, device_id_type=MESH)

    if groups - 1 <= HALVES:
        for j in range(1, group):
            greet(device(g, flipped(p, j, group)))
        for up in range(2):
            @pl.when(z_there[up])
            def _():
                greet(device(g + 2 * up - 1, p))
            for side in range(2):
                @pl.when(z_there[up] & r_there[side])
                def _():
                    greet(device(g + 2 * up - 1, place(b + 2 * side - 1)))
        below_1, above_1 = jnp.minimum(g, 1), jnp.minimum(groups - 1 - g, 1)
        before_1, after_1 = jnp.minimum(b, 1), jnp.minimum(group - 1 - b, 1)
        pl.semaphore_wait(barrier, group - 1 + (below_1 + above_1) * (1 + before_1 + after_1))
    else:
        def greet_all(j, carry):
            t = (me + j) % count
            greet((t // ga, t % ga))
            return carry
        lax.fori_loop(1, count, greet_all, 0)
        pl.semaphore_wait(barrier, count - 1)

    def incoming(c, j):
        q = flipped(p, j, group)
        return pltpu.make_async_remote_copy(
            src_ref=held.at[c, :, block_rows(place(q)), :],
            dst_ref=X.at[c, 0, pl.ds(2 + planes * p, planes)],
            send_sem=in_send.at[c, j], recv_sem=in_recv.at[c, j],
            device_id=device(g, q), device_id_type=MESH)

    def incoming_from(c, j):
        return incoming(c, j if group & (group - 1) == 0 else group - j)

    def own_in(c):
        return pltpu.make_async_copy(
            held.at[c, :, block_rows(b), :],
            X.at[c, 0, pl.ds(2 + planes * p, planes)], own_sem.at[c])

    loads[0].wait()
    for j in order:
        incoming(0, j).start()
    own_in(0).start()
    loads[1].wait()
    early = len(order) // 2 + 1
    for j in order[:early]:
        incoming(1, j).start()
    own_in(1).start()

    for side, missing, at in ((0, g == 0, 0), (1, g == groups - 1, tall + 2)):
        @pl.when(missing)
        def _():
            for c in range(2):
                for k in range(0, S, 2):
                    X[c, k, at] = jnp.zeros((rows, depth), jnp.float32)
                    X[c, k, at + 1] = jnp.zeros((rows, depth), jnp.float32)
    for side, missing in ((0, b == 0), (1, b == group - 1)):
        @pl.when(missing)
        def _():
            for c in range(2):
                for k in range(0, S, 2):
                    for d in range(2):
                        halo[c, k, side, d] = jnp.zeros((tall, depth), jnp.float32)
    for up in range(2):
        for side in range(2):
            @pl.when(jnp.logical_not(z_there[up] & r_there[side]))
            def _():
                for c in range(2):
                    for h in range(HALVES):
                        edge_in[c, h, up, side] = jnp.zeros((1, depth), jnp.float32)

    def deep(c, k):
        return 1 if c == 1 and k == S - 2 else 2

    def z_copy(c, k, up):
        d = deep(c, k)
        source = 2 + tall - d if up else 2
        target = 2 - d if up else tall + 2
        return pltpu.make_async_remote_copy(
            src_ref=X.at[c, k, pl.ds(source, d)],
            dst_ref=X.at[c, k, pl.ds(target, d)],
            send_sem=z_send.at[c, k // 2, up], recv_sem=z_recv.at[c, k // 2, up],
            device_id=device(g + 2 * up - 1, p), device_id_type=MESH)

    def r_copy(c, k, up):
        d = deep(c, k)
        return pltpu.make_async_remote_copy(
            src_ref=stage.at[c, k // 2, up, pl.ds(0, d)],
            dst_ref=halo.at[c, k, 1 - up, pl.ds(0, d)],
            send_sem=r_send.at[c, k // 2, up], recv_sem=r_recv.at[c, k // 2, up],
            device_id=device(g, place(b + 2 * up - 1)), device_id_type=MESH)

    def e_copy(c, k, up, side):
        return pltpu.make_async_remote_copy(
            src_ref=edge.at[c, k // 2, up, side],
            dst_ref=edge_in.at[c, k // 2, 1 - up, 1 - side],
            send_sem=e_send.at[c, k // 2, up, side], recv_sem=e_recv.at[c, k // 2, 1 - up, 1 - side],
            device_id=device(g + 2 * up - 1, place(b + 2 * side - 1)), device_id_type=MESH)

    def e_arrival(c, k, up, side):
        return pltpu.make_async_remote_copy(
            src_ref=edge.at[c, k // 2, up, side],
            dst_ref=edge_in.at[c, k // 2, up, side],
            send_sem=e_send.at[c, k // 2, up, side], recv_sem=e_recv.at[c, k // 2, up, side],
            device_id=device(g + 2 * up - 1, place(b + 2 * side - 1)), device_id_type=MESH)

    def send_z(c, k):
        for up in range(2):
            @pl.when(z_there[up])
            def _():
                z_copy(c, k, up).start()

    def send_edges(c, k):
        for up in range(2):
            for side in range(2):
                edge[c, k // 2, up, side] = X[c, k, 2 + (tall - 1) * up, (rows - 1) * side:(rows - 1) * side + 1, :]
        for up in range(2):
            for side in range(2):
                @pl.when(z_there[up] & r_there[side])
                def _():
                    e_copy(c, k, up, side).start()

    def send_rows(c, k):
        for side in range(2):
            @pl.when(r_there[side])
            def _():
                r_copy(c, k, side).start()

    def receive(c, k):
        for side in range(2):
            @pl.when(r_there[side])
            def _():
                r_copy(c, k, 1 - side).wait_recv()
        for up in range(2):
            if deep(c, k) == 2:
                for side in range(2):
                    @pl.when(z_there[up] & r_there[side])
                    def _():
                        e_arrival(c, k, up, side).wait_recv()

            @pl.when(z_there[up])
            def _():
                z_copy(c, k, 1 - up).wait_recv()

    def iotas(height):
        row_ids = lax.broadcasted_iota(jnp.int32, (height, depth), 0)
        col_ids = lax.broadcasted_iota(jnp.int32, (height, depth), 1)
        return row_ids == 0, row_ids == height - 1, col_ids == 0, col_ids == depth - 1

    def folded(x):
        total = x[0:8]
        for i in range(8, rows, 8):
            total = total + x[i:i + 8]
        out = total[:, 0:LANES]
        for i in range(LANES, depth, LANES):
            out = out + total[:, i:i + LANES]
        return out

    def neighbours(cur, total, low, high, masks):
        height = cur.shape[0]
        first_row, last_row, first_col, last_col = masks
        total = total + jnp.where(first_row, low, pltpu.roll(cur, 1, 0))
        total = total + jnp.where(last_row, high, pltpu.roll(cur, height - 1, 0))
        total = total + jnp.where(first_col, 0.0, pltpu.roll(cur, 1, 1))
        return total + jnp.where(last_col, 0.0, pltpu.roll(cur, depth - 1, 1))

    plane_masks, row_masks = iotas(rows), iotas(tall)
    z_scale = [jnp.minimum(g, 1).astype(jnp.float32), jnp.minimum(groups - 1 - g, 1).astype(jnp.float32)]
    r_scale = [jnp.minimum(b, 1).astype(jnp.float32), jnp.minimum(group - 1 - b, 1).astype(jnp.float32)]

    def extend(c, k):
        scale = first_scale if k == 1 else next_scale
        h = (k - 1) // 2
        for side in range(2):
            cur = halo[c, k - 1, side, 0]
            total = halo[c, k - 1, side, 1] + stage[c, h, side, 0]
            total = neighbours(cur, total, edge_in[c, h, 0, side], edge_in[c, h, 1, side], row_masks)
            new = total * (r_scale[side] * scale)
            if k > 1:
                new = new - halo[c, k - 2, side, 0]
            halo[c, k, side, 0] = new
        for up in range(2):
            at, out, inside = (tall + 2, tall + 3, tall + 1) if up else (1, 0, 2)
            cur = X[c, k - 1, at]
            total = X[c, k - 1, out] + X[c, k - 1, inside]
            total = neighbours(cur, total, edge_in[c, h, up, 0], edge_in[c, h, up, 1], plane_masks)
            new = total * (z_scale[up] * scale)
            if k > 1:
                new = new - X[c, k - 2, at]
            X[c, k, at] = new

    def names_of(c, k):
        if c == 0:
            names = [(dd(k, 0), "new", "new"), (dd(k - 1, 1), "new", "cur")]
            if k == 1:
                names.append((dd(0, 0), "cur", "cur"))
        else:
            names = [(rr(k, 0), "new", "new"), (rr(k - 1, 1), "new", "cur"),
                     (dr(k, 0), "new", "other"), (dr(k - 1, 1), "cur", "other")]
            if k == S - 1:
                names.append((dr(k, 1), "new", "ahead"))
            if k == 1:
                names += [(rr(0, 0), "cur", "cur"), (dr(0, 0), "cur", "start")]
        return names

    def sent(c, k):
        return k % 2 == 0 and k < (S if c == 0 else S - 1)

    def plane(c, k, z, sums):
        names = names_of(c, k)
        cur = X[c, k - 1, z + 2]
        total = X[c, k - 1, z + 1] + X[c, k - 1, z + 3]
        low = halo[c, k - 1, 0, 0, pl.ds(z, 1), :]
        high = halo[c, k - 1, 1, 0, pl.ds(z, 1), :]
        total = neighbours(cur, total, low, high, plane_masks)
        if k == 1:
            new = total * first_scale
        else:
            new = total * next_scale - X[c, k - 2, z + 2]
        X[c, k, z + 2] = new
        if sent(c, k):
            put_rows(c, k, z, new)
        have = {"new": new, "cur": cur}
        if any("other" in n for n in names):
            have["other"] = X[0, k, z + 2]
        if any("ahead" in n for n in names):
            have["ahead"] = X[0, k + 1, z + 2]
        if any("start" in n for n in names):
            have["start"] = X[0, 0, z + 2]
        return tuple(s + folded(have[l] * have[r]) for s, (_, l, r) in zip(sums, names))

    def put_rows(c, k, z, new):
        at = pl.ds(z, 1)
        stage[c, k // 2, 0, 0, at, :] = new[0:1]
        stage[c, k // 2, 1, 0, at, :] = new[rows - 1:rows]
        if deep(c, k) == 2:
            stage[c, k // 2, 0, 1, at, :] = new[1:2]
            stage[c, k // 2, 1, 1, at, :] = new[rows - 2:rows - 1]

    def zero_sums(c, k):
        return tuple(jnp.zeros((8, LANES), jnp.float32) for _ in names_of(c, k))

    def keep(c, k, sums):
        for s, (slot, _, _) in zip(sums, names_of(c, k)):
            accs[slot] = s

    def ends(c, k, width_of, sums):
        def body(i, sums):
            return plane(c, k, i + (i // width_of) * (tall - 2 * width_of), sums)
        return lax.fori_loop(0, 2 * width_of, body, sums, unroll=True)

    def middle(c, k, width_of, sums):
        length = tall - 2 * width_of
        unroll = max(u for u in range(1, UNROLL + 1) if length % u == 0)
        return lax.fori_loop(width_of, tall - width_of, lambda z, s: plane(c, k, z, s), sums, unroll=unroll)

    def chain_round(c, k):
        a = k + 1
        top = S if c == 0 else S - 1
        if a == top:
            keep(c, a, middle(c, a, 0, zero_sums(c, a)))
            return
        n = k + 2
        extend(c, a)
        sums = ends(c, a, 3, zero_sums(c, a))
        later = ends(c, n, 2, zero_sums(c, n))
        if sent(c, n):
            send_z(c, n)
            if deep(c, n) == 2:
                send_edges(c, n)
        keep(c, a, middle(c, a, 3, sums))
        later = middle(c, n, 2, later)
        if sent(c, n):
            send_rows(c, n)
        keep(c, n, later)

    def arrive(c):
        own_in(c).wait()
        for j in order:
            incoming_from(c, j).wait_recv()
        send_z(c, 0)
        send_edges(c, 0)

        def copy_rows(z, carry):
            put_rows(c, 0, z, X[c, 0, z + 2])
            return carry
        lax.fori_loop(0, tall, copy_rows, 0, unroll=4)
        send_rows(c, 0)

    arrive(0)
    for j in order[early:]:
        incoming(1, j).start()
    receive(0, 0)
    chain_round(0, 0)
    arrive(1)
    for k in range(0, S, 2):
        if k:
            receive(0, k)
            chain_round(0, k)
        receive(1, k)
        chain_round(1, k)

    lanes = lax.broadcasted_iota(jnp.int32, (8, LANES), 1)
    packed = jnp.zeros((8, LANES), jnp.float32)
    for t in range(COUNT // 8):
        part = jnp.sum(jnp.sum(accs[8 * t:8 * t + 8], axis=1), axis=1, keepdims=True)
        packed = packed + jnp.where(lanes == t, part, 0.0)
    red[me] = jnp.sum(pltpu.roll(packed, 0, 1, stride=8, stride_axis=0), axis=0, keepdims=True)

    def moments_to(j):
        t = (me + j) % count
        return pltpu.make_async_remote_copy(
            src_ref=red.at[me], dst_ref=red.at[me], send_sem=a_send.at[0], recv_sem=a_recv.at[0],
            device_id=(t // ga, t % ga), device_id_type=MESH)

    def start_moments(j, carry):
        moments_to(j).start()
        return carry

    lax.fori_loop(1, count, start_moments, 0)
    others = red.at[pl.ds(0, count - 1)]
    pltpu.make_async_copy(others, others, a_recv.at[0]).wait()
    total = jnp.sum(red[...], axis=0)

    loads[2].wait()
    loads[3].wait()
    loads[4].wait()
    gram = jnp.zeros((SIDE, LANES), jnp.float32)
    moved = jnp.zeros((SIDE, LANES), jnp.float32)
    for e in range(COUNT):
        at = 8 * (e % 8) + e // 8
        value = total[0:1, at:at + 1]
        gram = gram + value * gram_tab[e]
        moved = moved + value * moved_tab[e]
    change, change_t = change_tab[0], change_tab[1]

    def full(x):
        return jnp.sum(jnp.sum(x, axis=0, keepdims=True), axis=1, keepdims=True)

    def unit(axis, at):
        ids = lax.broadcasted_iota(jnp.int32, (SIDE, LANES), axis)
        return jnp.where(ids == at, 1.0, 0.0).astype(jnp.float32)

    def advance(state):
        qc, qr, wc, wr, it, rho = state
        alpha = rho / full(qc * (moved * qr))
        mc = jnp.sum(change * qr, axis=1, keepdims=True)
        mr = jnp.sum(change_t * qc, axis=0, keepdims=True)
        it = it + alpha * qc
        wc = wc - alpha * mc
        wr = wr - alpha * mr
        rho_new = full(wc * (gram * wr))
        return wc, wr, it, rho_new, rho_new / rho

    def inner(_, state):
        wc, wr, it, rho, beta = advance(state)
        return wc + beta * state[0], wr + beta * state[1], wc, wr, it, rho

    wc, wr = unit(0, S + 1), unit(1, S + 1)
    state = (unit(0, 0), unit(1, 0), wc, wr, jnp.zeros((SIDE, LANES), jnp.float32),
             full(wc * (gram * wr)))
    state = lax.fori_loop(0, S - 1, inner, state)
    _, _, it, _, beta = advance(state)
    coef[0] = it
    coef[1] = state[0]
    beta_ref[...] = jnp.zeros((8, LANES), jnp.float32) + beta

    def combine(q):
        start = planes * q + 1 + q % 2

        def strip(s, carry):
            i, part = s // (rows // 8), s % (rows // 8)
            at = pl.ds(pl.multiple_of(part * 8, 8), 8)
            sums = [None, None]
            for v in range(2 * S - 1):
                c, k = (0, v) if v < S else (1, v - S)
                row = v if v < S else v + 1
                x = X[c, k, start + i, at, :]
                for o in range(2):
                    f = coef[o, row:row + 1, :]
                    f = jnp.concatenate([f] * (depth // LANES), axis=1)
                    term = f * x
                    sums[o] = term if sums[o] is None else sums[o] + term
            out_dx[q, i, at, :] = sums[0]
            out_q[q, i, at, :] = sums[1]
            return carry
        lax.fori_loop(0, (planes + 1) * (rows // 8), strip, 0, unroll=2)

    odd = p % 2

    def outgoing_dx(j):
        q = flipped(p, j, group)
        return pltpu.make_async_remote_copy(
            src_ref=out_dx.at[q], dst_ref=dx.at[pl.ds(q % 2, planes + 1), block_rows(b), :],
            send_sem=o_send.at[j], recv_sem=o_recv.at[j],
            device_id=device(g, q), device_id_type=MESH)

    def outgoing_q(j):
        q = flipped(p, j, group)
        return pltpu.make_async_remote_copy(
            src_ref=out_q.at[q, pl.ds(1 - q % 2, planes)], dst_ref=last.at[:, block_rows(b), :],
            send_sem=q_send.at[j], recv_sem=q_recv.at[j],
            device_id=device(g, q), device_id_type=MESH)

    def source_of(j):
        return flipped(p, j, group) if group & (group - 1) == 0 else (p + group - j) % group

    def dx_from(j):
        at = block_rows(place(source_of(j)))
        return pltpu.make_async_remote_copy(
            src_ref=out_dx.at[p], dst_ref=dx.at[pl.ds(odd, planes + 1), at, :],
            send_sem=o_send.at[j], recv_sem=o_recv.at[j],
            device_id=device(g, source_of(j)), device_id_type=MESH)

    def q_from(j):
        at = block_rows(place(source_of(j)))
        return pltpu.make_async_remote_copy(
            src_ref=out_q.at[p, pl.ds(1 - odd, planes)], dst_ref=last.at[:, at, :],
            send_sem=q_send.at[j], recv_sem=q_recv.at[j],
            device_id=device(g, source_of(j)), device_id_type=MESH)

    mate = p + 1 - 2 * odd

    def forwarded(block):
        at = block_rows(block)
        return pltpu.make_async_remote_copy(
            src_ref=dx.at[planes - odd * (planes - 1), at, :],
            dst_ref=dx.at[(1 - odd) * (planes + 1), at, :],
            send_sem=f_send.at[block], recv_sem=f_recv.at[block],
            device_id=device(g, mate), device_id_type=MESH)

    def forward_of(block):
        at = block_rows(block)
        return pltpu.make_async_remote_copy(
            src_ref=dx.at[planes - odd * (planes - 1), at, :],
            dst_ref=dx.at[odd * (planes + 1), at, :],
            send_sem=f_send.at[block], recv_sem=f_recv.at[block],
            device_id=device(g, mate), device_id_type=MESH)

    for j in order:
        combine(flipped(p, j, group))
        outgoing_dx(j).start()
    combine(p)
    for j in order:
        outgoing_q(j).start()
    own = pltpu.make_async_copy(out_dx.at[p], dx.at[pl.ds(odd, planes + 1), block_rows(b), :], own_sem.at[2])
    own.start()
    own_q = pltpu.make_async_copy(out_q.at[p, pl.ds(1 - odd, planes)], last.at[:, block_rows(b), :], own_sem.at[3])
    own_q.start()
    own.wait()
    forward_of(b).start()
    for j in [order[-1]] + order[:-1]:
        dx_from(j).wait_recv()
        forward_of(place(source_of(j))).start()
    own_q.wait()
    for block in range(group):
        forwarded(block).wait_recv()
    for j in order:
        q_from(j).wait_recv()

    for c in range(2):
        for j in order:
            incoming(c, j).wait_send()
        for k in range(0, S, 2):
            for up in range(2):
                @pl.when(z_there[up])
                def _():
                    z_copy(c, k, up).wait_send()

                @pl.when(r_there[up])
                def _():
                    r_copy(c, k, up).wait_send()

                if deep(c, k) == 2:
                    for side in range(2):
                        @pl.when(z_there[up] & r_there[side])
                        def _():
                            e_copy(c, k, up, side).wait_send()
    pltpu.make_async_copy(others, others, a_send.at[0]).wait()
    for j in order:
        outgoing_dx(j).wait_send()
        outgoing_q(j).wait_send()
    for block in range(group):
        forward_of(block).wait_send()


def finish(sol, res, dx, last, beta, sol_out, res_out, dir_out, buf, sem):
    planes, width, depth = sol.shape
    piece = width // PIECES
    row_ids = lax.broadcasted_iota(jnp.int32, (piece, depth), 0)
    col_ids = lax.broadcasted_iota(jnp.int32, (piece, depth), 1)
    factor = jnp.concatenate([beta[0:1, :]] * (depth // LANES), axis=1)
    copies = []
    for i in range(planes):
        for s in range(PIECES):
            at = pl.ds(s * piece, piece)
            cur = dx[i + 1, at, :]
            low = dx[i + 1, s * piece - 1:s * piece, :] if s else jnp.zeros((1, depth), jnp.float32)
            high = dx[i + 1, (s + 1) * piece:(s + 1) * piece + 1, :] if s < PIECES - 1 else jnp.zeros((1, depth), jnp.float32)
            total = dx[i, at, :] + dx[i + 2, at, :]
            total = total + jnp.where(row_ids == 0, low, pltpu.roll(cur, 1, 0))
            total = total + jnp.where(row_ids == piece - 1, high, pltpu.roll(cur, piece - 1, 0))
            total = total + jnp.where(col_ids == 0, 0.0, pltpu.roll(cur, 1, 1))
            total = total + jnp.where(col_ids == depth - 1, 0.0, pltpu.roll(cur, depth - 1, 1))
            buf[0, i, at, :] = sol[i, at, :] + cur
            remain = res[i, at, :] - (6.0 * cur - total)
            buf[1, i, at, :] = remain
            buf[2, i, at, :] = remain + factor * last[i, at, :]
            for o, target in enumerate((sol_out, res_out, dir_out)):
                copy = pltpu.make_async_copy(buf.at[o, i, at, :], target.at[i, at, :], sem.at[o, i, s])
                copy.start()
                copies.append(copy)
    for copy in copies:
        copy.wait()


def on_device(gz_count, ga, sol, res, direction):
    planes, width, depth = sol.shape
    group, groups = 2 * ga, gz_count // 2
    tall, rows = planes * group, width // group
    gram_tab, moved_tab, change_tab = (jnp.asarray(t) for t in gram_tables())
    vmem = pl.BlockSpec(memory_space=pltpu.VMEM)
    dma = pltpu.SemaphoreType.DMA
    anywhere = pl.BlockSpec(memory_space=pltpu.HBM)
    f32 = jnp.float32
    dx, last, beta = pl.pallas_call(
        functools.partial(kernel, gz_count, ga),
        out_shape=[pltpu.VMEM((planes + 2, width, depth), f32), pltpu.VMEM((planes, width, depth), f32),
                   pltpu.VMEM((8, LANES), f32)],
        in_specs=[anywhere] * 5,
        out_specs=[vmem] * 3,
        scratch_shapes=[
            pltpu.VMEM((2, S + 1, tall + 4, rows, depth), f32),
            pltpu.VMEM((2, S, 2, 2, tall, depth), f32),
            pltpu.VMEM((2, HALVES, 2, 2, tall, depth), f32),
            pltpu.VMEM((2, HALVES, 2, 2, 1, depth), f32),
            pltpu.VMEM((2, HALVES, 2, 2, 1, depth), f32),
            pltpu.VMEM((COUNT, 8, LANES), f32),
            pltpu.VMEM((gz_count * ga, 1, LANES), f32),
            pltpu.VMEM((2, SIDE, LANES), f32),
            pltpu.VMEM((group, planes + 1, rows, depth), f32),
            pltpu.VMEM((group, planes + 1, rows, depth), f32),
            pltpu.VMEM((2, planes, width, depth), f32),
            pltpu.VMEM((COUNT, SIDE, LANES), f32),
            pltpu.VMEM((COUNT, SIDE, LANES), f32),
            pltpu.VMEM((2, SIDE, LANES), f32),
            dma((2, group)), dma((2, group)), dma((4,)),
            dma((2, HALVES, 2)), dma((2, HALVES, 2)), dma((2, HALVES, 2)), dma((2, HALVES, 2)),
            dma((2, HALVES, 2, 2)), dma((2, HALVES, 2, 2)),
            dma((1,)), dma((1,)),
            dma((group,)), dma((group,)), dma((group,)), dma((group,)), dma((group,)), dma((group,)),
            dma((5,)),
        ],
        compiler_params=pltpu.CompilerParams(collective_id=0, has_side_effects=True, vmem_limit_bytes=VMEM_LIMIT),
    )(*(pltpu.with_memory_space_constraint(x, pltpu.HBM) for x in (res, direction, gram_tab, moved_tab, change_tab)))
    shape = jax.ShapeDtypeStruct(sol.shape, f32)
    return pl.pallas_call(
        finish,
        out_shape=[shape] * 3,
        in_specs=[vmem] * 5,
        out_specs=[anywhere] * 3,
        scratch_shapes=[pltpu.VMEM((3,) + sol.shape, f32), dma((3, planes, PIECES))],
        compiler_params=pltpu.CompilerParams(vmem_limit_bytes=8 * 2 ** 20),
    )(sol, res, dx, last, beta)


def solution(mesh):
    spec = P(("gz", "ga"), None, None)
    return jax.shard_map(
        functools.partial(on_device, mesh.shape["gz"], mesh.shape["ga"]),
        mesh=mesh, in_specs=(spec, spec, spec), out_specs=(spec, spec, spec), check_vma=False,
    )
```

```python
import functools

import jax
import jax.numpy as jnp
import numpy as np
from jax import lax
from jax.experimental import pallas as pl
from jax.experimental.pallas import tpu as pltpu
from jax.sharding import PartitionSpec as P

S = 8
MESH = pl.DeviceIdType.MESH
first_scale = -1.0 / 6.0
next_scale = -1.0 / 3.0
SIDE = 24
LANES = 128
HALVES = S // 2
UNROLL = 12
PIECES = 4
VMEM_LIMIT = 32 * 2 ** 20


def change_matrix(steps):
    count = 2 * steps + 1
    table = np.zeros((count, count), np.float64)
    for offset, length in ((0, steps + 1), (steps + 1, steps)):
        for power in range(length - 1):
            column = offset + power
            table[column, column] = 6.0
            if power == 0:
                table[column + 1, column] = 6.0
            else:
                table[column + 1, column] = 3.0
                table[column - 1, column] = 3.0
    return table


def dd(power, odd):
    return 2 * power + odd


def rr(power, odd):
    return 2 * S + 1 + 2 * power + odd


def dr(power, odd):
    return 4 * S + 2 * power + odd


COUNT = 6 * S


def gram_tables():
    def moment(kind, order):
        half, odd = order // 2, order % 2
        row = np.zeros(COUNT)
        row[kind(half, odd)] += 2.0
        row[kind(0, odd)] -= 1.0
        return row

    size = 2 * S + 1
    table = np.zeros((COUNT, size, size))
    for i in range(size):
        for j in range(size):
            a, b = (i if i <= S else i - S - 1), (j if j <= S else j - S - 1)
            kind = dd if (i <= S and j <= S) else rr if (i > S and j > S) else dr
            table[:, i, j] = 0.5 * (moment(kind, a + b) + moment(kind, abs(a - b)))
    moved = table @ change_matrix(S)

    def padded(t):
        out = np.zeros((t.shape[0], SIDE, LANES), np.float32)
        out[:, :size, :size] = t
        return out

    change = np.stack([change_matrix(S), change_matrix(S).T])
    return padded(table), padded(moved), padded(change)


def flipped(p, bits, group):
    if group & (group - 1):
        return (p + bits) % group
    out, step = p, 1
    while step < group:
        if bits & step:
            out = out + step * (1 - 2 * ((p // step) % 2))
        step *= 2
    return out


def send_order(group):
    if group & (group - 1):
        return list(range(1, group))
    first = [j for j in range(2, group) if (j // 2) & (j // 2 - 1) == 0]
    first = first[::2] + first[1::2]
    return first + [j for j in range(2, group) if j not in first] + [1]


def kernel(gz_count, ga, res_ref, dir_ref, table_hbm,
           dx, last, beta_ref,
           X, halo, stage, edge, edge_in, accs, red, coef, out_dx, out_q, held, table,
           in_send, in_recv, own_sem, z_send, z_recv, r_send, r_recv, e_send, e_recv,
           a_send, a_recv, o_send, o_recv, q_send, q_recv, f_send, f_recv, load_sem):
    group = 2 * ga
    groups = gz_count // 2
    count = gz_count * ga
    planes, width, depth = res_ref.shape
    tall = planes * group
    rows = width // group
    iz, ia = lax.axis_index("gz"), lax.axis_index("ga")
    me = iz * ga + ia
    g = iz // 2
    p = (iz % 2) * ga + ia
    order = send_order(group)

    def place(position):
        upper = position // ga
        return upper * (3 * ga - 1 - position) + (1 - upper) * position

    b = place(p)

    def device(which, position):
        return (which * 2 + position // ga, position % ga)

    def block_rows(block):
        return pl.ds(pl.multiple_of(block * rows, rows), rows)

    loads = [pltpu.make_async_copy(source, target, load_sem.at[i]) for i, (source, target) in enumerate((
        (dir_ref, held.at[0]), (res_ref, held.at[1]), (table_hbm, table)))]
    for load in loads:
        load.start()

    below, above = g > 0, g < groups - 1
    before, after = b > 0, b < group - 1
    z_there, r_there = (below, above), (before, after)

    barrier = pltpu.get_barrier_semaphore()

    def greet(target):
        pl.semaphore_signal(barrier, inc=1, device_id=target, device_id_type=MESH)

    if groups - 1 <= HALVES:
        for j in range(1, group):
            greet(device(g, flipped(p, j, group)))
        for up in range(2):
            @pl.when(z_there[up])
            def _():
                greet(device(g + 2 * up - 1, p))
            for side in range(2):
                @pl.when(z_there[up] & r_there[side])
                def _():
                    greet(device(g + 2 * up - 1, place(b + 2 * side - 1)))
        below_1, above_1 = jnp.minimum(g, 1), jnp.minimum(groups - 1 - g, 1)
        before_1, after_1 = jnp.minimum(b, 1), jnp.minimum(group - 1 - b, 1)
        pl.semaphore_wait(barrier, group - 1 + (below_1 + above_1) * (1 + before_1 + after_1))
    else:
        def greet_all(j, carry):
            t = (me + j) % count
            greet((t // ga, t % ga))
            return carry
        lax.fori_loop(1, count, greet_all, 0)
        pl.semaphore_wait(barrier, count - 1)

    def incoming(c, j):
        q = flipped(p, j, group)
        return pltpu.make_async_remote_copy(
            src_ref=held.at[c, :, block_rows(place(q)), :],
            dst_ref=X.at[c, 0, pl.ds(2 + planes * p, planes)],
            send_sem=in_send.at[0], recv_sem=in_recv.at[c],
            device_id=device(g, q), device_id_type=MESH)

    def own_in(c):
        return pltpu.make_async_copy(
            held.at[c, :, block_rows(b), :],
            X.at[c, 0, pl.ds(2 + planes * p, planes)], own_sem.at[c])

    loads[0].wait()
    for j in order:
        incoming(0, j).start()
    own_in(0).start()
    loads[1].wait()
    early = len(order) // 2 + 1
    for j in order[:early]:
        incoming(1, j).start()
    own_in(1).start()

    for side, missing, at in ((0, g == 0, 0), (1, g == groups - 1, tall + 2)):
        @pl.when(missing)
        def _():
            for c in range(2):
                for k in range(0, S, 2):
                    X[c, k, at] = jnp.zeros((rows, depth), jnp.float32)
                    X[c, k, at + 1] = jnp.zeros((rows, depth), jnp.float32)
    for side, missing in ((0, b == 0), (1, b == group - 1)):
        @pl.when(missing)
        def _():
            for c in range(2):
                for k in range(0, S, 2):
                    for d in range(2):
                        halo[c, k, side, d] = jnp.zeros((tall, depth), jnp.float32)
    for up in range(2):
        for side in range(2):
            @pl.when(jnp.logical_not(z_there[up] & r_there[side]))
            def _():
                for c in range(2):
                    for h in range(HALVES):
                        edge_in[c, h, up, side] = jnp.zeros((1, depth), jnp.float32)

    def deep(c, k):
        return 1 if c == 1 and k == S - 2 else 2

    def z_copy(c, k, up):
        d = deep(c, k)
        source = 2 + tall - d if up else 2
        target = 2 - d if up else tall + 2
        return pltpu.make_async_remote_copy(
            src_ref=X.at[c, k, pl.ds(source, d)],
            dst_ref=X.at[c, k, pl.ds(target, d)],
            send_sem=z_send.at[up], recv_sem=z_recv.at[c, k // 2 % 2, up],
            device_id=device(g + 2 * up - 1, p), device_id_type=MESH)

    def r_copy(c, k, up):
        return pltpu.make_async_remote_copy(
            src_ref=stage.at[c, k // 2, up],
            dst_ref=halo.at[c, k, 1 - up],
            send_sem=r_send.at[up], recv_sem=r_recv.at[c, k // 2 % 2, up],
            device_id=device(g, place(b + 2 * up - 1)), device_id_type=MESH)

    def e_copy(c, k, up, side):
        return pltpu.make_async_remote_copy(
            src_ref=edge.at[c, k // 2, up, side],
            dst_ref=edge_in.at[c, k // 2, 1 - up, 1 - side],
            send_sem=e_send.at[up, side], recv_sem=e_recv.at[c, k // 2 % 2, 1 - up, 1 - side],
            device_id=device(g + 2 * up - 1, place(b + 2 * side - 1)), device_id_type=MESH)

    def e_arrival(c, k, up, side):
        return pltpu.make_async_remote_copy(
            src_ref=edge.at[c, k // 2, up, side],
            dst_ref=edge_in.at[c, k // 2, up, side],
            send_sem=e_send.at[up, side], recv_sem=e_recv.at[c, k // 2 % 2, up, side],
            device_id=device(g + 2 * up - 1, place(b + 2 * side - 1)), device_id_type=MESH)

    def send_z(c, k):
        for up in range(2):
            @pl.when(z_there[up])
            def _():
                z_copy(c, k, up).start()

    def send_edges(c, k):
        for up in range(2):
            for side in range(2):
                edge[c, k // 2, up, side] = X[c, k, 2 + (tall - 1) * up, (rows - 1) * side:(rows - 1) * side + 1, :]
        for up in range(2):
            for side in range(2):
                @pl.when(z_there[up] & r_there[side])
                def _():
                    e_copy(c, k, up, side).start()

    def send_rows(c, k):
        for side in range(2):
            @pl.when(r_there[side])
            def _():
                r_copy(c, k, side).start()

    def receive(c, k):
        for side in range(2):
            @pl.when(r_there[side])
            def _():
                r_copy(c, k, 1 - side).wait_recv()
        for up in range(2):
            for side in range(2):
                @pl.when(z_there[up] & r_there[side])
                def _():
                    e_arrival(c, k, up, side).wait_recv()

            @pl.when(z_there[up])
            def _():
                z_copy(c, k, 1 - up).wait_recv()

    def iotas(height):
        row_ids = lax.broadcasted_iota(jnp.int32, (height, depth), 0)
        col_ids = lax.broadcasted_iota(jnp.int32, (height, depth), 1)
        return row_ids == 0, row_ids == height - 1, col_ids == 0, col_ids == depth - 1

    def folded(x):
        total = x[0:8]
        for i in range(8, rows, 8):
            total = total + x[i:i + 8]
        out = total[:, 0:LANES]
        for i in range(LANES, depth, LANES):
            out = out + total[:, i:i + LANES]
        return out

    def neighbours(cur, total, low, high, masks):
        height = cur.shape[0]
        first_row, last_row, first_col, last_col = masks
        total = total + jnp.where(first_row, low, pltpu.roll(cur, 1, 0))
        total = total + jnp.where(last_row, high, pltpu.roll(cur, height - 1, 0))
        total = total + jnp.where(first_col, 0.0, pltpu.roll(cur, 1, 1))
        return total + jnp.where(last_col, 0.0, pltpu.roll(cur, depth - 1, 1))

    plane_masks, row_masks = iotas(rows), iotas(tall)
    z_scale = [jnp.minimum(g, 1).astype(jnp.float32), jnp.minimum(groups - 1 - g, 1).astype(jnp.float32)]
    r_scale = [jnp.minimum(b, 1).astype(jnp.float32), jnp.minimum(group - 1 - b, 1).astype(jnp.float32)]

    def extend(c, k):
        scale = first_scale if k == 1 else next_scale
        h = (k - 1) // 2
        for side in range(2):
            cur = halo[c, k - 1, side, 0]
            total = halo[c, k - 1, side, 1] + stage[c, h, side, 0]
            total = neighbours(cur, total, edge_in[c, h, 0, side], edge_in[c, h, 1, side], row_masks)
            new = total * (r_scale[side] * scale)
            if k > 1:
                new = new - halo[c, k - 2, side, 0]
            halo[c, k, side, 0] = new
        for up in range(2):
            at, out, inside = (tall + 2, tall + 3, tall + 1) if up else (1, 0, 2)
            cur = X[c, k - 1, at]
            total = X[c, k - 1, out] + X[c, k - 1, inside]
            total = neighbours(cur, total, edge_in[c, h, up, 0], edge_in[c, h, up, 1], plane_masks)
            new = total * (z_scale[up] * scale)
            if k > 1:
                new = new - X[c, k - 2, at]
            X[c, k, at] = new

    def names_of(c, k):
        if c == 0:
            names = [(dd(k, 0), "new", "new"), (dd(k - 1, 1), "new", "cur")]
            if k == 1:
                names.append((dd(0, 0), "cur", "cur"))
        else:
            names = [(rr(k, 0), "new", "new"), (rr(k - 1, 1), "new", "cur"),
                     (dr(k, 0), "new", "other"), (dr(k - 1, 1), "cur", "other")]
            if k == S - 1:
                names.append((dr(k, 1), "new", "ahead"))
            if k == 1:
                names += [(rr(0, 0), "cur", "cur"), (dr(0, 0), "cur", "start")]
        return names

    def sent(c, k):
        return k % 2 == 0 and k < (S if c == 0 else S - 1)

    def plane(c, k, z, sums):
        names = names_of(c, k)
        cur = X[c, k - 1, z + 2]
        total = X[c, k - 1, z + 1] + X[c, k - 1, z + 3]
        low = halo[c, k - 1, 0, 0, pl.ds(z, 1), :]
        high = halo[c, k - 1, 1, 0, pl.ds(z, 1), :]
        total = neighbours(cur, total, low, high, plane_masks)
        if k == 1:
            new = total * first_scale
        else:
            new = total * next_scale - X[c, k - 2, z + 2]
        X[c, k, z + 2] = new
        if sent(c, k):
            put_rows(c, k, z, new)
        have = {"new": new, "cur": cur}
        if any("other" in n for n in names):
            have["other"] = X[0, k, z + 2]
        if any("ahead" in n for n in names):
            have["ahead"] = X[0, k + 1, z + 2]
        if any("start" in n for n in names):
            have["start"] = X[0, 0, z + 2]
        return tuple(s + folded(have[l] * have[r]) for s, (_, l, r) in zip(sums, names))

    def put_rows(c, k, z, new):
        at = pl.ds(z, 1)
        stage[c, k // 2, 0, 0, at, :] = new[0:1]
        stage[c, k // 2, 1, 0, at, :] = new[rows - 1:rows]
        stage[c, k // 2, 0, 1, at, :] = new[1:2]
        stage[c, k // 2, 1, 1, at, :] = new[rows - 2:rows - 1]

    def zero_sums(c, k):
        return tuple(jnp.zeros((8, LANES), jnp.float32) for _ in names_of(c, k))

    def keep(c, k, sums):
        for s, (slot, _, _) in zip(sums, names_of(c, k)):
            accs[slot] = s

    def ends(c, k, width_of, sums):
        def body(i, sums):
            return plane(c, k, i + (i // width_of) * (tall - 2 * width_of), sums)
        return lax.fori_loop(0, 2 * width_of, body, sums, unroll=True)

    def middle(c, k, width_of, sums):
        length = tall - 2 * width_of
        unroll = max(u for u in range(1, UNROLL + 1) if length % u == 0)
        return lax.fori_loop(width_of, tall - width_of, lambda z, s: plane(c, k, z, s), sums, unroll=unroll)

    def chain_round(c, k):
        a = k + 1
        top = S if c == 0 else S - 1
        if a == top:
            keep(c, a, middle(c, a, 0, zero_sums(c, a)))
            return
        n = k + 2
        extend(c, a)
        sums = ends(c, a, 3, zero_sums(c, a))
        later = ends(c, n, 2, zero_sums(c, n))
        if sent(c, n):
            send_z(c, n)
            send_edges(c, n)
        keep(c, a, middle(c, a, 3, sums))
        later = middle(c, n, 2, later)
        if sent(c, n):
            send_rows(c, n)
        keep(c, n, later)

    def arrive(c):
        own_in(c).wait()
        others = held.at[c, :, pl.ds(0, width - rows), :]
        pltpu.make_async_copy(others, others, in_recv.at[c]).wait()
        send_z(c, 0)
        send_edges(c, 0)

        def copy_rows(z, carry):
            put_rows(c, 0, z, X[c, 0, z + 2])
            return carry
        lax.fori_loop(0, tall, copy_rows, 0, unroll=4)
        send_rows(c, 0)

    arrive(0)
    for j in order[early:]:
        incoming(1, j).start()
    receive(0, 0)
    chain_round(0, 0)
    arrive(1)
    for k in range(0, S, 2):
        if k:
            receive(0, k)
            chain_round(0, k)
        receive(1, k)
        chain_round(1, k)

    lanes = lax.broadcasted_iota(jnp.int32, (8, LANES), 1)
    packed = jnp.zeros((8, LANES), jnp.float32)
    for t in range(COUNT // 8):
        part = jnp.sum(jnp.sum(accs[8 * t:8 * t + 8], axis=1), axis=1, keepdims=True)
        packed = packed + jnp.where(lanes == t, part, 0.0)
    red[me] = jnp.sum(pltpu.roll(packed, 0, 1, stride=8, stride_axis=0), axis=0, keepdims=True)

    def moments_to(j):
        t = (me + j) % count
        return pltpu.make_async_remote_copy(
            src_ref=red.at[me], dst_ref=red.at[me], send_sem=a_send.at[0], recv_sem=a_recv.at[0],
            device_id=(t // ga, t % ga), device_id_type=MESH)

    def start_moments(j, carry):
        moments_to(j).start()
        return carry

    lax.fori_loop(1, count, start_moments, 0, unroll=count <= 64)
    def drained(ref, sem):
        pltpu.make_async_copy(ref, ref, sem).wait()

    drained(held.at[:, :, pl.ds(0, width - rows), :], in_send.at[0])
    for up in range(2):
        @pl.when(z_there[up])
        def _():
            drained(X.at[0, pl.ds(0, S // 2 + 1), pl.ds(0, 3)], z_send.at[up])

        @pl.when(r_there[up])
        def _():
            drained(stage.at[:, :, 0], r_send.at[up])

        for side in range(2):
            @pl.when(z_there[up] & r_there[side])
            def _():
                drained(edge.at[:, :, 0, 0], e_send.at[up, side])
    others = red.at[pl.ds(0, count - 1)]
    drained(others, a_recv.at[0])
    total = jnp.sum(red[...], axis=0)

    loads[2].wait()
    gram = jnp.zeros((SIDE, LANES), jnp.float32)
    moved = jnp.zeros((SIDE, LANES), jnp.float32)
    for e in range(COUNT):
        at = 8 * (e % 8) + e // 8
        value = total[0:1, at:at + 1]
        gram = gram + value * table[e]
        moved = moved + value * table[COUNT + e]
    change, change_t = table[2 * COUNT], table[2 * COUNT + 1]

    def unit(axis, at):
        ids = lax.broadcasted_iota(jnp.int32, (SIDE, LANES), axis)
        return jnp.where(ids == at, 1.0, 0.0).astype(jnp.float32)

    def down(x):
        return jnp.sum(x, axis=0, keepdims=True)

    def across(x):
        return jnp.sum(x, axis=1, keepdims=True)

    def advance(state):
        qc, qr, wc, wr, it, uc, rho = state
        mc = across(change * qr)
        gc = across(moved * qr)
        mr = down(change_t * qc)
        alpha = rho / down(qc * gc)
        it = it + alpha * qc
        wc = wc - alpha * mc
        wr = wr - alpha * mr
        uc = uc - alpha * gc
        rho_new = down(wc * uc)
        return wc, wr, it, uc, rho_new, rho_new / rho

    def inner(_, state):
        wc, wr, it, uc, rho, beta = advance(state)
        return wc + beta * state[0], wr + beta * state[1], wc, wr, it, uc, rho

    wc, wr = unit(0, S + 1), unit(1, S + 1)
    start = across(gram * wr) + jnp.zeros((SIDE, LANES), jnp.float32)
    state = (unit(0, 0), unit(1, 0), wc, wr, jnp.zeros((SIDE, LANES), jnp.float32), start, down(wc * start))
    state = lax.fori_loop(0, S - 1, inner, state)
    _, _, it, _, _, beta = advance(state)
    coef[0] = it
    coef[1] = state[0]
    beta_ref[...] = jnp.zeros((8, LANES), jnp.float32) + beta

    def combine(q):
        start = planes * q + 1 + q % 2

        def strip(s, carry):
            i, part = s // (rows // 8), s % (rows // 8)
            at = pl.ds(pl.multiple_of(part * 8, 8), 8)
            sums = [None, None]
            for v in range(2 * S - 1):
                c, k = (0, v) if v < S else (1, v - S)
                row = v if v < S else v + 1
                x = X[c, k, start + i, at, :]
                for o in range(2):
                    f = coef[o, row:row + 1, :]
                    f = jnp.concatenate([f] * (depth // LANES), axis=1)
                    term = f * x
                    sums[o] = term if sums[o] is None else sums[o] + term
            out_dx[q, i, at, :] = sums[0]
            out_q[q, i, at, :] = sums[1]
            return carry
        lax.fori_loop(0, (planes + 1) * (rows // 8), strip, 0, unroll=2)

    odd = p % 2

    def outgoing_dx(j):
        q = flipped(p, j, group)
        return pltpu.make_async_remote_copy(
            src_ref=out_dx.at[q], dst_ref=dx.at[pl.ds(q % 2, planes + 1), block_rows(b), :],
            send_sem=o_send.at[0], recv_sem=o_recv.at[j],
            device_id=device(g, q), device_id_type=MESH)

    def outgoing_q(j):
        q = flipped(p, j, group)
        return pltpu.make_async_remote_copy(
            src_ref=out_q.at[q, pl.ds(1 - q % 2, planes)], dst_ref=last.at[:, block_rows(b), :],
            send_sem=q_send.at[0], recv_sem=q_recv.at[0],
            device_id=device(g, q), device_id_type=MESH)

    def source_of(j):
        return flipped(p, j, group) if group & (group - 1) == 0 else (p + group - j) % group

    def dx_from(j):
        at = block_rows(place(source_of(j)))
        return pltpu.make_async_remote_copy(
            src_ref=out_dx.at[p], dst_ref=dx.at[pl.ds(odd, planes + 1), at, :],
            send_sem=o_send.at[0], recv_sem=o_recv.at[j],
            device_id=device(g, source_of(j)), device_id_type=MESH)

    mate = p + 1 - 2 * odd

    def forward_of(block):
        at = block_rows(block)
        return pltpu.make_async_remote_copy(
            src_ref=dx.at[planes - odd * (planes - 1), at, :],
            dst_ref=dx.at[odd * (planes + 1), at, :],
            send_sem=f_send.at[0], recv_sem=f_recv.at[0],
            device_id=device(g, mate), device_id_type=MESH)

    for j in order:
        combine(flipped(p, j, group))
        outgoing_dx(j).start()
    combine(p)
    for j in order:
        outgoing_q(j).start()
    own = pltpu.make_async_copy(out_dx.at[p], dx.at[pl.ds(odd, planes + 1), block_rows(b), :], own_sem.at[2])
    own.start()
    own_q = pltpu.make_async_copy(out_q.at[p, pl.ds(1 - odd, planes)], last.at[:, block_rows(b), :], own_sem.at[3])
    own_q.start()
    own.wait()
    forward_of(b).start()
    for j in [order[-1]] + order[:-1]:
        dx_from(j).wait_recv()
        forward_of(place(source_of(j))).start()
    own_q.wait()
    drained(dx.at[0], f_recv.at[0])
    drained(others, a_send.at[0])
    drained(out_dx.at[pl.ds(0, group - 1)], o_send.at[0])
    drained(dx.at[0], f_send.at[0])
    drained(last.at[:, pl.ds(0, width - rows), :], q_recv.at[0])
    drained(last.at[:, pl.ds(0, width - rows), :], q_send.at[0])


def finish(sol, res, dx, last, beta, sol_out, res_out, dir_out, buf, sem):
    planes, width, depth = sol.shape
    piece = width // PIECES
    row_ids = lax.broadcasted_iota(jnp.int32, (piece, depth), 0)
    col_ids = lax.broadcasted_iota(jnp.int32, (piece, depth), 1)
    factor = jnp.concatenate([beta[0:1, :]] * (depth // LANES), axis=1)
    copies = []
    for i in range(planes):
        for s in range(PIECES):
            at = pl.ds(s * piece, piece)
            cur = dx[i + 1, at, :]
            low = dx[i + 1, s * piece - 1:s * piece, :] if s else jnp.zeros((1, depth), jnp.float32)
            high = dx[i + 1, (s + 1) * piece:(s + 1) * piece + 1, :] if s < PIECES - 1 else jnp.zeros((1, depth), jnp.float32)
            total = dx[i, at, :] + dx[i + 2, at, :]
            total = total + jnp.where(row_ids == 0, low, pltpu.roll(cur, 1, 0))
            total = total + jnp.where(row_ids == piece - 1, high, pltpu.roll(cur, piece - 1, 0))
            total = total + jnp.where(col_ids == 0, 0.0, pltpu.roll(cur, 1, 1))
            total = total + jnp.where(col_ids == depth - 1, 0.0, pltpu.roll(cur, depth - 1, 1))
            buf[0, i, at, :] = sol[i, at, :] + cur
            remain = res[i, at, :] - (6.0 * cur - total)
            buf[1, i, at, :] = remain
            buf[2, i, at, :] = remain + factor * last[i, at, :]
            for o, target in enumerate((sol_out, res_out, dir_out)):
                copy = pltpu.make_async_copy(buf.at[o, i, at, :], target.at[i, at, :], sem.at[o, i, s])
                copy.start()
                copies.append(copy)
    for copy in copies:
        copy.wait()


def on_device(gz_count, ga, sol, res, direction):
    planes, width, depth = sol.shape
    group, groups = 2 * ga, gz_count // 2
    tall, rows = planes * group, width // group
    table = jnp.asarray(np.concatenate(gram_tables()))
    vmem = pl.BlockSpec(memory_space=pltpu.VMEM)
    dma = pltpu.SemaphoreType.DMA
    anywhere = pl.BlockSpec(memory_space=pltpu.HBM)
    f32 = jnp.float32
    dx, last, beta = pl.pallas_call(
        functools.partial(kernel, gz_count, ga),
        out_shape=[pltpu.VMEM((planes + 2, width, depth), f32), pltpu.VMEM((planes, width, depth), f32),
                   pltpu.VMEM((8, LANES), f32)],
        in_specs=[anywhere] * 3,
        out_specs=[vmem] * 3,
        scratch_shapes=[
            pltpu.VMEM((2, S + 1, tall + 4, rows, depth), f32),
            pltpu.VMEM((2, S, 2, 2, tall, depth), f32),
            pltpu.VMEM((2, HALVES, 2, 2, tall, depth), f32),
            pltpu.VMEM((2, HALVES, 2, 2, 1, depth), f32),
            pltpu.VMEM((2, HALVES, 2, 2, 1, depth), f32),
            pltpu.VMEM((COUNT, 8, LANES), f32),
            pltpu.VMEM((gz_count * ga, 1, LANES), f32),
            pltpu.VMEM((2, SIDE, LANES), f32),
            pltpu.VMEM((group, planes + 1, rows, depth), f32),
            pltpu.VMEM((group, planes + 1, rows, depth), f32),
            pltpu.VMEM((2, planes, width, depth), f32),
            pltpu.VMEM((2 * COUNT + 2, SIDE, LANES), f32),
            dma((1,)), dma((2,)), dma((4,)),
            dma((2,)), dma((2, 2, 2)), dma((2,)), dma((2, 2, 2)),
            dma((2, 2)), dma((2, 2, 2, 2)),
            dma((1,)), dma((1,)),
            dma((1,)), dma((group,)), dma((1,)), dma((1,)), dma((1,)), dma((1,)),
            dma((3,)),
        ],
        compiler_params=pltpu.CompilerParams(collective_id=0, has_side_effects=True, vmem_limit_bytes=VMEM_LIMIT),
    )(*(pltpu.with_memory_space_constraint(x, pltpu.HBM) for x in (res, direction, table)))
    shape = jax.ShapeDtypeStruct(sol.shape, f32)
    return pl.pallas_call(
        finish,
        out_shape=[shape] * 3,
        in_specs=[vmem] * 5,
        out_specs=[anywhere] * 3,
        scratch_shapes=[pltpu.VMEM((3,) + sol.shape, f32), dma((3, planes, PIECES))],
        compiler_params=pltpu.CompilerParams(vmem_limit_bytes=8 * 2 ** 20),
    )(sol, res, dx, last, beta)


def solution(mesh):
    spec = P(("gz", "ga"), None, None)
    return jax.shard_map(
        functools.partial(on_device, mesh.shape["gz"], mesh.shape["ga"]),
        mesh=mesh, in_specs=(spec, spec, spec), out_specs=(spec, spec, spec), check_vma=False,
    )
```

```python
import functools

import jax
import jax.numpy as jnp
import numpy as np
from jax import lax
from jax.experimental import pallas as pl
from jax.experimental.pallas import tpu as pltpu
from jax.sharding import PartitionSpec as P

S = 8
MESH = pl.DeviceIdType.MESH
first_scale = -1.0 / 6.0
next_scale = -1.0 / 3.0
SIDE = 24
LANES = 128
FIRST = (S - 2, S - 3)
DEEP = max(FIRST)
UNROLL = 16
PIECES = 4
VMEM_LIMIT = 44 * 2 ** 20


def change_matrix(steps):
    count = 2 * steps + 1
    table = np.zeros((count, count), np.float64)
    for offset, length in ((0, steps + 1), (steps + 1, steps)):
        for power in range(length - 1):
            column = offset + power
            table[column, column] = 6.0
            if power == 0:
                table[column + 1, column] = 6.0
            else:
                table[column + 1, column] = 3.0
                table[column - 1, column] = 3.0
    return table


def dd(power, odd):
    return 2 * power + odd


def rr(power, odd):
    return 2 * S + 1 + 2 * power + odd


def dr(power, odd):
    return 4 * S + 2 * power + odd


COUNT = 6 * S


def gram_tables():
    def moment(kind, order):
        half, odd = order // 2, order % 2
        row = np.zeros(COUNT)
        row[kind(half, odd)] += 2.0
        row[kind(0, odd)] -= 1.0
        return row

    size = 2 * S + 1
    table = np.zeros((COUNT, size, size))
    for i in range(size):
        for j in range(size):
            a, b = (i if i <= S else i - S - 1), (j if j <= S else j - S - 1)
            kind = dd if (i <= S and j <= S) else rr if (i > S and j > S) else dr
            table[:, i, j] = 0.5 * (moment(kind, a + b) + moment(kind, abs(a - b)))
    moved = table @ change_matrix(S)

    def padded(t):
        out = np.zeros((t.shape[0], SIDE, LANES), np.float32)
        out[:, :size, :size] = t
        return out

    change = np.stack([change_matrix(S), change_matrix(S).T])
    return padded(table), padded(moved), padded(change)


def flipped(p, bits, group):
    if group & (group - 1):
        return (p + bits) % group
    out, step = p, 1
    while step < group:
        if bits & step:
            out = out + step * (1 - 2 * ((p // step) % 2))
        step *= 2
    return out


def send_order(group):
    if group & (group - 1):
        return list(range(1, group))
    first = [j for j in range(2, group) if (j // 2) & (j // 2 - 1) == 0]
    first = first[::2] + first[1::2]
    return first + [j for j in range(2, group) if j not in first] + [1]


def kernel(gz_count, ga, res_ref, dir_ref, table_hbm,
           dx, last, beta_ref,
           X, halo, stage, edge, edge_in, edge_1, edge_1_in, accs, red, coef, out_dx, out_q, held, table,
           in_send, in_recv, own_sem, z_send, z_recv, r_send, r_recv, e_send, e_recv,
           a_send, a_recv, o_send, o_recv, q_send, q_recv, f_send, f_recv, load_sem):
    group = 2 * ga
    groups = gz_count // 2
    count = gz_count * ga
    planes, width, depth = res_ref.shape
    tall = planes * group
    rows = width // group
    iz, ia = lax.axis_index("gz"), lax.axis_index("ga")
    me = iz * ga + ia
    g = iz // 2
    p = (iz % 2) * ga + ia
    order = send_order(group)

    def place(position):
        upper = position // ga
        return upper * (3 * ga - 1 - position) + (1 - upper) * position

    b = place(p)

    def device(which, position):
        return (which * 2 + position // ga, position % ga)

    def block_rows(block):
        return pl.ds(pl.multiple_of(block * rows, rows), rows)

    loads = [pltpu.make_async_copy(source, target, load_sem.at[i]) for i, (source, target) in enumerate((
        (dir_ref, held.at[0]), (res_ref, held.at[1]), (table_hbm, table)))]
    for load in loads:
        load.start()

    below, above = g > 0, g < groups - 1
    before, after = b > 0, b < group - 1
    z_there, r_there = (below, above), (before, after)

    barrier = pltpu.get_barrier_semaphore()

    def greet(target):
        pl.semaphore_signal(barrier, inc=1, device_id=target, device_id_type=MESH)

    if groups - 1 <= 3:
        for j in range(1, group):
            greet(device(g, flipped(p, j, group)))
        for up in range(2):
            @pl.when(z_there[up])
            def _():
                greet(device(g + 2 * up - 1, p))
            for side in range(2):
                @pl.when(z_there[up] & r_there[side])
                def _():
                    greet(device(g + 2 * up - 1, place(b + 2 * side - 1)))
        below_1, above_1 = jnp.minimum(g, 1), jnp.minimum(groups - 1 - g, 1)
        before_1, after_1 = jnp.minimum(b, 1), jnp.minimum(group - 1 - b, 1)
        pl.semaphore_wait(barrier, group - 1 + (below_1 + above_1) * (1 + before_1 + after_1))
    else:
        def greet_all(j, carry):
            t = (me + j) % count
            greet((t // ga, t % ga))
            return carry
        lax.fori_loop(1, count, greet_all, 0)
        pl.semaphore_wait(barrier, count - 1)

    def incoming(c, j):
        q = flipped(p, j, group)
        return pltpu.make_async_remote_copy(
            src_ref=held.at[c, :, block_rows(place(q)), :],
            dst_ref=X.at[c, 0, pl.ds(DEEP + planes * p, planes)],
            send_sem=in_send.at[0], recv_sem=in_recv.at[c],
            device_id=device(g, q), device_id_type=MESH)

    def own_in(c):
        return pltpu.make_async_copy(
            held.at[c, :, block_rows(b), :],
            X.at[c, 0, pl.ds(DEEP + planes * p, planes)], own_sem.at[c])

    loads[0].wait()
    for j in order:
        incoming(0, j).start()
    own_in(0).start()
    loads[1].wait()
    for j in order:
        incoming(1, j).start()
    own_in(1).start()

    def deep(c, k):
        return 2 if k else FIRST[c]

    def spread(c, k):
        return 1 if k else 4 if deep(c, k) < 6 else 8

    exchanges = [(c, k) for c in range(2) for k in (0, FIRST[c])]

    def edges_of(c, k, incoming_side, up, side):
        if k:
            return (edge_1_in if incoming_side else edge_1).at[c, up, side]
        if spread(c, k) == 4:
            return (edge_in if incoming_side else edge).at[up, side, pl.ds(0, deep(c, k) - 1)]
        if incoming_side:
            return halo.at[c, k, side, pl.ds(1, deep(c, k) - 1), pl.ds(up * (tall + 8), 8)]
        return stage.at[c, 0, side, pl.ds(0, deep(c, k) - 1), pl.ds(up * (tall - 8), 8)]

    for c, k in exchanges:
        d = deep(c, k)
        for missing, at in ((g == 0, DEEP - d), (g == groups - 1, tall + DEEP)):
            @pl.when(missing)
            def _():
                X[c, k, at:at + d] = jnp.zeros((d, rows, depth), jnp.float32)
        for side, missing in ((0, b == 0), (1, b == group - 1)):
            @pl.when(missing)
            def _():
                halo[c, k, side, 1:d + 1] = jnp.zeros((d, tall + 16, depth), jnp.float32)
        for up in range(2):
            for side in range(2):
                @pl.when(jnp.logical_not(z_there[up] & r_there[side]))
                def _():
                    ref = edges_of(c, k, True, up, side)
                    ref[...] = jnp.zeros(ref.shape, jnp.float32)

    def z_copy(c, k, up):
        d = deep(c, k)
        source = DEEP + tall - d if up else DEEP
        target = DEEP - d if up else tall + DEEP
        return pltpu.make_async_remote_copy(
            src_ref=X.at[c, k, pl.ds(source, d)],
            dst_ref=X.at[c, k, pl.ds(target, d)],
            send_sem=z_send.at[up], recv_sem=z_recv.at[c, min(k, 1), up],
            device_id=device(g + 2 * up - 1, p), device_id_type=MESH)

    def r_copy(c, k, up):
        d = deep(c, k)
        return pltpu.make_async_remote_copy(
            src_ref=stage.at[c, min(k, 1), up, pl.ds(0, d)],
            dst_ref=halo.at[c, k, 1 - up, pl.ds(1, d), pl.ds(8, tall)],
            send_sem=r_send.at[up], recv_sem=r_recv.at[c, min(k, 1), up],
            device_id=device(g, place(b + 2 * up - 1)), device_id_type=MESH)

    def e_copy(c, k, up, side):
        h = min(k, 1)
        return pltpu.make_async_remote_copy(
            src_ref=edges_of(c, k, False, up, side),
            dst_ref=edges_of(c, k, True, 1 - up, 1 - side),
            send_sem=e_send.at[c, h, up, side], recv_sem=e_recv.at[c, h, 1 - up, 1 - side],
            device_id=device(g + 2 * up - 1, place(b + 2 * side - 1)), device_id_type=MESH)

    def e_arrival(c, k, up, side):
        h = min(k, 1)
        return pltpu.make_async_remote_copy(
            src_ref=edges_of(c, k, False, up, side),
            dst_ref=edges_of(c, k, True, up, side),
            send_sem=e_send.at[c, h, up, side], recv_sem=e_recv.at[c, h, up, side],
            device_id=device(g + 2 * up - 1, place(b + 2 * side - 1)), device_id_type=MESH)

    def send_z(c, k):
        for up in range(2):
            @pl.when(z_there[up])
            def _():
                z_copy(c, k, up).start()

    def send_edges(c, k):
        n = spread(c, k)
        if n < 8:
            for up in range(2):
                for side in range(2):
                    ref = edges_of(c, k, False, up, side)
                    for i in range(deep(c, k) - 1):
                        if n == 1:
                            row = (rows - 1) * side
                            ref[i] = X[c, k, DEEP + (tall - 1) * up, row:row + 1, :]
                        else:
                            ref[i] = stage[c, 0, side, i, up * (tall - n):up * (tall - n) + n, :]
        for up in range(2):
            for side in range(2):
                @pl.when(z_there[up] & r_there[side])
                def _():
                    e_copy(c, k, up, side).start()

    def send_rows(c, k):
        for side in range(2):
            @pl.when(r_there[side])
            def _():
                r_copy(c, k, side).start()

    def receive(c, k):
        for side in range(2):
            @pl.when(r_there[side])
            def _():
                r_copy(c, k, 1 - side).wait_recv()
        for up in range(2):
            for side in range(2):
                @pl.when(z_there[up] & r_there[side])
                def _():
                    e_arrival(c, k, up, side).wait_recv()

            @pl.when(z_there[up])
            def _():
                z_copy(c, k, 1 - up).wait_recv()

    def iotas(height):
        row_ids = lax.broadcasted_iota(jnp.int32, (height, depth), 0)
        col_ids = lax.broadcasted_iota(jnp.int32, (height, depth), 1)
        return row_ids == 0, row_ids == height - 1, col_ids == 0, col_ids == depth - 1

    def folded(x):
        total = x[0:8]
        for i in range(8, rows, 8):
            total = total + x[i:i + 8]
        out = total[:, 0:LANES]
        for i in range(LANES, depth, LANES):
            out = out + total[:, i:i + LANES]
        return out

    def neighbours(cur, total, low, high, masks):
        height = cur.shape[0]
        first_row, last_row, _, _ = masks
        total = total + jnp.where(first_row, low, pltpu.roll(cur, 1, 0))
        total = total + jnp.where(last_row, high, pltpu.roll(cur, height - 1, 0))
        return across_columns(cur, total, masks)

    def across_columns(cur, total, masks):
        _, _, first_col, last_col = masks
        total = total + jnp.where(first_col, 0.0, pltpu.roll(cur, 1, 1))
        return total + jnp.where(last_col, 0.0, pltpu.roll(cur, depth - 1, 1))

    plane_masks, row_masks = iotas(rows), iotas(tall + 16)
    z_scale = [jnp.minimum(g, 1).astype(jnp.float32), jnp.minimum(groups - 1 - g, 1).astype(jnp.float32)]
    r_scale = [jnp.minimum(b, 1).astype(jnp.float32), jnp.minimum(group - 1 - b, 1).astype(jnp.float32)]

    plane_ids = lax.broadcasted_iota(jnp.int32, (tall + 16, depth), 0)
    inside = (jnp.where(plane_ids < 8, z_scale[0], 1.0) * jnp.where(plane_ids >= tall + 8, z_scale[1], 1.0))

    def settle(c, k):
        n = spread(c, k)
        if n < 8:
            for up in range(2):
                at = tall + 8 if up else 8 - n
                for side in range(2):
                    ref = edges_of(c, k, True, up, side)
                    for i in range(deep(c, k) - 1):
                        halo[c, k, side, i + 1, at:at + n, :] = ref[i]
        for e in range(1, deep(c, k)):
            for up in range(2):
                at = tall - 1 + e if up else -e
                put_row(c, k, at, X[c, k, DEEP + at])

    def put_row(c, k, z, new):
        at = pl.ds(8 + z, 1)
        halo[c, k, 0, 0, at, :] = new[0:1]
        halo[c, k, 1, 0, at, :] = new[rows - 1:rows]

    def extend_rows(c, k, reach):
        scale = first_scale if k == 1 else next_scale

        def extend_row(i, carry):
            for side in range(2):
                cur = halo[c, k - 1, side, i]
                total = halo[c, k - 1, side, i - 1] + halo[c, k - 1, side, i + 1]
                total = total + pltpu.roll(cur, 1, 0) + pltpu.roll(cur, tall + 15, 0)
                total = across_columns(cur, total, row_masks)
                new = total * (inside * (r_scale[side] * scale))
                if k > 1:
                    new = new - halo[c, k - 2, side, i]
                halo[c, k, side, i] = new
            return carry

        lax.fori_loop(1, reach + 1, extend_row, 0, unroll=True)

    def extend_planes(c, k, reach):
        scale = first_scale if k == 1 else next_scale

        def extend_plane(e, carry):
            for up in range(2):
                z = tall - 1 + e if up else -e
                at = DEEP + z
                cur = X[c, k - 1, at]
                total = X[c, k - 1, at - 1] + X[c, k - 1, at + 1]
                low = halo[c, k - 1, 0, 1, pl.ds(8 + z, 1), :]
                high = halo[c, k - 1, 1, 1, pl.ds(8 + z, 1), :]
                total = neighbours(cur, total, low, high, plane_masks)
                new = total * (z_scale[up] * scale)
                if k > 1:
                    new = new - X[c, k - 2, at]
                X[c, k, at] = new
                if reach > 1:
                    put_row(c, k, z, new)
            return carry

        lax.fori_loop(1, reach + 1, extend_plane, 0, unroll=True)

    def names_of(c, k):
        if c == 0:
            names = [(dd(k, 0), "new", "new"), (dd(k - 1, 1), "new", "cur")]
            if k == 1:
                names.append((dd(0, 0), "cur", "cur"))
        else:
            names = [(rr(k, 0), "new", "new"), (rr(k - 1, 1), "new", "cur"),
                     (dr(k, 0), "new", "other"), (dr(k - 1, 1), "cur", "other")]
            if k == S - 1:
                names.append((dr(k, 1), "new", "ahead"))
            if k == 1:
                names += [(rr(0, 0), "cur", "cur"), (dr(0, 0), "cur", "start")]
        return names

    def sent(c, k):
        return k == FIRST[c]

    def plane(c, k, z, sums, reach):
        names = names_of(c, k)
        at = z + DEEP
        cur = X[c, k - 1, at]
        total = X[c, k - 1, at - 1] + X[c, k - 1, at + 1]
        low = halo[c, k - 1, 0, 1, pl.ds(8 + z, 1), :]
        high = halo[c, k - 1, 1, 1, pl.ds(8 + z, 1), :]
        total = neighbours(cur, total, low, high, plane_masks)
        if k == 1:
            new = total * first_scale
        else:
            new = total * next_scale - X[c, k - 2, at]
        X[c, k, at] = new
        if sent(c, k):
            put_rows(c, k, z, new)
        elif reach > 1:
            put_row(c, k, z, new)
        have = {"new": new, "cur": cur}
        if any("other" in n for n in names):
            have["other"] = X[0, k, at]
        if any("ahead" in n for n in names):
            have["ahead"] = X[0, k + 1, at]
        if any("start" in n for n in names):
            have["start"] = X[0, 0, at]
        return tuple(s + folded(have[l] * have[r]) for s, (_, l, r) in zip(sums, names))

    def put_rows(c, k, z, new):
        put_row(c, k, z, new)
        at = pl.ds(z, 1)
        for i in range(deep(c, k)):
            stage[c, min(k, 1), 0, i, at, :] = new[i:i + 1]
            stage[c, min(k, 1), 1, i, at, :] = new[rows - 1 - i:rows - i]

    def zero_sums(c, k):
        return tuple(jnp.zeros((8, LANES), jnp.float32) for _ in names_of(c, k))

    def keep(c, k, sums):
        for s, (slot, _, _) in zip(sums, names_of(c, k)):
            accs[slot] = s

    def ends(c, k, width_of, sums, reach):
        def body(i, sums):
            return plane(c, k, i + (i // width_of) * (tall - 2 * width_of), sums, reach)
        return lax.fori_loop(0, 2 * width_of, body, sums, unroll=True)

    def middle(c, k, width_of, sums, reach):
        length = tall - 2 * width_of
        unroll = max(u for u in range(1, UNROLL + 1) if length % u == 0)
        return lax.fori_loop(width_of, tall - width_of, lambda z, s: plane(c, k, z, s, reach), sums, unroll=unroll)

    def chain_round(c, k):
        d = deep(c, k)
        settle(c, k)
        outer = c == 1 and k == 0 and 2 * (d + 1) < tall
        sums = []
        for m in range(1, d + 1):
            n, reach = k + m, d - m
            if reach:
                extend_rows(c, n, reach)
                extend_planes(c, n, reach)
            sums.append((ends if outer else middle)(c, n, 2 + reach if outer else 0, zero_sums(c, n), reach))
        if sent(c, k + d):
            send_z(c, k + d)
            if outer:
                send_edges(c, k + d)
        for m in range(1, d + 1):
            n, reach = k + m, d - m
            if outer and m > 1 and reach:
                extend_rows(c, n, reach)
            keep(c, n, middle(c, n, 2 + reach, sums[m - 1], reach) if outer else sums[m - 1])
        if sent(c, k + d):
            send_rows(c, k + d)
            if not outer:
                send_edges(c, k + d)

    def arrive(c):
        own_in(c).wait()
        others = held.at[c, :, pl.ds(0, width - rows), :]
        pltpu.make_async_copy(others, others, in_recv.at[c]).wait()
        send_z(c, 0)

        def copy_rows(z, carry):
            put_rows(c, 0, z, X[c, 0, z + DEEP])
            return carry
        lax.fori_loop(0, tall, copy_rows, 0, unroll=4)
        send_edges(c, 0)
        send_rows(c, 0)

    arrive(0)
    arrive(1)
    for h in range(2):
        for c in range(2):
            receive(c, h * FIRST[c])
            chain_round(c, h * FIRST[c])

    lanes = lax.broadcasted_iota(jnp.int32, (8, LANES), 1)
    packed = jnp.zeros((8, LANES), jnp.float32)
    for t in range(COUNT // 8):
        part = jnp.sum(jnp.sum(accs[8 * t:8 * t + 8], axis=1), axis=1, keepdims=True)
        packed = packed + jnp.where(lanes == t, part, 0.0)
    red[me] = jnp.sum(pltpu.roll(packed, 0, 1, stride=8, stride_axis=0), axis=0, keepdims=True)

    def moments_to(j):
        t = (me + j) % count
        return pltpu.make_async_remote_copy(
            src_ref=red.at[me], dst_ref=red.at[me], send_sem=a_send.at[0], recv_sem=a_recv.at[0],
            device_id=(t // ga, t % ga), device_id_type=MESH)

    def start_moments(j, carry):
        moments_to(j).start()
        return carry

    lax.fori_loop(1, count, start_moments, 0, unroll=count <= 64)
    def drained(ref, sem):
        pltpu.make_async_copy(ref, ref, sem).wait()

    drained(held.at[:, :, pl.ds(0, width - rows), :], in_send.at[0])
    for up in range(2):
        @pl.when(z_there[up])
        def _():
            drained(X.at[0, pl.ds(0, 5), pl.ds(0, 3)], z_send.at[up])

        @pl.when(r_there[up])
        def _():
            drained(halo.at[0, pl.ds(0, 3), 0, pl.ds(0, 5), pl.ds(8, tall)], r_send.at[up])

        for side in range(2):
            @pl.when(z_there[up] & r_there[side])
            def _():
                for c, k in exchanges:
                    e_copy(c, k, up, side).wait_send()
    others = red.at[pl.ds(0, count - 1)]
    drained(others, a_recv.at[0])
    total = jnp.sum(red[...], axis=0)

    loads[2].wait()
    gram = jnp.zeros((SIDE, LANES), jnp.float32)
    moved = jnp.zeros((SIDE, LANES), jnp.float32)
    for e in range(COUNT):
        at = 8 * (e % 8) + e // 8
        value = total[0:1, at:at + 1]
        gram = gram + value * table[e]
        moved = moved + value * table[COUNT + e]
    change, change_t = table[2 * COUNT], table[2 * COUNT + 1]

    def unit(axis, at):
        ids = lax.broadcasted_iota(jnp.int32, (SIDE, LANES), axis)
        return jnp.where(ids == at, 1.0, 0.0).astype(jnp.float32)

    def down(x):
        return jnp.sum(x, axis=0, keepdims=True)

    def across(x):
        return jnp.sum(x, axis=1, keepdims=True)

    def advance(state):
        qc, qr, wc, wr, it, uc, rho = state
        mc = across(change * qr)
        gc = across(moved * qr)
        mr = down(change_t * qc)
        alpha = rho / down(qc * gc)
        it = it + alpha * qc
        wc = wc - alpha * mc
        wr = wr - alpha * mr
        uc = uc - alpha * gc
        rho_new = down(wc * uc)
        return wc, wr, it, uc, rho_new, rho_new / rho

    def inner(_, state):
        wc, wr, it, uc, rho, beta = advance(state)
        return wc + beta * state[0], wr + beta * state[1], wc, wr, it, uc, rho

    wc, wr = unit(0, S + 1), unit(1, S + 1)
    start = across(gram * wr) + jnp.zeros((SIDE, LANES), jnp.float32)
    state = (unit(0, 0), unit(1, 0), wc, wr, jnp.zeros((SIDE, LANES), jnp.float32), start, down(wc * start))
    state = lax.fori_loop(0, S - 1, inner, state)
    _, _, it, _, _, beta = advance(state)
    coef[0] = it
    coef[1] = state[0]
    beta_ref[...] = jnp.zeros((8, LANES), jnp.float32) + beta

    def combine(q):
        start = planes * q + DEEP - 1 + q % 2

        def strip(s, carry):
            i, part = s // (rows // 8), s % (rows // 8)
            at = pl.ds(pl.multiple_of(part * 8, 8), 8)
            sums = [None, None]
            for v in range(2 * S - 1):
                c, k = (0, v) if v < S else (1, v - S)
                row = v if v < S else v + 1
                x = X[c, k, start + i, at, :]
                for o in range(2):
                    f = coef[o, row:row + 1, :]
                    f = jnp.concatenate([f] * (depth // LANES), axis=1)
                    term = f * x
                    sums[o] = term if sums[o] is None else sums[o] + term
            out_dx[q, i, at, :] = sums[0]
            out_q[q, i, at, :] = sums[1]
            return carry
        lax.fori_loop(0, (planes + 1) * (rows // 8), strip, 0, unroll=2)

    odd = p % 2

    def outgoing_dx(j):
        q = flipped(p, j, group)
        return pltpu.make_async_remote_copy(
            src_ref=out_dx.at[q], dst_ref=dx.at[pl.ds(q % 2, planes + 1), block_rows(b), :],
            send_sem=o_send.at[0], recv_sem=o_recv.at[j],
            device_id=device(g, q), device_id_type=MESH)

    def outgoing_q(j):
        q = flipped(p, j, group)
        return pltpu.make_async_remote_copy(
            src_ref=out_q.at[q, pl.ds(1 - q % 2, planes)], dst_ref=last.at[:, block_rows(b), :],
            send_sem=q_send.at[0], recv_sem=q_recv.at[0],
            device_id=device(g, q), device_id_type=MESH)

    def source_of(j):
        return flipped(p, j, group) if group & (group - 1) == 0 else (p + group - j) % group

    def dx_from(j):
        at = block_rows(place(source_of(j)))
        return pltpu.make_async_remote_copy(
            src_ref=out_dx.at[p], dst_ref=dx.at[pl.ds(odd, planes + 1), at, :],
            send_sem=o_send.at[0], recv_sem=o_recv.at[j],
            device_id=device(g, source_of(j)), device_id_type=MESH)

    mate = p + 1 - 2 * odd

    def forward_of(block):
        at = block_rows(block)
        return pltpu.make_async_remote_copy(
            src_ref=dx.at[planes - odd * (planes - 1), at, :],
            dst_ref=dx.at[odd * (planes + 1), at, :],
            send_sem=f_send.at[0], recv_sem=f_recv.at[0],
            device_id=device(g, mate), device_id_type=MESH)

    for j in order:
        combine(flipped(p, j, group))
        outgoing_dx(j).start()
    combine(p)
    for j in order:
        outgoing_q(j).start()
    own = pltpu.make_async_copy(out_dx.at[p], dx.at[pl.ds(odd, planes + 1), block_rows(b), :], own_sem.at[2])
    own.start()
    own_q = pltpu.make_async_copy(out_q.at[p, pl.ds(1 - odd, planes)], last.at[:, block_rows(b), :], own_sem.at[3])
    own_q.start()
    own.wait()
    forward_of(b).start()
    for j in [order[-1]] + order[:-1]:
        dx_from(j).wait_recv()
        forward_of(place(source_of(j))).start()
    own_q.wait()
    drained(dx.at[0], f_recv.at[0])
    drained(others, a_send.at[0])
    drained(out_dx.at[pl.ds(0, group - 1)], o_send.at[0])
    drained(dx.at[0], f_send.at[0])
    drained(last.at[:, pl.ds(0, width - rows), :], q_recv.at[0])
    drained(last.at[:, pl.ds(0, width - rows), :], q_send.at[0])


def finish(sol, res, dx, last, beta, sol_out, res_out, dir_out, buf, sem):
    planes, width, depth = sol.shape
    piece = width // PIECES
    row_ids = lax.broadcasted_iota(jnp.int32, (piece, depth), 0)
    col_ids = lax.broadcasted_iota(jnp.int32, (piece, depth), 1)
    factor = jnp.concatenate([beta[0:1, :]] * (depth // LANES), axis=1)
    copies = []
    for i in range(planes):
        for s in range(PIECES):
            at = pl.ds(s * piece, piece)
            cur = dx[i + 1, at, :]
            low = dx[i + 1, s * piece - 1:s * piece, :] if s else jnp.zeros((1, depth), jnp.float32)
            high = dx[i + 1, (s + 1) * piece:(s + 1) * piece + 1, :] if s < PIECES - 1 else jnp.zeros((1, depth), jnp.float32)
            total = dx[i, at, :] + dx[i + 2, at, :]
            total = total + jnp.where(row_ids == 0, low, pltpu.roll(cur, 1, 0))
            total = total + jnp.where(row_ids == piece - 1, high, pltpu.roll(cur, piece - 1, 0))
            total = total + jnp.where(col_ids == 0, 0.0, pltpu.roll(cur, 1, 1))
            total = total + jnp.where(col_ids == depth - 1, 0.0, pltpu.roll(cur, depth - 1, 1))
            buf[0, i, at, :] = sol[i, at, :] + cur
            remain = res[i, at, :] - (6.0 * cur - total)
            buf[1, i, at, :] = remain
            buf[2, i, at, :] = remain + factor * last[i, at, :]
            for o, target in enumerate((sol_out, res_out, dir_out)):
                copy = pltpu.make_async_copy(buf.at[o, i, at, :], target.at[i, at, :], sem.at[o, i, s])
                copy.start()
                copies.append(copy)
    for copy in copies:
        copy.wait()


def on_device(gz_count, ga, sol, res, direction):
    planes, width, depth = sol.shape
    group, groups = 2 * ga, gz_count // 2
    tall, rows = planes * group, width // group
    table = jnp.asarray(np.concatenate(gram_tables()))
    vmem = pl.BlockSpec(memory_space=pltpu.VMEM)
    dma = pltpu.SemaphoreType.DMA
    anywhere = pl.BlockSpec(memory_space=pltpu.HBM)
    f32 = jnp.float32
    dx, last, beta = pl.pallas_call(
        functools.partial(kernel, gz_count, ga),
        out_shape=[pltpu.VMEM((planes + 2, width, depth), f32), pltpu.VMEM((planes, width, depth), f32),
                   pltpu.VMEM((8, LANES), f32)],
        in_specs=[anywhere] * 3,
        out_specs=[vmem] * 3,
        scratch_shapes=[
            pltpu.VMEM((2, S + 1, tall + 2 * DEEP, rows, depth), f32),
            pltpu.VMEM((2, S, 2, DEEP + 1, tall + 16, depth), f32),
            pltpu.VMEM((2, 2, 2, DEEP, tall, depth), f32),
            pltpu.VMEM((2, 2, FIRST[1] - 1, 4, depth), f32),
            pltpu.VMEM((2, 2, FIRST[1] - 1, 4, depth), f32),
            pltpu.VMEM((2, 2, 2, 1, 1, depth), f32),
            pltpu.VMEM((2, 2, 2, 1, 1, depth), f32),
            pltpu.VMEM((COUNT, 8, LANES), f32),
            pltpu.VMEM((gz_count * ga, 1, LANES), f32),
            pltpu.VMEM((2, SIDE, LANES), f32),
            pltpu.VMEM((group, planes + 1, rows, depth), f32),
            pltpu.VMEM((group, planes + 1, rows, depth), f32),
            pltpu.VMEM((2, planes, width, depth), f32),
            pltpu.VMEM((2 * COUNT + 2, SIDE, LANES), f32),
            dma((1,)), dma((2,)), dma((4,)),
            dma((2,)), dma((2, 2, 2)), dma((2,)), dma((2, 2, 2)),
            dma((2, 2, 2, 2)), dma((2, 2, 2, 2)),
            dma((1,)), dma((1,)),
            dma((1,)), dma((group,)), dma((1,)), dma((1,)), dma((1,)), dma((1,)),
            dma((3,)),
        ],
        compiler_params=pltpu.CompilerParams(collective_id=0, has_side_effects=True, vmem_limit_bytes=VMEM_LIMIT),
    )(*(pltpu.with_memory_space_constraint(x, pltpu.HBM) for x in (res, direction, table)))
    shape = jax.ShapeDtypeStruct(sol.shape, f32)
    return pl.pallas_call(
        finish,
        out_shape=[shape] * 3,
        in_specs=[vmem] * 5,
        out_specs=[anywhere] * 3,
        scratch_shapes=[pltpu.VMEM((3,) + sol.shape, f32), dma((3, planes, PIECES))],
        compiler_params=pltpu.CompilerParams(vmem_limit_bytes=8 * 2 ** 20),
    )(sol, res, dx, last, beta)


def solution(mesh):
    spec = P(("gz", "ga"), None, None)
    return jax.shard_map(
        functools.partial(on_device, mesh.shape["gz"], mesh.shape["ga"]),
        mesh=mesh, in_specs=(spec, spec, spec), out_specs=(spec, spec, spec), check_vma=False,
    )
```

```python
import functools

import jax
import jax.numpy as jnp
import numpy as np
from jax import lax
from jax.experimental import pallas as pl
from jax.experimental.pallas import tpu as pltpu
from jax.sharding import PartitionSpec as P

S = 8
MESH = pl.DeviceIdType.MESH
first_scale = -1.0 / 6.0
next_scale = -1.0 / 3.0
SIDE = 24
LANES = 128
FIRST = (S - 2, S - 3)
DEEP = max(FIRST)
UNROLL = 16
PIECES = 4
VMEM_LIMIT = 44 * 2 ** 20


def change_matrix(steps):
    count = 2 * steps + 1
    table = np.zeros((count, count), np.float64)
    for offset, length in ((0, steps + 1), (steps + 1, steps)):
        for power in range(length - 1):
            column = offset + power
            table[column, column] = 6.0
            if power == 0:
                table[column + 1, column] = 6.0
            else:
                table[column + 1, column] = 3.0
                table[column - 1, column] = 3.0
    return table


def dd(power, odd):
    return 2 * power + odd


def rr(power, odd):
    return 2 * S + 1 + 2 * power + odd


def dr(power, odd):
    return 4 * S + 2 * power + odd


COUNT = 6 * S


def gram_tables():
    def moment(kind, order):
        half, odd = order // 2, order % 2
        row = np.zeros(COUNT)
        row[kind(half, odd)] += 2.0
        row[kind(0, odd)] -= 1.0
        return row

    size = 2 * S + 1
    table = np.zeros((COUNT, size, size))
    for i in range(size):
        for j in range(size):
            a, b = (i if i <= S else i - S - 1), (j if j <= S else j - S - 1)
            kind = dd if (i <= S and j <= S) else rr if (i > S and j > S) else dr
            table[:, i, j] = 0.5 * (moment(kind, a + b) + moment(kind, abs(a - b)))
    moved = table @ change_matrix(S)

    def padded(t):
        out = np.zeros((t.shape[0], SIDE, LANES), np.float32)
        out[:, :size, :size] = t
        return out

    change = np.stack([change_matrix(S), change_matrix(S).T])
    return padded(table), padded(moved), padded(change)


def flipped(p, bits, group):
    if group & (group - 1):
        return (p + bits) % group
    out, step = p, 1
    while step < group:
        if bits & step:
            out = out + step * (1 - 2 * ((p // step) % 2))
        step *= 2
    return out


def send_order(group):
    if group & (group - 1):
        return list(range(1, group))
    first = [j for j in range(2, group) if (j // 2) & (j // 2 - 1) == 0]
    first = first[::2] + first[1::2]
    return first + [j for j in range(2, group) if j not in first] + [1]


def neighbours(cur, total, low, high):
    height = cur.shape[0]
    total = total + jnp.concatenate([low, cur[:height - 1]], axis=0)
    total = total + jnp.concatenate([cur[1:], high], axis=0)
    return across_columns(cur, total)


def across_columns(cur, total):
    none = jnp.zeros((cur.shape[0], 1), jnp.float32)
    total = total + jnp.concatenate([none, cur[:, :cur.shape[1] - 1]], axis=1)
    return total + jnp.concatenate([cur[:, 1:], none], axis=1)


def kernel(gz_count, ga, res_ref, dir_ref, table_hbm, sol_ref,
           sol_out, res_out, last, beta_ref,
           X, halo, stage, edge, edge_in, edge_1, edge_1_in, accs, red, coef, dx, out_dx, out_q, held, sol_in, table,
           in_send, in_recv, own_sem, z_send, z_recv, r_send, r_recv, e_send, e_recv,
           a_send, a_recv, o_send, o_recv, q_send, q_recv, f_send, f_recv, load_sem):
    group = 2 * ga
    groups = gz_count // 2
    count = gz_count * ga
    planes, width, depth = res_ref.shape
    tall = planes * group
    rows = width // group
    iz, ia = lax.axis_index("gz"), lax.axis_index("ga")
    me = iz * ga + ia
    g = iz // 2
    p = (iz % 2) * ga + ia
    order = send_order(group)

    def place(position):
        upper = position // ga
        return upper * (3 * ga - 1 - position) + (1 - upper) * position

    b = place(p)

    def device(which, position):
        return (which * 2 + position // ga, position % ga)

    def block_rows(block):
        return pl.ds(pl.multiple_of(block * rows, rows), rows)

    loads = [pltpu.make_async_copy(source, target, load_sem.at[i]) for i, (source, target) in enumerate((
        (dir_ref, held.at[0]), (res_ref, held.at[1]), (table_hbm, table), (sol_ref, sol_in)))]
    for load in loads:
        load.start()

    below, above = g > 0, g < groups - 1
    before, after = b > 0, b < group - 1
    z_there, r_there = (below, above), (before, after)

    barrier = pltpu.get_barrier_semaphore()

    def greet(target):
        pl.semaphore_signal(barrier, inc=1, device_id=target, device_id_type=MESH)

    if groups - 1 <= 3:
        for j in range(1, group):
            greet(device(g, flipped(p, j, group)))
        for up in range(2):
            @pl.when(z_there[up])
            def _():
                greet(device(g + 2 * up - 1, p))
            for side in range(2):
                @pl.when(z_there[up] & r_there[side])
                def _():
                    greet(device(g + 2 * up - 1, place(b + 2 * side - 1)))
        below_1, above_1 = jnp.minimum(g, 1), jnp.minimum(groups - 1 - g, 1)
        before_1, after_1 = jnp.minimum(b, 1), jnp.minimum(group - 1 - b, 1)
        pl.semaphore_wait(barrier, group - 1 + (below_1 + above_1) * (1 + before_1 + after_1))
    else:
        def greet_all(j, carry):
            t = (me + j) % count
            greet((t // ga, t % ga))
            return carry
        lax.fori_loop(1, count, greet_all, 0)
        pl.semaphore_wait(barrier, count - 1)

    def incoming(c, j):
        q = flipped(p, j, group)
        return pltpu.make_async_remote_copy(
            src_ref=held.at[c, :, block_rows(place(q)), :],
            dst_ref=X.at[c, 0, pl.ds(DEEP + planes * p, planes)],
            send_sem=in_send.at[0], recv_sem=in_recv.at[c],
            device_id=device(g, q), device_id_type=MESH)

    def own_in(c):
        return pltpu.make_async_copy(
            held.at[c, :, block_rows(b), :],
            X.at[c, 0, pl.ds(DEEP + planes * p, planes)], own_sem.at[c])

    loads[0].wait()
    for j in order:
        incoming(0, j).start()
    own_in(0).start()
    loads[1].wait()
    for j in order:
        incoming(1, j).start()
    own_in(1).start()

    def deep(c, k):
        return 2 if k else FIRST[c]

    def spread(c, k):
        return 1 if k else 4 if deep(c, k) < 6 else 8

    exchanges = [(c, k) for c in range(2) for k in (0, FIRST[c])]

    def edges_of(c, k, incoming_side, up, side):
        if k:
            return (edge_1_in if incoming_side else edge_1).at[c, up, side]
        if spread(c, k) == 4:
            return (edge_in if incoming_side else edge).at[up, side, pl.ds(0, deep(c, k) - 1)]
        if incoming_side:
            return halo.at[c, k, side, pl.ds(1, deep(c, k) - 1), pl.ds(up * (tall + 8), 8)]
        return stage.at[c, 0, side, pl.ds(0, deep(c, k) - 1), pl.ds(up * (tall - 8), 8)]

    for c, k in exchanges:
        d = deep(c, k)
        for missing, at in ((g == 0, DEEP - d), (g == groups - 1, tall + DEEP)):
            @pl.when(missing)
            def _():
                X[c, k, at:at + d] = jnp.zeros((d, rows, depth), jnp.float32)
        for side, missing in ((0, b == 0), (1, b == group - 1)):
            @pl.when(missing)
            def _():
                halo[c, k, side, 1:d + 1] = jnp.zeros((d, tall + 16, depth), jnp.float32)
        for up in range(2):
            for side in range(2):
                @pl.when(jnp.logical_not(z_there[up] & r_there[side]))
                def _():
                    ref = edges_of(c, k, True, up, side)
                    ref[...] = jnp.zeros(ref.shape, jnp.float32)

    def z_copy(c, k, up):
        d = deep(c, k)
        source = DEEP + tall - d if up else DEEP
        target = DEEP - d if up else tall + DEEP
        return pltpu.make_async_remote_copy(
            src_ref=X.at[c, k, pl.ds(source, d)],
            dst_ref=X.at[c, k, pl.ds(target, d)],
            send_sem=z_send.at[up], recv_sem=z_recv.at[c, min(k, 1), up],
            device_id=device(g + 2 * up - 1, p), device_id_type=MESH)

    def r_copy(c, k, up):
        d = deep(c, k)
        return pltpu.make_async_remote_copy(
            src_ref=stage.at[c, min(k, 1), up, pl.ds(0, d)],
            dst_ref=halo.at[c, k, 1 - up, pl.ds(1, d), pl.ds(8, tall)],
            send_sem=r_send.at[up], recv_sem=r_recv.at[c, min(k, 1), up],
            device_id=device(g, place(b + 2 * up - 1)), device_id_type=MESH)

    def e_copy(c, k, up, side):
        h = min(k, 1)
        return pltpu.make_async_remote_copy(
            src_ref=edges_of(c, k, False, up, side),
            dst_ref=edges_of(c, k, True, 1 - up, 1 - side),
            send_sem=e_send.at[c, h, up, side], recv_sem=e_recv.at[c, h, 1 - up, 1 - side],
            device_id=device(g + 2 * up - 1, place(b + 2 * side - 1)), device_id_type=MESH)

    def e_arrival(c, k, up, side):
        h = min(k, 1)
        return pltpu.make_async_remote_copy(
            src_ref=edges_of(c, k, False, up, side),
            dst_ref=edges_of(c, k, True, up, side),
            send_sem=e_send.at[c, h, up, side], recv_sem=e_recv.at[c, h, up, side],
            device_id=device(g + 2 * up - 1, place(b + 2 * side - 1)), device_id_type=MESH)

    def send_z(c, k):
        for up in range(2):
            @pl.when(z_there[up])
            def _():
                z_copy(c, k, up).start()

    def send_edges(c, k):
        n = spread(c, k)
        if n < 8:
            for up in range(2):
                for side in range(2):
                    ref = edges_of(c, k, False, up, side)
                    for i in range(deep(c, k) - 1):
                        if n == 1:
                            row = (rows - 1) * side
                            ref[i] = X[c, k, DEEP + (tall - 1) * up, row:row + 1, :]
                        else:
                            ref[i] = stage[c, 0, side, i, up * (tall - n):up * (tall - n) + n, :]
        for up in range(2):
            for side in range(2):
                @pl.when(z_there[up] & r_there[side])
                def _():
                    e_copy(c, k, up, side).start()

    def send_rows(c, k):
        for side in range(2):
            @pl.when(r_there[side])
            def _():
                r_copy(c, k, side).start()

    def receive(c, k):
        for side in range(2):
            @pl.when(r_there[side])
            def _():
                r_copy(c, k, 1 - side).wait_recv()
        for up in range(2):
            for side in range(2):
                @pl.when(z_there[up] & r_there[side])
                def _():
                    e_arrival(c, k, up, side).wait_recv()

            @pl.when(z_there[up])
            def _():
                z_copy(c, k, 1 - up).wait_recv()

    def folded(x):
        total = x[0:8]
        for i in range(8, rows, 8):
            total = total + x[i:i + 8]
        out = total[:, 0:LANES]
        for i in range(LANES, depth, LANES):
            out = out + total[:, i:i + LANES]
        return out

    z_scale = [jnp.minimum(g, 1).astype(jnp.float32), jnp.minimum(groups - 1 - g, 1).astype(jnp.float32)]
    r_scale = [jnp.minimum(b, 1).astype(jnp.float32), jnp.minimum(group - 1 - b, 1).astype(jnp.float32)]

    plane_ids = lax.broadcasted_iota(jnp.int32, (tall + 16, depth), 0)
    inside = (jnp.where(plane_ids < 8, z_scale[0], 1.0) * jnp.where(plane_ids >= tall + 8, z_scale[1], 1.0))

    def settle(c, k):
        n = spread(c, k)
        if n < 8:
            for up in range(2):
                at = tall + 8 if up else 8 - n
                for side in range(2):
                    ref = edges_of(c, k, True, up, side)
                    for i in range(deep(c, k) - 1):
                        halo[c, k, side, i + 1, at:at + n, :] = ref[i]
        for e in range(1, deep(c, k)):
            for up in range(2):
                at = tall - 1 + e if up else -e
                put_row(c, k, at, X[c, k, DEEP + at])

    def put_row(c, k, z, new):
        at = pl.ds(8 + z, 1)
        halo[c, k, 0, 0, at, :] = new[0:1]
        halo[c, k, 1, 0, at, :] = new[rows - 1:rows]

    def extend_rows(c, k, reach):
        scale = first_scale if k == 1 else next_scale

        def extend_row(i, carry):
            for side in range(2):
                cur = halo[c, k - 1, side, i]
                total = halo[c, k - 1, side, i - 1] + halo[c, k - 1, side, i + 1]
                total = total + pltpu.roll(cur, 1, 0) + pltpu.roll(cur, tall + 15, 0)
                total = across_columns(cur, total)
                new = total * (inside * (r_scale[side] * scale))
                if k > 1:
                    new = new - halo[c, k - 2, side, i]
                halo[c, k, side, i] = new
            return carry

        lax.fori_loop(1, reach + 1, extend_row, 0, unroll=True)

    def extend_planes(c, k, reach):
        scale = first_scale if k == 1 else next_scale

        def extend_plane(e, carry):
            for up in range(2):
                z = tall - 1 + e if up else -e
                at = DEEP + z
                cur = X[c, k - 1, at]
                total = X[c, k - 1, at - 1] + X[c, k - 1, at + 1]
                low = halo[c, k - 1, 0, 1, pl.ds(8 + z, 1), :]
                high = halo[c, k - 1, 1, 1, pl.ds(8 + z, 1), :]
                total = neighbours(cur, total, low, high)
                new = total * (z_scale[up] * scale)
                if k > 1:
                    new = new - X[c, k - 2, at]
                X[c, k, at] = new
                if reach > 1:
                    put_row(c, k, z, new)
            return carry

        lax.fori_loop(1, reach + 1, extend_plane, 0, unroll=True)

    def names_of(c, k):
        if c == 0:
            names = [(dd(k, 0), "new", "new"), (dd(k - 1, 1), "new", "cur")]
            if k == 1:
                names.append((dd(0, 0), "cur", "cur"))
        else:
            names = [(rr(k, 0), "new", "new"), (rr(k - 1, 1), "new", "cur"),
                     (dr(k, 0), "new", "other"), (dr(k - 1, 1), "cur", "other")]
            if k == S - 1:
                names.append((dr(k, 1), "new", "ahead"))
            if k == 1:
                names += [(rr(0, 0), "cur", "cur"), (dr(0, 0), "cur", "start")]
        return names

    def sent(c, k):
        return k == FIRST[c]

    def plane(c, k, z, sums, reach):
        at = z + DEEP
        cur = X[c, k - 1, at]
        total = X[c, k - 1, at - 1] + X[c, k - 1, at + 1]
        low = halo[c, k - 1, 0, 1, pl.ds(8 + z, 1), :]
        high = halo[c, k - 1, 1, 1, pl.ds(8 + z, 1), :]
        total = neighbours(cur, total, low, high)
        if k == 1:
            new = total * first_scale
        else:
            new = total * next_scale - X[c, k - 2, at]
        X[c, k, at] = new
        if sent(c, k):
            put_rows(c, k, z, new)
        elif reach > 1:
            put_row(c, k, z, new)
        return products(c, k, z, sums, new, cur) if sums else sums

    def products(c, k, z, sums, new, cur):
        names = names_of(c, k)
        at = z + DEEP
        have = {"new": new, "cur": cur}
        if any("other" in n for n in names):
            have["other"] = X[0, k, at]
        if any("ahead" in n for n in names):
            have["ahead"] = X[0, k + 1, at]
        if any("start" in n for n in names):
            have["start"] = X[0, 0, at]
        return tuple(s + folded(have[l] * have[r]) for s, (_, l, r) in zip(sums, names))

    def all_products(c, k):
        def body(z, sums):
            return products(c, k, z, sums, X[c, k, z + DEEP], X[c, k - 1, z + DEEP])
        return lax.fori_loop(0, tall, body, zero_sums(c, k), unroll=4)

    def put_rows(c, k, z, new):
        put_row(c, k, z, new)
        at = pl.ds(z, 1)
        for i in range(deep(c, k)):
            stage[c, min(k, 1), 0, i, at, :] = new[i:i + 1]
            stage[c, min(k, 1), 1, i, at, :] = new[rows - 1 - i:rows - i]

    def zero_sums(c, k):
        return tuple(jnp.zeros((8, LANES), jnp.float32) for _ in names_of(c, k))

    def keep(c, k, sums):
        for s, (slot, _, _) in zip(sums, names_of(c, k)):
            accs[slot] = s

    def ends(c, k, width_of, sums, reach):
        def body(i, sums):
            return plane(c, k, i + (i // width_of) * (tall - 2 * width_of), sums, reach)
        return lax.fori_loop(0, 2 * width_of, body, sums, unroll=True)

    def middle(c, k, width_of, sums, reach):
        length = tall - 2 * width_of
        unroll = max(u for u in range(1, UNROLL + 1) if length % u == 0)
        return lax.fori_loop(width_of, tall - width_of, lambda z, s: plane(c, k, z, s, reach), sums, unroll=unroll)

    def chain_round(c, k):
        d = deep(c, k)
        settle(c, k)
        outer = c == 1 and k == 0 and 2 * (d + 1) < tall
        sums = []
        for m in range(1, d + 1):
            n, reach = k + m, d - m
            if reach:
                extend_rows(c, n, reach)
                extend_planes(c, n, reach)
            sums.append((ends if outer else middle)(c, n, 2 + reach if outer else 0, () if outer else zero_sums(c, n), reach))
        if sent(c, k + d):
            send_z(c, k + d)
            if outer:
                send_edges(c, k + d)
        for m in range(1, d + 1):
            n, reach = k + m, d - m
            if outer and m > 1 and reach:
                extend_rows(c, n, reach)
            if outer:
                middle(c, n, 2 + reach, (), reach)
            else:
                keep(c, n, sums[m - 1])
        if sent(c, k + d):
            send_rows(c, k + d)
            if not outer:
                send_edges(c, k + d)
        if outer:
            for m in range(1, d + 1):
                keep(c, k + m, all_products(c, k + m))

    def arrive(c):
        own_in(c).wait()
        others = held.at[c, :, pl.ds(0, width - rows), :]
        pltpu.make_async_copy(others, others, in_recv.at[c]).wait()
        send_z(c, 0)

        def copy_rows(z, carry):
            put_rows(c, 0, z, X[c, 0, z + DEEP])
            return carry
        lax.fori_loop(0, tall, copy_rows, 0, unroll=4)
        send_edges(c, 0)
        send_rows(c, 0)

    arrive(0)
    arrive(1)
    for h in range(2):
        for c in range(2):
            receive(c, h * FIRST[c])
            chain_round(c, h * FIRST[c])

    lanes = lax.broadcasted_iota(jnp.int32, (8, LANES), 1)
    packed = jnp.zeros((8, LANES), jnp.float32)
    for t in range(COUNT // 8):
        part = jnp.sum(jnp.sum(accs[8 * t:8 * t + 8], axis=1), axis=1, keepdims=True)
        packed = packed + jnp.where(lanes == t, part, 0.0)
    red[me] = jnp.sum(pltpu.roll(packed, 0, 1, stride=8, stride_axis=0), axis=0, keepdims=True)

    far = 2 * ((2 * g) // groups) - 1

    def moments_to(j):
        t = (me + far * j + count) % count
        return pltpu.make_async_remote_copy(
            src_ref=red.at[me], dst_ref=red.at[me], send_sem=a_send.at[0], recv_sem=a_recv.at[0],
            device_id=(t // ga, t % ga), device_id_type=MESH)

    def start_moments(j, carry):
        moments_to(j).start()
        return carry

    lax.fori_loop(1, count, start_moments, 0, unroll=count <= 64)
    def drained(ref, sem):
        pltpu.make_async_copy(ref, ref, sem).wait()

    drained(held.at[:, :, pl.ds(0, width - rows), :], in_send.at[0])
    for up in range(2):
        @pl.when(z_there[up])
        def _():
            drained(X.at[0, pl.ds(0, 5), pl.ds(0, 3)], z_send.at[up])

        @pl.when(r_there[up])
        def _():
            drained(halo.at[0, pl.ds(0, 3), 0, pl.ds(0, 5), pl.ds(8, tall)], r_send.at[up])

        for side in range(2):
            @pl.when(z_there[up] & r_there[side])
            def _():
                for c, k in exchanges:
                    e_copy(c, k, up, side).wait_send()
    others = red.at[pl.ds(0, count - 1)]
    drained(others, a_recv.at[0])
    total = jnp.sum(red[...], axis=0)

    loads[2].wait()
    gram = jnp.zeros((SIDE, LANES), jnp.float32)
    moved = jnp.zeros((SIDE, LANES), jnp.float32)
    for e in range(COUNT):
        at = 8 * (e % 8) + e // 8
        value = total[0:1, at:at + 1]
        gram = gram + value * table[e]
        moved = moved + value * table[COUNT + e]
    change, change_t = table[2 * COUNT], table[2 * COUNT + 1]

    def unit(axis, at):
        ids = lax.broadcasted_iota(jnp.int32, (SIDE, LANES), axis)
        return jnp.where(ids == at, 1.0, 0.0).astype(jnp.float32)

    def down(x):
        return jnp.sum(x, axis=0, keepdims=True)

    def across(x):
        return jnp.sum(x, axis=1, keepdims=True)

    def advance(state):
        qc, qr, wc, wr, it, uc, rho = state
        mc = across(change * qr)
        gc = across(moved * qr)
        mr = down(change_t * qc)
        alpha = rho / down(qc * gc)
        it = it + alpha * qc
        wc = wc - alpha * mc
        wr = wr - alpha * mr
        uc = uc - alpha * gc
        rho_new = down(wc * uc)
        return wc, wr, it, uc, rho_new, rho_new / rho

    def inner(_, state):
        wc, wr, it, uc, rho, beta = advance(state)
        return wc + beta * state[0], wr + beta * state[1], wc, wr, it, uc, rho

    wc, wr = unit(0, S + 1), unit(1, S + 1)
    start = across(gram * wr) + jnp.zeros((SIDE, LANES), jnp.float32)
    state = (unit(0, 0), unit(1, 0), wc, wr, jnp.zeros((SIDE, LANES), jnp.float32), start, down(wc * start))
    state = lax.fori_loop(0, S - 1, inner, state)
    _, _, it, _, _, beta = advance(state)
    coef[0] = it
    coef[1] = state[0]
    beta_ref[...] = jnp.zeros((8, LANES), jnp.float32) + beta

    tile = 16 if rows % 16 == 0 else 8

    def combine(o, start, out, height):
        def strip(s, carry):
            i, part = s // (rows // tile), s % (rows // tile)
            at = pl.ds(pl.multiple_of(part * tile, tile), tile)
            total = None
            for v in range(2 * S - 1):
                c, k = (0, v) if v < S else (1, v - S)
                row = v if v < S else v + 1
                f = coef[o, row:row + 1, :]
                f = jnp.concatenate([f] * (depth // LANES), axis=1)
                term = f * X[c, k, start + i, at, :]
                total = term if total is None else total + term
            out[i, at, :] = total
            return carry
        lax.fori_loop(0, height * (rows // tile), strip, 0, unroll=2)

    def combine_dx(q):
        combine(0, planes * q + DEEP - 1 + q % 2, out_dx.at[q], planes + 1)

    def combine_q(q):
        combine(1, planes * q + DEEP, out_q.at[q], planes)

    odd = p % 2

    def outgoing_dx(j):
        q = flipped(p, j, group)
        return pltpu.make_async_remote_copy(
            src_ref=out_dx.at[q], dst_ref=dx.at[pl.ds(q % 2, planes + 1), block_rows(b), :],
            send_sem=o_send.at[0], recv_sem=o_recv.at[j],
            device_id=device(g, q), device_id_type=MESH)

    def outgoing_q(j):
        q = flipped(p, j, group)
        return pltpu.make_async_remote_copy(
            src_ref=out_q.at[q], dst_ref=last.at[:, block_rows(b), :],
            send_sem=q_send.at[0], recv_sem=q_recv.at[0],
            device_id=device(g, q), device_id_type=MESH)

    def source_of(j):
        return flipped(p, j, group) if group & (group - 1) == 0 else (p + group - j) % group

    def dx_from(j):
        at = block_rows(place(source_of(j)))
        return pltpu.make_async_remote_copy(
            src_ref=out_dx.at[p], dst_ref=dx.at[pl.ds(odd, planes + 1), at, :],
            send_sem=o_send.at[0], recv_sem=o_recv.at[j],
            device_id=device(g, source_of(j)), device_id_type=MESH)

    mate = p + 1 - 2 * odd

    def forward_of(block):
        at = block_rows(block)
        return pltpu.make_async_remote_copy(
            src_ref=dx.at[planes - odd * (planes - 1), at, :],
            dst_ref=dx.at[odd * (planes + 1), at, :],
            send_sem=f_send.at[0], recv_sem=f_recv.at[0],
            device_id=device(g, mate), device_id_type=MESH)

    for j in order:
        combine_dx(flipped(p, j, group))
        outgoing_dx(j).start()
    combine_dx(p)
    own = pltpu.make_async_copy(out_dx.at[p], dx.at[pl.ds(odd, planes + 1), block_rows(b), :], own_sem.at[2])
    own.start()
    for j in order:
        combine_q(flipped(p, j, group))
        outgoing_q(j).start()
    combine_q(p)
    own_q = pltpu.make_async_copy(out_q.at[p], last.at[:, block_rows(b), :], own_sem.at[3])
    own_q.start()
    own.wait()
    forward_of(b).start()
    for j in [order[-1]] + order[:-1]:
        dx_from(j).wait_recv()
        forward_of(place(source_of(j))).start()
    own_q.wait()
    drained(dx.at[0], f_recv.at[0])
    drained(others, a_send.at[0])
    drained(out_dx.at[pl.ds(0, group - 1)], o_send.at[0])
    drained(dx.at[0], f_send.at[0])
    loads[3].wait()

    piece = width // PIECES
    for i in range(planes):
        for t in range(PIECES):
            at = pl.ds(t * piece, piece)
            cur = dx[i + 1, at, :]
            none = jnp.zeros((1, depth), jnp.float32)
            low = dx[i + 1, t * piece - 1:t * piece, :] if t else none
            high = dx[i + 1, (t + 1) * piece:(t + 1) * piece + 1, :] if t < PIECES - 1 else none
            total = neighbours(cur, dx[i, at, :] + dx[i + 2, at, :], low, high)
            sol_out[i, at, :] = sol_in[i, at, :] + cur
            res_out[i, at, :] = held[1, i, at, :] - (6.0 * cur - total)
    drained(last.at[:, pl.ds(0, width - rows), :], q_recv.at[0])
    drained(last.at[:, pl.ds(0, width - rows), :], q_send.at[0])


def finish(sol, res, last, beta, sol_out, res_out, dir_out, buf, sem):
    planes, width, depth = sol.shape
    piece = width // PIECES
    factor = jnp.concatenate([beta[0:1, :]] * (depth // LANES), axis=1)
    copies = [pltpu.make_async_copy(source, target, sem.at[i])
              for i, (source, target) in enumerate(((sol, sol_out), (res, res_out)))]
    for copy in copies:
        copy.start()
    for i in range(planes):
        for s in range(PIECES):
            at = pl.ds(s * piece, piece)
            buf[i, at, :] = res[i, at, :] + factor * last[i, at, :]
        copies.append(pltpu.make_async_copy(buf.at[i], dir_out.at[i], sem.at[2 + i]))
        copies[-1].start()
    for copy in copies:
        copy.wait()


def on_device(gz_count, ga, sol, res, direction):
    planes, width, depth = sol.shape
    group, groups = 2 * ga, gz_count // 2
    tall, rows = planes * group, width // group
    table = jnp.asarray(np.concatenate(gram_tables()))
    vmem = pl.BlockSpec(memory_space=pltpu.VMEM)
    dma = pltpu.SemaphoreType.DMA
    anywhere = pl.BlockSpec(memory_space=pltpu.HBM)
    f32 = jnp.float32
    outs = pl.pallas_call(
        functools.partial(kernel, gz_count, ga),
        out_shape=[pltpu.VMEM(sol.shape, f32)] * 3 + [pltpu.VMEM((8, LANES), f32)],
        in_specs=[anywhere] * 4,
        out_specs=[vmem] * 4,
        scratch_shapes=[
            pltpu.VMEM((2, S + 1, tall + 2 * DEEP, rows, depth), f32),
            pltpu.VMEM((2, S, 2, DEEP + 1, tall + 16, depth), f32),
            pltpu.VMEM((2, 2, 2, DEEP, tall, depth), f32),
            pltpu.VMEM((2, 2, FIRST[1] - 1, 4, depth), f32),
            pltpu.VMEM((2, 2, FIRST[1] - 1, 4, depth), f32),
            pltpu.VMEM((2, 2, 2, 1, 1, depth), f32),
            pltpu.VMEM((2, 2, 2, 1, 1, depth), f32),
            pltpu.VMEM((COUNT, 8, LANES), f32),
            pltpu.VMEM((gz_count * ga, 1, LANES), f32),
            pltpu.VMEM((2, SIDE, LANES), f32),
            pltpu.VMEM((planes + 2, width, depth), f32),
            pltpu.VMEM((group, planes + 1, rows, depth), f32),
            pltpu.VMEM((group, planes, rows, depth), f32),
            pltpu.VMEM((2, planes, width, depth), f32),
            pltpu.VMEM(sol.shape, f32),
            pltpu.VMEM((2 * COUNT + 2, SIDE, LANES), f32),
            dma((1,)), dma((2,)), dma((4,)),
            dma((2,)), dma((2, 2, 2)), dma((2,)), dma((2, 2, 2)),
            dma((2, 2, 2, 2)), dma((2, 2, 2, 2)),
            dma((1,)), dma((1,)),
            dma((1,)), dma((group,)), dma((1,)), dma((1,)), dma((1,)), dma((1,)),
            dma((4,)),
        ],
        compiler_params=pltpu.CompilerParams(collective_id=0, has_side_effects=True, vmem_limit_bytes=VMEM_LIMIT),
    )(*(pltpu.with_memory_space_constraint(x, pltpu.HBM) for x in (res, direction, table, sol)))
    shape = jax.ShapeDtypeStruct(sol.shape, f32)
    return pl.pallas_call(
        finish,
        out_shape=[shape] * 3,
        in_specs=[vmem] * 4,
        out_specs=[anywhere] * 3,
        scratch_shapes=[pltpu.VMEM(sol.shape, f32), dma((2 + planes,))],
        compiler_params=pltpu.CompilerParams(vmem_limit_bytes=8 * 2 ** 20),
    )(*outs)


def solution(mesh):
    spec = P(("gz", "ga"), None, None)
    return jax.shard_map(
        functools.partial(on_device, mesh.shape["gz"], mesh.shape["ga"]),
        mesh=mesh, in_specs=(spec, spec, spec), out_specs=(spec, spec, spec), check_vma=False,
    )
```

```python
import functools

import jax
import jax.numpy as jnp
import numpy as np
from jax import lax
from jax.experimental import pallas as pl
from jax.experimental.pallas import tpu as pltpu
from jax.sharding import PartitionSpec as P

S = 8
MESH = pl.DeviceIdType.MESH
first_scale = -1.0 / 6.0
next_scale = -1.0 / 3.0
SIDE = 24
LANES = 128
FIRST = (S - 2, S - 3)
DEEP = max(FIRST)
UNROLL = 16
PIECES = 4
VMEM_LIMIT = 44 * 2 ** 20


def change_matrix(steps):
    count = 2 * steps + 1
    table = np.zeros((count, count), np.float64)
    for offset, length in ((0, steps + 1), (steps + 1, steps)):
        for power in range(length - 1):
            column = offset + power
            table[column, column] = 6.0
            if power == 0:
                table[column + 1, column] = 6.0
            else:
                table[column + 1, column] = 3.0
                table[column - 1, column] = 3.0
    return table


def dd(power, odd):
    return 2 * power + odd


def rr(power, odd):
    return 2 * S + 1 + 2 * power + odd


def dr(power, odd):
    return 4 * S + 2 * power + odd


COUNT = 6 * S


def gram_tables():
    def moment(kind, order):
        half, odd = order // 2, order % 2
        row = np.zeros(COUNT)
        row[kind(half, odd)] += 2.0
        row[kind(0, odd)] -= 1.0
        return row

    size = 2 * S + 1
    table = np.zeros((COUNT, size, size))
    for i in range(size):
        for j in range(size):
            a, b = (i if i <= S else i - S - 1), (j if j <= S else j - S - 1)
            kind = dd if (i <= S and j <= S) else rr if (i > S and j > S) else dr
            table[:, i, j] = 0.5 * (moment(kind, a + b) + moment(kind, abs(a - b)))
    moved = table @ change_matrix(S)

    def padded(t):
        out = np.zeros((t.shape[0], SIDE, LANES), np.float32)
        out[:, :size, :size] = t
        return out

    change = np.stack([change_matrix(S), change_matrix(S).T])
    return padded(table), padded(moved), padded(change)


def flipped(p, bits, group):
    if group & (group - 1):
        return (p + bits) % group
    out, step = p, 1
    while step < group:
        if bits & step:
            out = out + step * (1 - 2 * ((p // step) % 2))
        step *= 2
    return out


def send_order(group):
    if group & (group - 1):
        return list(range(1, group))
    first = [j for j in range(2, group) if (j // 2) & (j // 2 - 1) == 0]
    first = first[::2] + first[1::2]
    return first + [j for j in range(2, group) if j not in first] + [1]


def neighbours(cur, total, low, high):
    height = cur.shape[0]
    total = total + jnp.concatenate([low, cur[:height - 1]], axis=0)
    total = total + jnp.concatenate([cur[1:], high], axis=0)
    return across_columns(cur, total)


def across_columns(cur, total):
    none = jnp.zeros((cur.shape[0], 1), jnp.float32)
    total = total + jnp.concatenate([none, cur[:, :cur.shape[1] - 1]], axis=1)
    return total + jnp.concatenate([cur[:, 1:], none], axis=1)


def kernel(gz_count, ga, res_ref, dir_ref, table_hbm, sol_ref,
           sol_out, res_out, last, beta_ref,
           X, halo, stage, edge, edge_in, edge_1, edge_1_in, accs, red, coef, dx, out_dx, out_q, held, sol_in, table,
           in_send, in_recv, own_sem, z_send, z_recv, r_send, r_recv, e_send, e_recv,
           a_send, a_recv, o_send, o_recv, q_send, q_recv, f_send, f_recv, load_sem):
    group = 2 * ga
    groups = gz_count // 2
    count = gz_count * ga
    planes, width, depth = res_ref.shape
    tall = planes * group
    rows = width // group
    iz, ia = lax.axis_index("gz"), lax.axis_index("ga")
    me = iz * ga + ia
    g = iz // 2
    p = (iz % 2) * ga + ia
    order = send_order(group)

    def place(position):
        upper = position // ga
        return upper * (3 * ga - 1 - position) + (1 - upper) * position

    b = place(p)

    def device(which, position):
        return (which * 2 + position // ga, position % ga)

    def block_rows(block):
        return pl.ds(pl.multiple_of(block * rows, rows), rows)

    loads = [pltpu.make_async_copy(source, target, load_sem.at[i]) for i, (source, target) in enumerate((
        (dir_ref, held.at[0]), (res_ref, held.at[1]), (table_hbm, table), (sol_ref, sol_in)))]
    for load in loads:
        load.start()

    below, above = g > 0, g < groups - 1
    before, after = b > 0, b < group - 1
    z_there, r_there = (below, above), (before, after)

    barrier = pltpu.get_barrier_semaphore()

    def greet(target):
        pl.semaphore_signal(barrier, inc=1, device_id=target, device_id_type=MESH)

    if groups - 1 <= 3:
        for j in range(1, group):
            greet(device(g, flipped(p, j, group)))
        for up in range(2):
            @pl.when(z_there[up])
            def _():
                greet(device(g + 2 * up - 1, p))
            for side in range(2):
                @pl.when(z_there[up] & r_there[side])
                def _():
                    greet(device(g + 2 * up - 1, place(b + 2 * side - 1)))
        below_1, above_1 = jnp.minimum(g, 1), jnp.minimum(groups - 1 - g, 1)
        before_1, after_1 = jnp.minimum(b, 1), jnp.minimum(group - 1 - b, 1)
        pl.semaphore_wait(barrier, group - 1 + (below_1 + above_1) * (1 + before_1 + after_1))
    else:
        def greet_all(j, carry):
            t = (me + j) % count
            greet((t // ga, t % ga))
            return carry
        lax.fori_loop(1, count, greet_all, 0)
        pl.semaphore_wait(barrier, count - 1)

    def incoming(c, j):
        q = flipped(p, j, group)
        return pltpu.make_async_remote_copy(
            src_ref=held.at[c, :, block_rows(place(q)), :],
            dst_ref=X.at[c, 0, pl.ds(DEEP + planes * p, planes)],
            send_sem=in_send.at[0], recv_sem=in_recv.at[c],
            device_id=device(g, q), device_id_type=MESH)

    def own_in(c):
        return pltpu.make_async_copy(
            held.at[c, :, block_rows(b), :],
            X.at[c, 0, pl.ds(DEEP + planes * p, planes)], own_sem.at[c])

    loads[0].wait()
    for j in order:
        incoming(0, j).start()
    own_in(0).start()
    loads[1].wait()
    for j in order:
        incoming(1, j).start()
    own_in(1).start()

    def deep(c, k):
        return 2 if k else FIRST[c]

    def spread(c, k):
        return 1 if k else 4 if deep(c, k) < 6 else 8

    exchanges = [(c, k) for c in range(2) for k in (0, FIRST[c])]

    def edges_of(c, k, incoming_side, up, side):
        if k:
            return (edge_1_in if incoming_side else edge_1).at[c, up, side]
        if spread(c, k) == 4:
            return (edge_in if incoming_side else edge).at[up, side, pl.ds(0, deep(c, k) - 1)]
        if incoming_side:
            return halo.at[c, k, side, pl.ds(1, deep(c, k) - 1), pl.ds(up * (tall + 8), 8)]
        return stage.at[c, 0, side, pl.ds(0, deep(c, k) - 1), pl.ds(up * (tall - 8), 8)]

    for c, k in exchanges:
        d = deep(c, k)
        for missing, at in ((g == 0, DEEP - d), (g == groups - 1, tall + DEEP)):
            @pl.when(missing)
            def _():
                X[c, k, at:at + d] = jnp.zeros((d, rows, depth), jnp.float32)
        for side, missing in ((0, b == 0), (1, b == group - 1)):
            @pl.when(missing)
            def _():
                halo[c, k, side, 1:d + 1] = jnp.zeros((d, tall + 16, depth), jnp.float32)
        for up in range(2):
            for side in range(2):
                @pl.when(jnp.logical_not(z_there[up] & r_there[side]))
                def _():
                    ref = edges_of(c, k, True, up, side)
                    ref[...] = jnp.zeros(ref.shape, jnp.float32)

    def z_copy(c, k, up):
        d = deep(c, k)
        source = DEEP + tall - d if up else DEEP
        target = DEEP - d if up else tall + DEEP
        return pltpu.make_async_remote_copy(
            src_ref=X.at[c, k, pl.ds(source, d)],
            dst_ref=X.at[c, k, pl.ds(target, d)],
            send_sem=z_send.at[up], recv_sem=z_recv.at[c, min(k, 1), up],
            device_id=device(g + 2 * up - 1, p), device_id_type=MESH)

    def r_copy(c, k, up):
        d = deep(c, k)
        return pltpu.make_async_remote_copy(
            src_ref=stage.at[c, min(k, 1), up, pl.ds(0, d)],
            dst_ref=halo.at[c, k, 1 - up, pl.ds(1, d), pl.ds(8, tall)],
            send_sem=r_send.at[up], recv_sem=r_recv.at[c, min(k, 1), up],
            device_id=device(g, place(b + 2 * up - 1)), device_id_type=MESH)

    def e_copy(c, k, up, side):
        h = min(k, 1)
        return pltpu.make_async_remote_copy(
            src_ref=edges_of(c, k, False, up, side),
            dst_ref=edges_of(c, k, True, 1 - up, 1 - side),
            send_sem=e_send.at[c, h, up, side], recv_sem=e_recv.at[c, h, 1 - up, 1 - side],
            device_id=device(g + 2 * up - 1, place(b + 2 * side - 1)), device_id_type=MESH)

    def e_arrival(c, k, up, side):
        h = min(k, 1)
        return pltpu.make_async_remote_copy(
            src_ref=edges_of(c, k, False, up, side),
            dst_ref=edges_of(c, k, True, up, side),
            send_sem=e_send.at[c, h, up, side], recv_sem=e_recv.at[c, h, up, side],
            device_id=device(g + 2 * up - 1, place(b + 2 * side - 1)), device_id_type=MESH)

    def send_z(c, k):
        for up in range(2):
            @pl.when(z_there[up])
            def _():
                z_copy(c, k, up).start()

    def send_edges(c, k):
        n = spread(c, k)
        if n < 8:
            for up in range(2):
                for side in range(2):
                    ref = edges_of(c, k, False, up, side)
                    for i in range(deep(c, k) - 1):
                        if n == 1:
                            row = (rows - 1) * side
                            ref[i] = X[c, k, DEEP + (tall - 1) * up, row:row + 1, :]
                        else:
                            ref[i] = stage[c, 0, side, i, up * (tall - n):up * (tall - n) + n, :]
        for up in range(2):
            for side in range(2):
                @pl.when(z_there[up] & r_there[side])
                def _():
                    e_copy(c, k, up, side).start()

    def send_rows(c, k):
        for side in range(2):
            @pl.when(r_there[side])
            def _():
                r_copy(c, k, side).start()

    def receive_rows(c, k):
        for side in range(2):
            @pl.when(r_there[side])
            def _():
                r_copy(c, k, 1 - side).wait_recv()

    def receive_planes(c, k):
        for up in range(2):
            for side in range(2):
                @pl.when(z_there[up] & r_there[side])
                def _():
                    e_arrival(c, k, up, side).wait_recv()

            @pl.when(z_there[up])
            def _():
                z_copy(c, k, 1 - up).wait_recv()

    def folded(x):
        total = x[0:8]
        for i in range(8, rows, 8):
            total = total + x[i:i + 8]
        out = total[:, 0:LANES]
        for i in range(LANES, depth, LANES):
            out = out + total[:, i:i + LANES]
        return out

    z_scale = [jnp.minimum(g, 1).astype(jnp.float32), jnp.minimum(groups - 1 - g, 1).astype(jnp.float32)]
    r_scale = [jnp.minimum(b, 1).astype(jnp.float32), jnp.minimum(group - 1 - b, 1).astype(jnp.float32)]

    plane_ids = lax.broadcasted_iota(jnp.int32, (tall + 16, depth), 0)
    inside = (jnp.where(plane_ids < 8, z_scale[0], 1.0) * jnp.where(plane_ids >= tall + 8, z_scale[1], 1.0))

    def settle(c, k):
        n = spread(c, k)
        if n < 8:
            for up in range(2):
                at = tall + 8 if up else 8 - n
                for side in range(2):
                    ref = edges_of(c, k, True, up, side)
                    for i in range(deep(c, k) - 1):
                        halo[c, k, side, i + 1, at:at + n, :] = ref[i]
        for e in range(1, deep(c, k)):
            for up in range(2):
                at = tall - 1 + e if up else -e
                put_row(c, k, at, X[c, k, DEEP + at])

    def put_row(c, k, z, new):
        at = pl.ds(8 + z, 1)
        halo[c, k, 0, 0, at, :] = new[0:1]
        halo[c, k, 1, 0, at, :] = new[rows - 1:rows]

    def extend_rows(c, k, reach):
        scale = first_scale if k == 1 else next_scale

        def extend_row(i, carry):
            for side in range(2):
                cur = halo[c, k - 1, side, i]
                total = halo[c, k - 1, side, i - 1] + halo[c, k - 1, side, i + 1]
                total = total + pltpu.roll(cur, 1, 0) + pltpu.roll(cur, tall + 15, 0)
                total = across_columns(cur, total)
                new = total * (inside * (r_scale[side] * scale))
                if k > 1:
                    new = new - halo[c, k - 2, side, i]
                halo[c, k, side, i] = new
            return carry

        lax.fori_loop(1, reach + 1, extend_row, 0, unroll=True)

    def extend_planes(c, k, reach):
        scale = first_scale if k == 1 else next_scale

        def extend_plane(e, carry):
            for up in range(2):
                z = tall - 1 + e if up else -e
                at = DEEP + z
                cur = X[c, k - 1, at]
                total = X[c, k - 1, at - 1] + X[c, k - 1, at + 1]
                low = halo[c, k - 1, 0, 1, pl.ds(8 + z, 1), :]
                high = halo[c, k - 1, 1, 1, pl.ds(8 + z, 1), :]
                total = neighbours(cur, total, low, high)
                new = total * (z_scale[up] * scale)
                if k > 1:
                    new = new - X[c, k - 2, at]
                X[c, k, at] = new
                if reach > 1:
                    put_row(c, k, z, new)
            return carry

        lax.fori_loop(1, reach + 1, extend_plane, 0, unroll=True)

    def names_of(c, k):
        if c == 0:
            names = [(dd(k, 0), "new", "new"), (dd(k - 1, 1), "new", "cur")]
            if k == 1:
                names.append((dd(0, 0), "cur", "cur"))
        else:
            names = [(rr(k, 0), "new", "new"), (rr(k - 1, 1), "new", "cur"),
                     (dr(k, 0), "new", "other"), (dr(k - 1, 1), "cur", "other")]
            if k == S - 1:
                names.append((dr(k, 1), "new", "ahead"))
            if k == 1:
                names += [(rr(0, 0), "cur", "cur"), (dr(0, 0), "cur", "start")]
        return names

    def sent(c, k):
        return k == FIRST[c]

    def plane(c, k, z, sums, reach):
        at = z + DEEP
        cur = X[c, k - 1, at]
        total = X[c, k - 1, at - 1] + X[c, k - 1, at + 1]
        low = halo[c, k - 1, 0, 1, pl.ds(8 + z, 1), :]
        high = halo[c, k - 1, 1, 1, pl.ds(8 + z, 1), :]
        total = neighbours(cur, total, low, high)
        if k == 1:
            new = total * first_scale
        else:
            new = total * next_scale - X[c, k - 2, at]
        X[c, k, at] = new
        if sent(c, k):
            put_rows(c, k, z, new)
        elif reach > 1:
            put_row(c, k, z, new)
        return products(c, k, z, sums, new, cur) if sums else sums

    def products(c, k, z, sums, new, cur):
        names = names_of(c, k)
        at = z + DEEP
        have = {"new": new, "cur": cur}
        if any("other" in n for n in names):
            have["other"] = X[0, k, at]
        if any("ahead" in n for n in names):
            have["ahead"] = X[0, k + 1, at]
        if any("start" in n for n in names):
            have["start"] = X[0, 0, at]
        return tuple(s + folded(have[l] * have[r]) for s, (_, l, r) in zip(sums, names))

    def all_products(c, k):
        def body(z, sums):
            return products(c, k, z, sums, X[c, k, z + DEEP], X[c, k - 1, z + DEEP])
        return lax.fori_loop(0, tall, body, zero_sums(c, k), unroll=4)

    def put_rows(c, k, z, new):
        put_row(c, k, z, new)
        at = pl.ds(z, 1)
        for i in range(deep(c, k)):
            stage[c, min(k, 1), 0, i, at, :] = new[i:i + 1]
            stage[c, min(k, 1), 1, i, at, :] = new[rows - 1 - i:rows - i]

    def zero_sums(c, k):
        return tuple(jnp.zeros((8, LANES), jnp.float32) for _ in names_of(c, k))

    def keep(c, k, sums):
        for s, (slot, _, _) in zip(sums, names_of(c, k)):
            accs[slot] = s

    def ends(c, k, width_of, sums, reach):
        def body(i, sums):
            return plane(c, k, i + (i // width_of) * (tall - 2 * width_of), sums, reach)
        return lax.fori_loop(0, 2 * width_of, body, sums, unroll=True)

    def middle(c, k, width_of, sums, reach):
        length = tall - 2 * width_of
        unroll = max(u for u in range(1, UNROLL + 1) if length % u == 0)
        return lax.fori_loop(width_of, tall - width_of, lambda z, s: plane(c, k, z, s, reach), sums, unroll=unroll)

    def chain_round(c, k):
        d = deep(c, k)
        outer = c == 1 and k == 0 and 2 * (d + 1) < tall
        receive_rows(c, k)
        inner = middle(c, k + 1, 1, () if outer else zero_sums(c, k + 1), d - 1)
        receive_planes(c, k)
        settle(c, k)
        sums = []
        for m in range(1, d + 1):
            n, reach = k + m, d - m
            if reach:
                extend_rows(c, n, reach)
                extend_planes(c, n, reach)
            if m == 1:
                sums.append(ends(c, n, 1, inner, reach))
            elif outer:
                ends(c, n, 2 + reach, (), reach)
            else:
                sums.append(middle(c, n, 0, zero_sums(c, n), reach))
        if sent(c, k + d):
            send_z(c, k + d)
            if outer:
                send_edges(c, k + d)
        if outer:
            for m in range(2, d + 1):
                n, reach = k + m, d - m
                if m > 2 and reach:
                    extend_rows(c, n, reach)
                middle(c, n, 2 + reach, (), reach)
        if sent(c, k + d):
            send_rows(c, k + d)
            if not outer:
                send_edges(c, k + d)
        for m in range(1, d + 1):
            keep(c, k + m, all_products(c, k + m) if outer else sums[m - 1])

    def arrive(c):
        own_in(c).wait()
        others = held.at[c, :, pl.ds(0, width - rows), :]
        pltpu.make_async_copy(others, others, in_recv.at[c]).wait()
        send_z(c, 0)

        def copy_rows(z, carry):
            put_rows(c, 0, z, X[c, 0, z + DEEP])
            return carry
        lax.fori_loop(0, tall, copy_rows, 0, unroll=4)
        send_edges(c, 0)
        send_rows(c, 0)

    arrive(0)
    arrive(1)
    for h in range(2):
        for c in range(2):
            chain_round(c, h * FIRST[c])

    lanes = lax.broadcasted_iota(jnp.int32, (8, LANES), 1)
    packed = jnp.zeros((8, LANES), jnp.float32)
    for t in range(COUNT // 8):
        part = jnp.sum(jnp.sum(accs[8 * t:8 * t + 8], axis=1), axis=1, keepdims=True)
        packed = packed + jnp.where(lanes == t, part, 0.0)
    red[me] = jnp.sum(pltpu.roll(packed, 0, 1, stride=8, stride_axis=0), axis=0, keepdims=True)

    far = 2 * ((2 * g) // groups) - 1

    def moments_to(j):
        t = (me + far * j + count) % count
        return pltpu.make_async_remote_copy(
            src_ref=red.at[me], dst_ref=red.at[me], send_sem=a_send.at[0], recv_sem=a_recv.at[0],
            device_id=(t // ga, t % ga), device_id_type=MESH)

    def start_moments(j, carry):
        moments_to(j).start()
        return carry

    lax.fori_loop(1, count, start_moments, 0, unroll=count <= 64)
    def drained(ref, sem):
        pltpu.make_async_copy(ref, ref, sem).wait()

    drained(held.at[:, :, pl.ds(0, width - rows), :], in_send.at[0])
    for up in range(2):
        @pl.when(z_there[up])
        def _():
            drained(X.at[0, pl.ds(0, 5), pl.ds(0, 3)], z_send.at[up])

        @pl.when(r_there[up])
        def _():
            drained(halo.at[0, pl.ds(0, 3), 0, pl.ds(0, 5), pl.ds(8, tall)], r_send.at[up])

        for side in range(2):
            @pl.when(z_there[up] & r_there[side])
            def _():
                for c, k in exchanges:
                    e_copy(c, k, up, side).wait_send()
    others = red.at[pl.ds(0, count - 1)]
    drained(others, a_recv.at[0])
    total = jnp.sum(red[...], axis=0)

    loads[2].wait()
    gram = jnp.zeros((SIDE, LANES), jnp.float32)
    moved = jnp.zeros((SIDE, LANES), jnp.float32)
    for e in range(COUNT):
        at = 8 * (e % 8) + e // 8
        value = total[0:1, at:at + 1]
        gram = gram + value * table[e]
        moved = moved + value * table[COUNT + e]
    change, change_t = table[2 * COUNT], table[2 * COUNT + 1]

    def unit(axis, at):
        ids = lax.broadcasted_iota(jnp.int32, (SIDE, LANES), axis)
        return jnp.where(ids == at, 1.0, 0.0).astype(jnp.float32)

    def down(x):
        return jnp.sum(x, axis=0, keepdims=True)

    def across(x):
        return jnp.sum(x, axis=1, keepdims=True)

    def advance(state):
        qc, qr, wc, wr, it, uc, rho = state
        mc = across(change * qr)
        gc = across(moved * qr)
        mr = down(change_t * qc)
        alpha = rho / down(qc * gc)
        it = it + alpha * qc
        wc = wc - alpha * mc
        wr = wr - alpha * mr
        uc = uc - alpha * gc
        rho_new = down(wc * uc)
        return wc, wr, it, uc, rho_new, rho_new / rho

    def inner(_, state):
        wc, wr, it, uc, rho, beta = advance(state)
        return wc + beta * state[0], wr + beta * state[1], wc, wr, it, uc, rho

    wc, wr = unit(0, S + 1), unit(1, S + 1)
    start = across(gram * wr) + jnp.zeros((SIDE, LANES), jnp.float32)
    state = (unit(0, 0), unit(1, 0), wc, wr, jnp.zeros((SIDE, LANES), jnp.float32), start, down(wc * start))
    state = lax.fori_loop(0, S - 1, inner, state)
    _, _, it, _, _, beta = advance(state)
    coef[0] = it
    coef[1] = state[0]
    beta_ref[...] = jnp.zeros((8, LANES), jnp.float32) + beta

    tile = 16 if rows % 16 == 0 else 8

    def combine(o, start, out, height):
        def strip(s, carry):
            i, part = s // (rows // tile), s % (rows // tile)
            at = pl.ds(pl.multiple_of(part * tile, tile), tile)
            total = None
            for v in range(2 * S - 1):
                c, k = (0, v) if v < S else (1, v - S)
                row = v if v < S else v + 1
                f = coef[o, row:row + 1, :]
                f = jnp.concatenate([f] * (depth // LANES), axis=1)
                term = f * X[c, k, start + i, at, :]
                total = term if total is None else total + term
            out[i, at, :] = total
            return carry
        lax.fori_loop(0, height * (rows // tile), strip, 0, unroll=2)

    def combine_dx(q):
        combine(0, planes * q + DEEP - 1 + q % 2, out_dx.at[q], planes + 1)

    def combine_q(q):
        combine(1, planes * q + DEEP, out_q.at[q], planes)

    odd = p % 2

    def outgoing_dx(j):
        q = flipped(p, j, group)
        return pltpu.make_async_remote_copy(
            src_ref=out_dx.at[q], dst_ref=dx.at[pl.ds(q % 2, planes + 1), block_rows(b), :],
            send_sem=o_send.at[0], recv_sem=o_recv.at[j],
            device_id=device(g, q), device_id_type=MESH)

    def outgoing_q(j):
        q = flipped(p, j, group)
        return pltpu.make_async_remote_copy(
            src_ref=out_q.at[q], dst_ref=last.at[:, block_rows(b), :],
            send_sem=q_send.at[0], recv_sem=q_recv.at[0],
            device_id=device(g, q), device_id_type=MESH)

    def source_of(j):
        return flipped(p, j, group) if group & (group - 1) == 0 else (p + group - j) % group

    def dx_from(j):
        at = block_rows(place(source_of(j)))
        return pltpu.make_async_remote_copy(
            src_ref=out_dx.at[p], dst_ref=dx.at[pl.ds(odd, planes + 1), at, :],
            send_sem=o_send.at[0], recv_sem=o_recv.at[j],
            device_id=device(g, source_of(j)), device_id_type=MESH)

    mate = p + 1 - 2 * odd

    def forward_of(block):
        at = block_rows(block)
        return pltpu.make_async_remote_copy(
            src_ref=dx.at[planes - odd * (planes - 1), at, :],
            dst_ref=dx.at[odd * (planes + 1), at, :],
            send_sem=f_send.at[0], recv_sem=f_recv.at[0],
            device_id=device(g, mate), device_id_type=MESH)

    for j in order:
        combine_dx(flipped(p, j, group))
        outgoing_dx(j).start()
    combine_dx(p)
    own = pltpu.make_async_copy(out_dx.at[p], dx.at[pl.ds(odd, planes + 1), block_rows(b), :], own_sem.at[2])
    own.start()
    for j in order:
        combine_q(flipped(p, j, group))
        outgoing_q(j).start()
    combine_q(p)
    own_q = pltpu.make_async_copy(out_q.at[p], last.at[:, block_rows(b), :], own_sem.at[3])
    own_q.start()
    own.wait()
    forward_of(b).start()
    for j in [order[-1]] + order[:-1]:
        dx_from(j).wait_recv()
        forward_of(place(source_of(j))).start()
    own_q.wait()
    drained(dx.at[0], f_recv.at[0])
    drained(others, a_send.at[0])
    drained(out_dx.at[pl.ds(0, group - 1)], o_send.at[0])
    drained(dx.at[0], f_send.at[0])
    loads[3].wait()

    piece = width // PIECES
    for i in range(planes):
        for t in range(PIECES):
            at = pl.ds(t * piece, piece)
            cur = dx[i + 1, at, :]
            none = jnp.zeros((1, depth), jnp.float32)
            low = dx[i + 1, t * piece - 1:t * piece, :] if t else none
            high = dx[i + 1, (t + 1) * piece:(t + 1) * piece + 1, :] if t < PIECES - 1 else none
            total = neighbours(cur, dx[i, at, :] + dx[i + 2, at, :], low, high)
            sol_out[i, at, :] = sol_in[i, at, :] + cur
            res_out[i, at, :] = held[1, i, at, :] - (6.0 * cur - total)
    drained(last.at[:, pl.ds(0, width - rows), :], q_recv.at[0])
    drained(last.at[:, pl.ds(0, width - rows), :], q_send.at[0])


def finish(sol, res, last, beta, sol_out, res_out, dir_out, buf, sem):
    planes, width, depth = sol.shape
    piece = width // PIECES
    factor = jnp.concatenate([beta[0:1, :]] * (depth // LANES), axis=1)
    copies = [pltpu.make_async_copy(source, target, sem.at[i])
              for i, (source, target) in enumerate(((sol, sol_out), (res, res_out)))]
    for copy in copies:
        copy.start()
    for i in range(planes):
        for s in range(PIECES):
            at = pl.ds(s * piece, piece)
            buf[i, at, :] = res[i, at, :] + factor * last[i, at, :]
        copies.append(pltpu.make_async_copy(buf.at[i], dir_out.at[i], sem.at[2 + i]))
        copies[-1].start()
    for copy in copies:
        copy.wait()


def on_device(gz_count, ga, sol, res, direction):
    planes, width, depth = sol.shape
    group, groups = 2 * ga, gz_count // 2
    tall, rows = planes * group, width // group
    table = jnp.asarray(np.concatenate(gram_tables()))
    vmem = pl.BlockSpec(memory_space=pltpu.VMEM)
    dma = pltpu.SemaphoreType.DMA
    anywhere = pl.BlockSpec(memory_space=pltpu.HBM)
    f32 = jnp.float32
    outs = pl.pallas_call(
        functools.partial(kernel, gz_count, ga),
        out_shape=[pltpu.VMEM(sol.shape, f32)] * 3 + [pltpu.VMEM((8, LANES), f32)],
        in_specs=[anywhere] * 4,
        out_specs=[vmem] * 4,
        scratch_shapes=[
            pltpu.VMEM((2, S + 1, tall + 2 * DEEP, rows, depth), f32),
            pltpu.VMEM((2, S, 2, DEEP + 1, tall + 16, depth), f32),
            pltpu.VMEM((2, 2, 2, DEEP, tall, depth), f32),
            pltpu.VMEM((2, 2, FIRST[1] - 1, 4, depth), f32),
            pltpu.VMEM((2, 2, FIRST[1] - 1, 4, depth), f32),
            pltpu.VMEM((2, 2, 2, 1, 1, depth), f32),
            pltpu.VMEM((2, 2, 2, 1, 1, depth), f32),
            pltpu.VMEM((COUNT, 8, LANES), f32),
            pltpu.VMEM((gz_count * ga, 1, LANES), f32),
            pltpu.VMEM((2, SIDE, LANES), f32),
            pltpu.VMEM((planes + 2, width, depth), f32),
            pltpu.VMEM((group, planes + 1, rows, depth), f32),
            pltpu.VMEM((group, planes, rows, depth), f32),
            pltpu.VMEM((2, planes, width, depth), f32),
            pltpu.VMEM(sol.shape, f32),
            pltpu.VMEM((2 * COUNT + 2, SIDE, LANES), f32),
            dma((1,)), dma((2,)), dma((4,)),
            dma((2,)), dma((2, 2, 2)), dma((2,)), dma((2, 2, 2)),
            dma((2, 2, 2, 2)), dma((2, 2, 2, 2)),
            dma((1,)), dma((1,)),
            dma((1,)), dma((group,)), dma((1,)), dma((1,)), dma((1,)), dma((1,)),
            dma((4,)),
        ],
        compiler_params=pltpu.CompilerParams(collective_id=0, has_side_effects=True, vmem_limit_bytes=VMEM_LIMIT),
    )(*(pltpu.with_memory_space_constraint(x, pltpu.HBM) for x in (res, direction, table, sol)))
    shape = jax.ShapeDtypeStruct(sol.shape, f32)
    return pl.pallas_call(
        finish,
        out_shape=[shape] * 3,
        in_specs=[vmem] * 4,
        out_specs=[anywhere] * 3,
        scratch_shapes=[pltpu.VMEM(sol.shape, f32), dma((2 + planes,))],
        compiler_params=pltpu.CompilerParams(vmem_limit_bytes=8 * 2 ** 20),
    )(*outs)


def solution(mesh):
    spec = P(("gz", "ga"), None, None)
    return jax.shard_map(
        functools.partial(on_device, mesh.shape["gz"], mesh.shape["ga"]),
        mesh=mesh, in_specs=(spec, spec, spec), out_specs=(spec, spec, spec), check_vma=False,
    )
```

```python
import functools

import jax
import jax.numpy as jnp
import numpy as np
from jax import lax
from jax.experimental import pallas as pl
from jax.experimental.pallas import tpu as pltpu
from jax.sharding import PartitionSpec as P

S = 8
MESH = pl.DeviceIdType.MESH
first_scale = -1.0 / 6.0
next_scale = -1.0 / 3.0
SIDE = 24
LANES = 128
FIRST = (S - 2, S - 3)
DEEP = max(FIRST)
UNROLL = 16
PIECES = 4
VMEM_LIMIT = 44 * 2 ** 20


def change_matrix(steps):
    count = 2 * steps + 1
    table = np.zeros((count, count), np.float64)
    for offset, length in ((0, steps + 1), (steps + 1, steps)):
        for power in range(length - 1):
            column = offset + power
            table[column, column] = 6.0
            if power == 0:
                table[column + 1, column] = 6.0
            else:
                table[column + 1, column] = 3.0
                table[column - 1, column] = 3.0
    return table


def dd(power, odd):
    return 2 * power + odd


def rr(power, odd):
    return 2 * S + 1 + 2 * power + odd


def dr(power, odd):
    return 4 * S + 2 * power + odd


COUNT = 6 * S


def gram_tables():
    def moment(kind, order):
        half, odd = order // 2, order % 2
        row = np.zeros(COUNT)
        row[kind(half, odd)] += 2.0
        row[kind(0, odd)] -= 1.0
        return row

    size = 2 * S + 1
    table = np.zeros((COUNT, size, size))
    for i in range(size):
        for j in range(size):
            a, b = (i if i <= S else i - S - 1), (j if j <= S else j - S - 1)
            kind = dd if (i <= S and j <= S) else rr if (i > S and j > S) else dr
            table[:, i, j] = 0.5 * (moment(kind, a + b) + moment(kind, abs(a - b)))
    moved = table @ change_matrix(S)

    def padded(t):
        out = np.zeros((t.shape[0], SIDE, LANES), np.float32)
        out[:, :size, :size] = t
        return out

    change = np.stack([change_matrix(S), change_matrix(S).T])
    return padded(table), padded(moved), padded(change)


def flipped(p, bits, group):
    if group & (group - 1):
        return (p + bits) % group
    out, step = p, 1
    while step < group:
        if bits & step:
            out = out + step * (1 - 2 * ((p // step) % 2))
        step *= 2
    return out


def send_order(group):
    if group & (group - 1):
        return list(range(1, group))
    first = [j for j in range(2, group) if (j // 2) & (j // 2 - 1) == 0]
    first = first[::2] + first[1::2]
    return first + [j for j in range(2, group) if j not in first] + [1]


def neighbours(cur, total, low, high):
    height = cur.shape[0]
    total = total + jnp.concatenate([low, cur[:height - 1]], axis=0)
    total = total + jnp.concatenate([cur[1:], high], axis=0)
    return across_columns(cur, total)


def across_columns(cur, total):
    none = jnp.zeros((cur.shape[0], 1), jnp.float32)
    total = total + jnp.concatenate([none, cur[:, :cur.shape[1] - 1]], axis=1)
    return total + jnp.concatenate([cur[:, 1:], none], axis=1)


def kernel(gz_count, ga, res_ref, dir_ref, table_hbm, sol_ref,
           sol_out, res_out, last, beta_ref,
           X, halo, stage, edge, edge_in, edge_0, edge_0_in, edge_1, edge_1_in, accs, red, coef, dx, out_dx, out_q, held, sol_in, table,
           in_send, in_recv, own_sem, z_send, z_recv, r_send, r_recv, e_send, e_recv,
           a_send, a_recv, o_send, o_recv, q_send, q_recv, f_send, f_recv, load_sem):
    group = 2 * ga
    groups = gz_count // 2
    count = gz_count * ga
    planes, width, depth = res_ref.shape
    tall = planes * group
    rows = width // group
    iz, ia = lax.axis_index("gz"), lax.axis_index("ga")
    me = iz * ga + ia
    g = iz // 2
    p = (iz % 2) * ga + ia
    order = send_order(group)

    def place(position):
        upper = position // ga
        return upper * (3 * ga - 1 - position) + (1 - upper) * position

    b = place(p)

    def device(which, position):
        return (which * 2 + position // ga, position % ga)

    def block_rows(block):
        return pl.ds(pl.multiple_of(block * rows, rows), rows)

    loads = [pltpu.make_async_copy(source, target, load_sem.at[i]) for i, (source, target) in enumerate((
        (dir_ref, held.at[0]), (res_ref, held.at[1]), (table_hbm, table), (sol_ref, sol_in)))]
    for load in loads:
        load.start()

    below, above = g > 0, g < groups - 1
    before, after = b > 0, b < group - 1
    z_there, r_there = (below, above), (before, after)

    barrier = pltpu.get_barrier_semaphore()

    def greet(target):
        pl.semaphore_signal(barrier, inc=1, device_id=target, device_id_type=MESH)

    if groups - 1 <= 3:
        for j in range(1, group):
            greet(device(g, flipped(p, j, group)))
        for up in range(2):
            @pl.when(z_there[up])
            def _():
                greet(device(g + 2 * up - 1, p))
            for side in range(2):
                @pl.when(z_there[up] & r_there[side])
                def _():
                    greet(device(g + 2 * up - 1, place(b + 2 * side - 1)))
        below_1, above_1 = jnp.minimum(g, 1), jnp.minimum(groups - 1 - g, 1)
        before_1, after_1 = jnp.minimum(b, 1), jnp.minimum(group - 1 - b, 1)
        pl.semaphore_wait(barrier, group - 1 + (below_1 + above_1) * (1 + before_1 + after_1))
    else:
        def greet_all(j, carry):
            t = (me + j) % count
            greet((t // ga, t % ga))
            return carry
        lax.fori_loop(1, count, greet_all, 0)
        pl.semaphore_wait(barrier, count - 1)

    def incoming(c, j):
        q = flipped(p, j, group)
        return pltpu.make_async_remote_copy(
            src_ref=held.at[c, :, block_rows(place(q)), :],
            dst_ref=X.at[c, 0, pl.ds(DEEP + planes * p, planes)],
            send_sem=in_send.at[0], recv_sem=in_recv.at[c],
            device_id=device(g, q), device_id_type=MESH)

    def own_in(c):
        return pltpu.make_async_copy(
            held.at[c, :, block_rows(b), :],
            X.at[c, 0, pl.ds(DEEP + planes * p, planes)], own_sem.at[c])

    loads[0].wait()
    for j in order:
        incoming(0, j).start()
    own_in(0).start()
    loads[1].wait()
    for j in order:
        incoming(1, j).start()
    own_in(1).start()

    def deep(c, k):
        return 2 if k else FIRST[c]

    def spread(c, k):
        return 1 if k else 4 if deep(c, k) < 6 else 8

    def drained(ref, sem):
        pltpu.make_async_copy(ref, ref, sem).wait()

    exchanges = [(c, k) for c in range(2) for k in (0, FIRST[c])]

    def parts(c, k):
        return range(2 if spread(c, k) == 8 else 1)

    def edges_of(c, k, incoming_side, up, side, part=0):
        if k:
            return (edge_1_in if incoming_side else edge_1).at[c, up, side]
        if spread(c, k) == 4:
            return (edge_in if incoming_side else edge).at[up, side, pl.ds(0, deep(c, k) - 1)]
        if part:
            return (edge_0_in if incoming_side else edge_0).at[up, side]
        if incoming_side:
            return halo.at[c, k, side, pl.ds(1, 1), pl.ds(up * (tall + 8), 8)]
        return stage.at[c, 0, side, pl.ds(0, 1), pl.ds(up * (tall - 8), 8)]

    for c, k in exchanges:
        d = deep(c, k)
        for missing, at in ((g == 0, DEEP - d), (g == groups - 1, tall + DEEP)):
            @pl.when(missing)
            def _():
                X[c, k, at:at + d] = jnp.zeros((d, rows, depth), jnp.float32)
        for side, missing in ((0, b == 0), (1, b == group - 1)):
            @pl.when(missing)
            def _():
                halo[c, k, side, 1:d + 1] = jnp.zeros((d, tall + 16, depth), jnp.float32)
        for up in range(2):
            for side in range(2):
                @pl.when(jnp.logical_not(z_there[up] & r_there[side]))
                def _():
                    for part in parts(c, k):
                        ref = edges_of(c, k, True, up, side, part)
                        ref[...] = jnp.zeros(ref.shape, jnp.float32)

    def z_copy(c, k, up):
        d = deep(c, k)
        source = DEEP + tall - d if up else DEEP
        target = DEEP - d if up else tall + DEEP
        return pltpu.make_async_remote_copy(
            src_ref=X.at[c, k, pl.ds(source, d)],
            dst_ref=X.at[c, k, pl.ds(target, d)],
            send_sem=z_send.at[up], recv_sem=z_recv.at[c, min(k, 1), up],
            device_id=device(g + 2 * up - 1, p), device_id_type=MESH)

    def r_copy(c, k, up):
        d = deep(c, k)
        return pltpu.make_async_remote_copy(
            src_ref=stage.at[c, min(k, 1), up, pl.ds(0, d)],
            dst_ref=halo.at[c, k, 1 - up, pl.ds(1, d), pl.ds(8, tall)],
            send_sem=r_send.at[up], recv_sem=r_recv.at[c, min(k, 1), up],
            device_id=device(g, place(b + 2 * up - 1)), device_id_type=MESH)

    def e_copy(c, k, up, side, part=0):
        h = min(k, 1)
        return pltpu.make_async_remote_copy(
            src_ref=edges_of(c, k, False, up, side, part),
            dst_ref=edges_of(c, k, True, 1 - up, 1 - side, part),
            send_sem=e_send.at[c, h, up, side], recv_sem=e_recv.at[c, h, 1 - up, 1 - side],
            device_id=device(g + 2 * up - 1, place(b + 2 * side - 1)), device_id_type=MESH)

    def e_arrival(c, k, up, side):
        h = min(k, 1)
        return pltpu.make_async_remote_copy(
            src_ref=edges_of(c, k, False, up, side),
            dst_ref=edges_of(c, k, True, up, side),
            send_sem=e_send.at[c, h, up, side], recv_sem=e_recv.at[c, h, up, side],
            device_id=device(g + 2 * up - 1, place(b + 2 * side - 1)), device_id_type=MESH)

    def whole_edge(c, k):
        return held.at[0, 0, pl.ds(0, 8 + 4 * (deep(c, k) - 2))]

    def edge_arrived(c, k, up, side):
        if spread(c, k) == 8:
            drained(whole_edge(c, k), e_recv.at[c, min(k, 1), up, side])
        else:
            e_arrival(c, k, up, side).wait_recv()

    def edge_left(c, k, up, side):
        if spread(c, k) == 8:
            drained(whole_edge(c, k), e_send.at[c, min(k, 1), up, side])
        else:
            e_copy(c, k, up, side).wait_send()

    def send_z(c, k):
        for up in range(2):
            @pl.when(z_there[up])
            def _():
                z_copy(c, k, up).start()

    def send_edges(c, k):
        n = spread(c, k)
        if n < 8:
            for up in range(2):
                for side in range(2):
                    ref = edges_of(c, k, False, up, side)
                    for i in range(deep(c, k) - 1):
                        if n == 1:
                            row = (rows - 1) * side
                            ref[i] = X[c, k, DEEP + (tall - 1) * up, row:row + 1, :]
                        else:
                            ref[i] = stage[c, 0, side, i, up * (tall - n):up * (tall - n) + n, :]
        else:
            for up in range(2):
                for side in range(2):
                    for i in range(1, deep(c, k) - 1):
                        edge_0[up, side, i - 1] = stage[c, 0, side, i, up * (tall - 4):up * (tall - 4) + 4, :]
        for up in range(2):
            for side in range(2):
                @pl.when(z_there[up] & r_there[side])
                def _():
                    for part in parts(c, k):
                        e_copy(c, k, up, side, part).start()

    def send_rows(c, k):
        for side in range(2):
            @pl.when(r_there[side])
            def _():
                r_copy(c, k, side).start()

    def receive_rows(c, k):
        for side in range(2):
            @pl.when(r_there[side])
            def _():
                r_copy(c, k, 1 - side).wait_recv()

    def receive_planes(c, k):
        for up in range(2):
            for side in range(2):
                @pl.when(z_there[up] & r_there[side])
                def _():
                    edge_arrived(c, k, up, side)

            @pl.when(z_there[up])
            def _():
                z_copy(c, k, 1 - up).wait_recv()

    def folded(x):
        total = x[0:8]
        for i in range(8, rows, 8):
            total = total + x[i:i + 8]
        out = total[:, 0:LANES]
        for i in range(LANES, depth, LANES):
            out = out + total[:, i:i + LANES]
        return out

    z_scale = [jnp.minimum(g, 1).astype(jnp.float32), jnp.minimum(groups - 1 - g, 1).astype(jnp.float32)]
    r_scale = [jnp.minimum(b, 1).astype(jnp.float32), jnp.minimum(group - 1 - b, 1).astype(jnp.float32)]

    plane_ids = lax.broadcasted_iota(jnp.int32, (tall + 16, depth), 0)
    inside = (jnp.where(plane_ids < 8, z_scale[0], 1.0) * jnp.where(plane_ids >= tall + 8, z_scale[1], 1.0))

    def settle(c, k):
        n = spread(c, k)
        if n < 8:
            for up in range(2):
                at = tall + 8 if up else 8 - n
                for side in range(2):
                    ref = edges_of(c, k, True, up, side)
                    for i in range(deep(c, k) - 1):
                        halo[c, k, side, i + 1, at:at + n, :] = ref[i]
        else:
            for up in range(2):
                at = tall + 8 if up else 4
                for side in range(2):
                    for i in range(1, deep(c, k) - 1):
                        halo[c, k, side, i + 1, at:at + 4, :] = edge_0_in[up, side, i - 1]
        for e in range(1, deep(c, k)):
            for up in range(2):
                at = tall - 1 + e if up else -e
                put_row(c, k, at, X[c, k, DEEP + at])

    def put_row(c, k, z, new):
        at = pl.ds(8 + z, 1)
        halo[c, k, 0, 0, at, :] = new[0:1]
        halo[c, k, 1, 0, at, :] = new[rows - 1:rows]

    def extend_rows(c, k, reach):
        scale = first_scale if k == 1 else next_scale

        def extend_row(i, carry):
            for side in range(2):
                cur = halo[c, k - 1, side, i]
                total = halo[c, k - 1, side, i - 1] + halo[c, k - 1, side, i + 1]
                total = total + pltpu.roll(cur, 1, 0) + pltpu.roll(cur, tall + 15, 0)
                total = across_columns(cur, total)
                new = total * (inside * (r_scale[side] * scale))
                if k > 1:
                    new = new - halo[c, k - 2, side, i]
                halo[c, k, side, i] = new
            return carry

        lax.fori_loop(1, reach + 1, extend_row, 0, unroll=True)

    def extend_planes(c, k, reach):
        scale = first_scale if k == 1 else next_scale

        def extend_plane(e, carry):
            for up in range(2):
                z = tall - 1 + e if up else -e
                at = DEEP + z
                cur = X[c, k - 1, at]
                total = X[c, k - 1, at - 1] + X[c, k - 1, at + 1]
                low = halo[c, k - 1, 0, 1, pl.ds(8 + z, 1), :]
                high = halo[c, k - 1, 1, 1, pl.ds(8 + z, 1), :]
                total = neighbours(cur, total, low, high)
                new = total * (z_scale[up] * scale)
                if k > 1:
                    new = new - X[c, k - 2, at]
                X[c, k, at] = new
                if reach > 1:
                    put_row(c, k, z, new)
            return carry

        lax.fori_loop(1, reach + 1, extend_plane, 0, unroll=True)

    def names_of(c, k):
        if c == 0:
            names = [(dd(k, 0), "new", "new"), (dd(k - 1, 1), "new", "cur")]
            if k == 1:
                names.append((dd(0, 0), "cur", "cur"))
        else:
            names = [(rr(k, 0), "new", "new"), (rr(k - 1, 1), "new", "cur"),
                     (dr(k, 0), "new", "other"), (dr(k - 1, 1), "cur", "other")]
            if k == S - 1:
                names.append((dr(k, 1), "new", "ahead"))
            if k == 1:
                names += [(rr(0, 0), "cur", "cur"), (dr(0, 0), "cur", "start")]
        return names

    def sent(c, k):
        return k == FIRST[c]

    def plane(c, k, z, sums, reach):
        at = z + DEEP
        cur = X[c, k - 1, at]
        total = X[c, k - 1, at - 1] + X[c, k - 1, at + 1]
        low = halo[c, k - 1, 0, 1, pl.ds(8 + z, 1), :]
        high = halo[c, k - 1, 1, 1, pl.ds(8 + z, 1), :]
        total = neighbours(cur, total, low, high)
        if k == 1:
            new = total * first_scale
        else:
            new = total * next_scale - X[c, k - 2, at]
        X[c, k, at] = new
        if sent(c, k):
            put_rows(c, k, z, new)
        elif reach > 1:
            put_row(c, k, z, new)
        return products(c, k, z, sums, new, cur) if sums else sums

    def products(c, k, z, sums, new, cur):
        names = names_of(c, k)
        at = z + DEEP
        have = {"new": new, "cur": cur}
        if any("other" in n for n in names):
            have["other"] = X[0, k, at]
        if any("ahead" in n for n in names):
            have["ahead"] = X[0, k + 1, at]
        if any("start" in n for n in names):
            have["start"] = X[0, 0, at]
        return tuple(s + folded(have[l] * have[r]) for s, (_, l, r) in zip(sums, names))

    def all_products(c, k):
        def body(z, sums):
            return products(c, k, z, sums, X[c, k, z + DEEP], X[c, k - 1, z + DEEP])
        return lax.fori_loop(0, tall, body, zero_sums(c, k), unroll=4)

    def put_rows(c, k, z, new):
        put_row(c, k, z, new)
        at = pl.ds(z, 1)
        for i in range(deep(c, k)):
            stage[c, min(k, 1), 0, i, at, :] = new[i:i + 1]
            stage[c, min(k, 1), 1, i, at, :] = new[rows - 1 - i:rows - i]

    def zero_sums(c, k):
        return tuple(jnp.zeros((8, LANES), jnp.float32) for _ in names_of(c, k))

    def keep(c, k, sums):
        for s, (slot, _, _) in zip(sums, names_of(c, k)):
            accs[slot] = s

    def ends(c, k, width_of, sums, reach):
        def body(i, sums):
            return plane(c, k, i + (i // width_of) * (tall - 2 * width_of), sums, reach)
        return lax.fori_loop(0, 2 * width_of, body, sums, unroll=True)

    def middle(c, k, width_of, sums, reach):
        length = tall - 2 * width_of
        unroll = max(u for u in range(1, UNROLL + 1) if length % u == 0)
        return lax.fori_loop(width_of, tall - width_of, lambda z, s: plane(c, k, z, s, reach), sums, unroll=unroll)

    def chain_round(c, k):
        d = deep(c, k)
        outer = c == 1 and k == 0 and 2 * (d + 1) < tall
        receive_rows(c, k)
        inner = middle(c, k + 1, 1, () if outer else zero_sums(c, k + 1), d - 1)
        receive_planes(c, k)
        settle(c, k)
        sums = []
        for m in range(1, d + 1):
            n, reach = k + m, d - m
            if reach:
                extend_rows(c, n, reach)
                extend_planes(c, n, reach)
            if m == 1:
                sums.append(ends(c, n, 1, inner, reach))
            elif outer:
                ends(c, n, 2 + reach, (), reach)
            else:
                sums.append(middle(c, n, 0, zero_sums(c, n), reach))
        if sent(c, k + d):
            send_z(c, k + d)
            if outer:
                send_edges(c, k + d)
        if outer:
            for m in range(2, d + 1):
                n, reach = k + m, d - m
                if m > 2 and reach:
                    extend_rows(c, n, reach)
                middle(c, n, 2 + reach, (), reach)
        if sent(c, k + d):
            send_rows(c, k + d)
            if not outer:
                send_edges(c, k + d)
        for m in range(1, d + 1):
            keep(c, k + m, all_products(c, k + m) if outer else sums[m - 1])

    def arrive(c):
        own_in(c).wait()
        others = held.at[c, :, pl.ds(0, width - rows), :]
        pltpu.make_async_copy(others, others, in_recv.at[c]).wait()
        send_z(c, 0)

        def copy_rows(z, carry):
            put_rows(c, 0, z, X[c, 0, z + DEEP])
            return carry
        lax.fori_loop(0, tall, copy_rows, 0, unroll=4)
        send_edges(c, 0)
        send_rows(c, 0)

    arrive(0)
    arrive(1)
    for h in range(2):
        for c in range(2):
            chain_round(c, h * FIRST[c])

    lanes = lax.broadcasted_iota(jnp.int32, (8, LANES), 1)
    packed = jnp.zeros((8, LANES), jnp.float32)
    for t in range(COUNT // 8):
        part = jnp.sum(jnp.sum(accs[8 * t:8 * t + 8], axis=1), axis=1, keepdims=True)
        packed = packed + jnp.where(lanes == t, part, 0.0)
    red[me] = jnp.sum(pltpu.roll(packed, 0, 1, stride=8, stride_axis=0), axis=0, keepdims=True)

    far = 2 * ((2 * g) // groups) - 1

    def moments_to(j):
        t = (me + far * j + count) % count
        return pltpu.make_async_remote_copy(
            src_ref=red.at[me], dst_ref=red.at[me], send_sem=a_send.at[0], recv_sem=a_recv.at[0],
            device_id=(t // ga, t % ga), device_id_type=MESH)

    def start_moments(j, carry):
        moments_to(j).start()
        return carry

    lax.fori_loop(1, count, start_moments, 0, unroll=count <= 64)
    drained(held.at[:, :, pl.ds(0, width - rows), :], in_send.at[0])
    for up in range(2):
        @pl.when(z_there[up])
        def _():
            drained(X.at[0, pl.ds(0, 5), pl.ds(0, 3)], z_send.at[up])

        @pl.when(r_there[up])
        def _():
            drained(halo.at[0, pl.ds(0, 3), 0, pl.ds(0, 5), pl.ds(8, tall)], r_send.at[up])

        for side in range(2):
            @pl.when(z_there[up] & r_there[side])
            def _():
                for c, k in exchanges:
                    edge_left(c, k, up, side)
    others = red.at[pl.ds(0, count - 1)]
    drained(others, a_recv.at[0])
    total = jnp.sum(red[...], axis=0)

    loads[2].wait()
    gram = jnp.zeros((SIDE, LANES), jnp.float32)
    moved = jnp.zeros((SIDE, LANES), jnp.float32)
    for e in range(COUNT):
        at = 8 * (e % 8) + e // 8
        value = total[0:1, at:at + 1]
        gram = gram + value * table[e]
        moved = moved + value * table[COUNT + e]
    change, change_t = table[2 * COUNT], table[2 * COUNT + 1]

    def unit(axis, at):
        ids = lax.broadcasted_iota(jnp.int32, (SIDE, LANES), axis)
        return jnp.where(ids == at, 1.0, 0.0).astype(jnp.float32)

    def down(x):
        return jnp.sum(x, axis=0, keepdims=True)

    def across(x):
        return jnp.sum(x, axis=1, keepdims=True)

    def advance(state):
        qc, qr, wc, wr, it, uc, rho = state
        mc = across(change * qr)
        gc = across(moved * qr)
        mr = down(change_t * qc)
        alpha = rho / down(qc * gc)
        it = it + alpha * qc
        wc = wc - alpha * mc
        wr = wr - alpha * mr
        uc = uc - alpha * gc
        rho_new = down(wc * uc)
        return wc, wr, it, uc, rho_new, rho_new / rho

    def inner(_, state):
        wc, wr, it, uc, rho, beta = advance(state)
        return wc + beta * state[0], wr + beta * state[1], wc, wr, it, uc, rho

    wc, wr = unit(0, S + 1), unit(1, S + 1)
    start = across(gram * wr) + jnp.zeros((SIDE, LANES), jnp.float32)
    state = (unit(0, 0), unit(1, 0), wc, wr, jnp.zeros((SIDE, LANES), jnp.float32), start, down(wc * start))
    state = lax.fori_loop(0, S - 1, inner, state)
    _, _, it, _, _, beta = advance(state)
    coef[0] = it
    coef[1] = state[0]
    beta_ref[...] = jnp.zeros((8, LANES), jnp.float32) + beta

    tile = 16 if rows % 16 == 0 else 8

    def combine(o, start, out, height):
        def strip(s, carry):
            i, part = s // (rows // tile), s % (rows // tile)
            at = pl.ds(pl.multiple_of(part * tile, tile), tile)
            total = None
            for v in range(2 * S - 1):
                c, k = (0, v) if v < S else (1, v - S)
                row = v if v < S else v + 1
                f = coef[o, row:row + 1, :]
                f = jnp.concatenate([f] * (depth // LANES), axis=1)
                term = f * X[c, k, start + i, at, :]
                total = term if total is None else total + term
            out[i, at, :] = total
            return carry
        lax.fori_loop(0, height * (rows // tile), strip, 0, unroll=2)

    def combine_dx(q):
        combine(0, planes * q + DEEP - 1 + q % 2, out_dx.at[q], planes + 1)

    def combine_q(q):
        combine(1, planes * q + DEEP, out_q.at[q], planes)

    odd = p % 2

    def outgoing_dx(j):
        q = flipped(p, j, group)
        return pltpu.make_async_remote_copy(
            src_ref=out_dx.at[q], dst_ref=dx.at[pl.ds(q % 2, planes + 1), block_rows(b), :],
            send_sem=o_send.at[0], recv_sem=o_recv.at[j],
            device_id=device(g, q), device_id_type=MESH)

    def outgoing_q(j):
        q = flipped(p, j, group)
        return pltpu.make_async_remote_copy(
            src_ref=out_q.at[q], dst_ref=last.at[:, block_rows(b), :],
            send_sem=q_send.at[0], recv_sem=q_recv.at[0],
            device_id=device(g, q), device_id_type=MESH)

    def source_of(j):
        return flipped(p, j, group) if group & (group - 1) == 0 else (p + group - j) % group

    def dx_from(j):
        at = block_rows(place(source_of(j)))
        return pltpu.make_async_remote_copy(
            src_ref=out_dx.at[p], dst_ref=dx.at[pl.ds(odd, planes + 1), at, :],
            send_sem=o_send.at[0], recv_sem=o_recv.at[j],
            device_id=device(g, source_of(j)), device_id_type=MESH)

    mate = p + 1 - 2 * odd

    def forward_of(block):
        at = block_rows(block)
        return pltpu.make_async_remote_copy(
            src_ref=dx.at[planes - odd * (planes - 1), at, :],
            dst_ref=dx.at[odd * (planes + 1), at, :],
            send_sem=f_send.at[0], recv_sem=f_recv.at[0],
            device_id=device(g, mate), device_id_type=MESH)

    for j in order:
        combine_dx(flipped(p, j, group))
        outgoing_dx(j).start()
    combine_dx(p)
    own = pltpu.make_async_copy(out_dx.at[p], dx.at[pl.ds(odd, planes + 1), block_rows(b), :], own_sem.at[2])
    own.start()
    for j in order:
        combine_q(flipped(p, j, group))
        outgoing_q(j).start()
    combine_q(p)
    own_q = pltpu.make_async_copy(out_q.at[p], last.at[:, block_rows(b), :], own_sem.at[3])
    own_q.start()
    own.wait()
    forward_of(b).start()
    for j in [order[-1]] + order[:-1]:
        dx_from(j).wait_recv()
        forward_of(place(source_of(j))).start()
    own_q.wait()
    drained(dx.at[0], f_recv.at[0])
    drained(others, a_send.at[0])
    drained(out_dx.at[pl.ds(0, group - 1)], o_send.at[0])
    drained(dx.at[0], f_send.at[0])
    loads[3].wait()

    piece = width // PIECES
    for i in range(planes):
        for t in range(PIECES):
            at = pl.ds(t * piece, piece)
            cur = dx[i + 1, at, :]
            none = jnp.zeros((1, depth), jnp.float32)
            low = dx[i + 1, t * piece - 1:t * piece, :] if t else none
            high = dx[i + 1, (t + 1) * piece:(t + 1) * piece + 1, :] if t < PIECES - 1 else none
            total = neighbours(cur, dx[i, at, :] + dx[i + 2, at, :], low, high)
            sol_out[i, at, :] = sol_in[i, at, :] + cur
            res_out[i, at, :] = held[1, i, at, :] - (6.0 * cur - total)
    drained(last.at[:, pl.ds(0, width - rows), :], q_recv.at[0])
    drained(last.at[:, pl.ds(0, width - rows), :], q_send.at[0])


def finish(sol, res, last, beta, sol_out, res_out, dir_out, buf, sem):
    planes, width, depth = sol.shape
    piece = width // PIECES
    factor = jnp.concatenate([beta[0:1, :]] * (depth // LANES), axis=1)
    copies = [pltpu.make_async_copy(source, target, sem.at[i])
              for i, (source, target) in enumerate(((sol, sol_out), (res, res_out)))]
    for copy in copies:
        copy.start()
    for i in range(planes):
        for s in range(PIECES):
            at = pl.ds(s * piece, piece)
            buf[i, at, :] = res[i, at, :] + factor * last[i, at, :]
        copies.append(pltpu.make_async_copy(buf.at[i], dir_out.at[i], sem.at[2 + i]))
        copies[-1].start()
    for copy in copies:
        copy.wait()


def on_device(gz_count, ga, sol, res, direction):
    planes, width, depth = sol.shape
    group, groups = 2 * ga, gz_count // 2
    tall, rows = planes * group, width // group
    table = jnp.asarray(np.concatenate(gram_tables()))
    vmem = pl.BlockSpec(memory_space=pltpu.VMEM)
    dma = pltpu.SemaphoreType.DMA
    anywhere = pl.BlockSpec(memory_space=pltpu.HBM)
    f32 = jnp.float32
    outs = pl.pallas_call(
        functools.partial(kernel, gz_count, ga),
        out_shape=[pltpu.VMEM(sol.shape, f32)] * 3 + [pltpu.VMEM((8, LANES), f32)],
        in_specs=[anywhere] * 4,
        out_specs=[vmem] * 4,
        scratch_shapes=[
            pltpu.VMEM((2, S + 1, tall + 2 * DEEP, rows, depth), f32),
            pltpu.VMEM((2, S, 2, DEEP + 1, tall + 16, depth), f32),
            pltpu.VMEM((2, 2, 2, DEEP, tall, depth), f32),
            pltpu.VMEM((2, 2, FIRST[1] - 1, 4, depth), f32),
            pltpu.VMEM((2, 2, FIRST[1] - 1, 4, depth), f32),
            pltpu.VMEM((2, 2, FIRST[0] - 2, 4, depth), f32),
            pltpu.VMEM((2, 2, FIRST[0] - 2, 4, depth), f32),
            pltpu.VMEM((2, 2, 2, 1, 1, depth), f32),
            pltpu.VMEM((2, 2, 2, 1, 1, depth), f32),
            pltpu.VMEM((COUNT, 8, LANES), f32),
            pltpu.VMEM((gz_count * ga, 1, LANES), f32),
            pltpu.VMEM((2, SIDE, LANES), f32),
            pltpu.VMEM((planes + 2, width, depth), f32),
            pltpu.VMEM((group, planes + 1, rows, depth), f32),
            pltpu.VMEM((group, planes, rows, depth), f32),
            pltpu.VMEM((2, planes, width, depth), f32),
            pltpu.VMEM(sol.shape, f32),
            pltpu.VMEM((2 * COUNT + 2, SIDE, LANES), f32),
            dma((1,)), dma((2,)), dma((4,)),
            dma((2,)), dma((2, 2, 2)), dma((2,)), dma((2, 2, 2)),
            dma((2, 2, 2, 2)), dma((2, 2, 2, 2)),
            dma((1,)), dma((1,)),
            dma((1,)), dma((group,)), dma((1,)), dma((1,)), dma((1,)), dma((1,)),
            dma((4,)),
        ],
        compiler_params=pltpu.CompilerParams(collective_id=0, has_side_effects=True, vmem_limit_bytes=VMEM_LIMIT),
    )(*(pltpu.with_memory_space_constraint(x, pltpu.HBM) for x in (res, direction, table, sol)))
    shape = jax.ShapeDtypeStruct(sol.shape, f32)
    return pl.pallas_call(
        finish,
        out_shape=[shape] * 3,
        in_specs=[vmem] * 4,
        out_specs=[anywhere] * 3,
        scratch_shapes=[pltpu.VMEM(sol.shape, f32), dma((2 + planes,))],
        compiler_params=pltpu.CompilerParams(vmem_limit_bytes=8 * 2 ** 20),
    )(*outs)


def solution(mesh):
    spec = P(("gz", "ga"), None, None)
    return jax.shard_map(
        functools.partial(on_device, mesh.shape["gz"], mesh.shape["ga"]),
        mesh=mesh, in_specs=(spec, spec, spec), out_specs=(spec, spec, spec), check_vma=False,
    )
```

```python
import functools

import jax
import jax.numpy as jnp
import numpy as np
from jax import lax
from jax.experimental import pallas as pl
from jax.experimental.pallas import tpu as pltpu
from jax.sharding import PartitionSpec as P

S = 8
MESH = pl.DeviceIdType.MESH
first_scale = -1.0 / 6.0
next_scale = -1.0 / 3.0
SIDE = 24
LANES = 128
FIRST = (S - 2, S - 3)
DEEP = max(FIRST)
UNROLL = 16
PIECES = 4
VMEM_LIMIT = 44 * 2 ** 20


def change_matrix(steps):
    count = 2 * steps + 1
    table = np.zeros((count, count), np.float64)
    for offset, length in ((0, steps + 1), (steps + 1, steps)):
        for power in range(length - 1):
            column = offset + power
            table[column, column] = 6.0
            if power == 0:
                table[column + 1, column] = 6.0
            else:
                table[column + 1, column] = 3.0
                table[column - 1, column] = 3.0
    return table


def dd(power, odd):
    return 2 * power + odd


def rr(power, odd):
    return 2 * S + 1 + 2 * power + odd


def dr(power, odd):
    return 4 * S + 2 * power + odd


COUNT = 6 * S


def gram_tables():
    def moment(kind, order):
        half, odd = order // 2, order % 2
        row = np.zeros(COUNT)
        row[kind(half, odd)] += 2.0
        row[kind(0, odd)] -= 1.0
        return row

    size = 2 * S + 1
    table = np.zeros((COUNT, size, size))
    for i in range(size):
        for j in range(size):
            a, b = (i if i <= S else i - S - 1), (j if j <= S else j - S - 1)
            kind = dd if (i <= S and j <= S) else rr if (i > S and j > S) else dr
            table[:, i, j] = 0.5 * (moment(kind, a + b) + moment(kind, abs(a - b)))
    moved = table @ change_matrix(S)

    def padded(t):
        out = np.zeros((t.shape[0], SIDE, LANES), np.float32)
        out[:, :size, :size] = t
        return out

    change = np.stack([change_matrix(S), change_matrix(S).T])
    return padded(table), padded(moved), padded(change)


def flipped(p, bits, group):
    if group & (group - 1):
        return (p + bits) % group
    out, step = p, 1
    while step < group:
        if bits & step:
            out = out + step * (1 - 2 * ((p // step) % 2))
        step *= 2
    return out


def send_order(group):
    if group & (group - 1):
        return list(range(1, group))
    first = [j for j in range(2, group) if (j // 2) & (j // 2 - 1) == 0]
    first = first[::2] + first[1::2]
    return first + [j for j in range(2, group) if j not in first] + [1]


def neighbours(cur, total, low, high):
    height = cur.shape[0]
    total = total + jnp.concatenate([low, cur[:height - 1]], axis=0)
    total = total + jnp.concatenate([cur[1:], high], axis=0)
    return across_columns(cur, total)


def across_columns(cur, total):
    none = jnp.zeros((cur.shape[0], 1), jnp.float32)
    total = total + jnp.concatenate([none, cur[:, :cur.shape[1] - 1]], axis=1)
    return total + jnp.concatenate([cur[:, 1:], none], axis=1)


def kernel(gz_count, ga, res_ref, dir_ref, table_hbm, sol_ref,
           sol_out, res_out, last, beta_ref,
           X, halo, stage, edge, edge_in, edge_0, edge_0_in, edge_1, edge_1_in, accs, red, coef, dx, out_dx, out_q, held, sol_in, table,
           in_send, in_recv, own_sem, z_send, z_recv, r_send, r_recv, e_send, e_recv,
           a_send, a_recv, o_send, o_recv, q_send, q_recv, f_send, f_recv, load_sem):
    group = 2 * ga
    groups = gz_count // 2
    count = gz_count * ga
    planes, width, depth = res_ref.shape
    tall = planes * group
    rows = width // group
    iz, ia = lax.axis_index("gz"), lax.axis_index("ga")
    me = iz * ga + ia
    g = iz // 2
    p = (iz % 2) * ga + ia
    order = send_order(group)

    def place(position):
        upper = position // ga
        return upper * (3 * ga - 1 - position) + (1 - upper) * position

    b = place(p)

    def device(which, position):
        return (which * 2 + position // ga, position % ga)

    def block_rows(block):
        return pl.ds(pl.multiple_of(block * rows, rows), rows)

    loads = [pltpu.make_async_copy(source, target, load_sem.at[i]) for i, (source, target) in enumerate((
        (dir_ref, held.at[0]), (res_ref, held.at[1]), (table_hbm, table), (sol_ref, sol_in)))]
    for load in loads:
        load.start()

    below, above = g > 0, g < groups - 1
    before, after = b > 0, b < group - 1
    z_there, r_there = (below, above), (before, after)

    barrier = pltpu.get_barrier_semaphore()

    def greet(target):
        pl.semaphore_signal(barrier, inc=1, device_id=target, device_id_type=MESH)

    if groups - 1 <= 3:
        for j in range(1, group):
            greet(device(g, flipped(p, j, group)))
        for up in range(2):
            @pl.when(z_there[up])
            def _():
                greet(device(g + 2 * up - 1, p))
            for side in range(2):
                @pl.when(z_there[up] & r_there[side])
                def _():
                    greet(device(g + 2 * up - 1, place(b + 2 * side - 1)))
        below_1, above_1 = jnp.minimum(g, 1), jnp.minimum(groups - 1 - g, 1)
        before_1, after_1 = jnp.minimum(b, 1), jnp.minimum(group - 1 - b, 1)
        pl.semaphore_wait(barrier, group - 1 + (below_1 + above_1) * (1 + before_1 + after_1))
    else:
        def greet_all(j, carry):
            t = (me + j) % count
            greet((t // ga, t % ga))
            return carry
        lax.fori_loop(1, count, greet_all, 0)
        pl.semaphore_wait(barrier, count - 1)

    def incoming(c, j):
        q = flipped(p, j, group)
        return pltpu.make_async_remote_copy(
            src_ref=held.at[c, :, block_rows(place(q)), :],
            dst_ref=X.at[c, 0, pl.ds(DEEP + planes * p, planes)],
            send_sem=in_send.at[0], recv_sem=in_recv.at[c],
            device_id=device(g, q), device_id_type=MESH)

    def own_in(c):
        return pltpu.make_async_copy(
            held.at[c, :, block_rows(b), :],
            X.at[c, 0, pl.ds(DEEP + planes * p, planes)], own_sem.at[c])

    loads[0].wait()
    for j in order:
        incoming(0, j).start()
    own_in(0).start()
    loads[1].wait()
    for j in order:
        incoming(1, j).start()
    own_in(1).start()

    def deep(c, k):
        return 2 if k else FIRST[c]

    def spread(c, k):
        return 1 if k else 4 if deep(c, k) < 6 else 8

    def drained(ref, sem):
        pltpu.make_async_copy(ref, ref, sem).wait()

    exchanges = [(c, k) for c in range(2) for k in (0, FIRST[c])]

    def parts(c, k):
        return range(2 if spread(c, k) == 8 else 1)

    def edges_of(c, k, incoming_side, up, side, part=0):
        if k:
            return (edge_1_in if incoming_side else edge_1).at[c, up, side]
        if spread(c, k) == 4:
            return (edge_in if incoming_side else edge).at[up, side, pl.ds(0, deep(c, k) - 1)]
        if part:
            return (edge_0_in if incoming_side else edge_0).at[up, side]
        if incoming_side:
            return halo.at[c, k, side, pl.ds(1, 1), pl.ds(up * (tall + 8), 8)]
        return stage.at[c, 0, side, pl.ds(0, 1), pl.ds(up * (tall - 8), 8)]

    for c, k in exchanges:
        d = deep(c, k)
        for missing, at in ((g == 0, DEEP - d), (g == groups - 1, tall + DEEP)):
            @pl.when(missing)
            def _():
                X[c, k, at:at + d] = jnp.zeros((d, rows, depth), jnp.float32)
        for side, missing in ((0, b == 0), (1, b == group - 1)):
            @pl.when(missing)
            def _():
                halo[c, k, side, 1:d + 1] = jnp.zeros((d, tall + 16, depth), jnp.float32)
        for up in range(2):
            for side in range(2):
                @pl.when(jnp.logical_not(z_there[up] & r_there[side]))
                def _():
                    for part in parts(c, k):
                        ref = edges_of(c, k, True, up, side, part)
                        ref[...] = jnp.zeros(ref.shape, jnp.float32)

    def z_copy(c, k, up):
        d = deep(c, k)
        source = DEEP + tall - d if up else DEEP
        target = DEEP - d if up else tall + DEEP
        return pltpu.make_async_remote_copy(
            src_ref=X.at[c, k, pl.ds(source, d)],
            dst_ref=X.at[c, k, pl.ds(target, d)],
            send_sem=z_send.at[up], recv_sem=z_recv.at[c, min(k, 1), up],
            device_id=device(g + 2 * up - 1, p), device_id_type=MESH)

    def r_copy(c, k, up):
        d = deep(c, k)
        return pltpu.make_async_remote_copy(
            src_ref=stage.at[c, min(k, 1), up, pl.ds(0, d)],
            dst_ref=halo.at[c, k, 1 - up, pl.ds(1, d), pl.ds(8, tall)],
            send_sem=r_send.at[up], recv_sem=r_recv.at[c, min(k, 1), up],
            device_id=device(g, place(b + 2 * up - 1)), device_id_type=MESH)

    def e_copy(c, k, up, side, part=0):
        h = min(k, 1)
        return pltpu.make_async_remote_copy(
            src_ref=edges_of(c, k, False, up, side, part),
            dst_ref=edges_of(c, k, True, 1 - up, 1 - side, part),
            send_sem=e_send.at[c, h, up, side], recv_sem=e_recv.at[c, h, 1 - up, 1 - side],
            device_id=device(g + 2 * up - 1, place(b + 2 * side - 1)), device_id_type=MESH)

    def e_arrival(c, k, up, side):
        h = min(k, 1)
        return pltpu.make_async_remote_copy(
            src_ref=edges_of(c, k, False, up, side),
            dst_ref=edges_of(c, k, True, up, side),
            send_sem=e_send.at[c, h, up, side], recv_sem=e_recv.at[c, h, up, side],
            device_id=device(g + 2 * up - 1, place(b + 2 * side - 1)), device_id_type=MESH)

    def whole_edge(c, k):
        return held.at[0, 0, pl.ds(0, 8 + 4 * (deep(c, k) - 2))]

    def edge_arrived(c, k, up, side):
        if spread(c, k) == 8:
            drained(whole_edge(c, k), e_recv.at[c, min(k, 1), up, side])
        else:
            e_arrival(c, k, up, side).wait_recv()

    def edge_left(c, k, up, side):
        if spread(c, k) == 8:
            drained(whole_edge(c, k), e_send.at[c, min(k, 1), up, side])
        else:
            e_copy(c, k, up, side).wait_send()

    def send_z(c, k):
        for up in range(2):
            @pl.when(z_there[up])
            def _():
                z_copy(c, k, up).start()

    def send_edges(c, k):
        n = spread(c, k)
        if n < 8:
            for up in range(2):
                for side in range(2):
                    ref = edges_of(c, k, False, up, side)
                    for i in range(deep(c, k) - 1):
                        if n == 1:
                            row = (rows - 1) * side
                            ref[i] = X[c, k, DEEP + (tall - 1) * up, row:row + 1, :]
                        else:
                            ref[i] = stage[c, 0, side, i, up * (tall - n):up * (tall - n) + n, :]
        else:
            for up in range(2):
                for side in range(2):
                    for i in range(1, deep(c, k) - 1):
                        edge_0[up, side, i - 1] = stage[c, 0, side, i, up * (tall - 4):up * (tall - 4) + 4, :]
        for up in range(2):
            for side in range(2):
                @pl.when(z_there[up] & r_there[side])
                def _():
                    for part in parts(c, k):
                        e_copy(c, k, up, side, part).start()

    def send_rows(c, k):
        for side in range(2):
            @pl.when(r_there[side])
            def _():
                r_copy(c, k, side).start()

    def receive_rows(c, k):
        for side in range(2):
            @pl.when(r_there[side])
            def _():
                r_copy(c, k, 1 - side).wait_recv()

    def receive_planes(c, k):
        for up in range(2):
            for side in range(2):
                @pl.when(z_there[up] & r_there[side])
                def _():
                    edge_arrived(c, k, up, side)

            @pl.when(z_there[up])
            def _():
                z_copy(c, k, 1 - up).wait_recv()

    def folded(x):
        total = x[0:8]
        for i in range(8, rows, 8):
            total = total + x[i:i + 8]
        out = total[:, 0:LANES]
        for i in range(LANES, depth, LANES):
            out = out + total[:, i:i + LANES]
        return out

    z_scale = [jnp.minimum(g, 1).astype(jnp.float32), jnp.minimum(groups - 1 - g, 1).astype(jnp.float32)]
    r_scale = [jnp.minimum(b, 1).astype(jnp.float32), jnp.minimum(group - 1 - b, 1).astype(jnp.float32)]

    plane_ids = lax.broadcasted_iota(jnp.int32, (tall + 16, depth), 0)
    inside = (jnp.where(plane_ids < 8, z_scale[0], 1.0) * jnp.where(plane_ids >= tall + 8, z_scale[1], 1.0))

    def settle(c, k):
        n = spread(c, k)
        if n < 8:
            for up in range(2):
                at = tall + 8 if up else 8 - n
                for side in range(2):
                    ref = edges_of(c, k, True, up, side)
                    for i in range(deep(c, k) - 1):
                        halo[c, k, side, i + 1, at:at + n, :] = ref[i]
        else:
            for up in range(2):
                at = tall + 8 if up else 4
                for side in range(2):
                    for i in range(1, deep(c, k) - 1):
                        halo[c, k, side, i + 1, at:at + 4, :] = edge_0_in[up, side, i - 1]
        for e in range(1, deep(c, k)):
            for up in range(2):
                at = tall - 1 + e if up else -e
                put_row(c, k, at, X[c, k, DEEP + at])

    def put_row(c, k, z, new):
        at = pl.ds(8 + z, 1)
        halo[c, k, 0, 0, at, :] = new[0:1]
        halo[c, k, 1, 0, at, :] = new[rows - 1:rows]

    def extend_rows(c, k, reach):
        scale = first_scale if k == 1 else next_scale

        def extend_row(i, carry):
            for side in range(2):
                cur = halo[c, k - 1, side, i]
                total = halo[c, k - 1, side, i - 1] + halo[c, k - 1, side, i + 1]
                total = total + pltpu.roll(cur, 1, 0) + pltpu.roll(cur, tall + 15, 0)
                total = across_columns(cur, total)
                new = total * (inside * (r_scale[side] * scale))
                if k > 1:
                    new = new - halo[c, k - 2, side, i]
                halo[c, k, side, i] = new
            return carry

        lax.fori_loop(1, reach + 1, extend_row, 0, unroll=True)

    def extend_planes(c, k, reach):
        scale = first_scale if k == 1 else next_scale

        def extend_plane(e, carry):
            for up in range(2):
                z = tall - 1 + e if up else -e
                at = DEEP + z
                cur = X[c, k - 1, at]
                total = X[c, k - 1, at - 1] + X[c, k - 1, at + 1]
                low = halo[c, k - 1, 0, 1, pl.ds(8 + z, 1), :]
                high = halo[c, k - 1, 1, 1, pl.ds(8 + z, 1), :]
                total = neighbours(cur, total, low, high)
                new = total * (z_scale[up] * scale)
                if k > 1:
                    new = new - X[c, k - 2, at]
                X[c, k, at] = new
                if reach > 1:
                    put_row(c, k, z, new)
            return carry

        lax.fori_loop(1, reach + 1, extend_plane, 0, unroll=True)

    def names_of(c, k):
        if c == 0:
            names = [(dd(k, 0), "new", "new"), (dd(k - 1, 1), "new", "cur")]
            if k == 1:
                names.append((dd(0, 0), "cur", "cur"))
        else:
            names = [(rr(k, 0), "new", "new"), (rr(k - 1, 1), "new", "cur"),
                     (dr(k, 0), "new", "other"), (dr(k - 1, 1), "cur", "other")]
            if k == S - 1:
                names.append((dr(k, 1), "new", "ahead"))
            if k == 1:
                names += [(rr(0, 0), "cur", "cur"), (dr(0, 0), "cur", "start")]
        return names

    def sent(c, k):
        return k == FIRST[c]

    def plane(c, k, z, sums, reach):
        at = z + DEEP
        cur = X[c, k - 1, at]
        total = X[c, k - 1, at - 1] + X[c, k - 1, at + 1]
        low = halo[c, k - 1, 0, 1, pl.ds(8 + z, 1), :]
        high = halo[c, k - 1, 1, 1, pl.ds(8 + z, 1), :]
        total = neighbours(cur, total, low, high)
        if k == 1:
            new = total * first_scale
        else:
            new = total * next_scale - X[c, k - 2, at]
        X[c, k, at] = new
        if sent(c, k):
            put_rows(c, k, z, new)
        elif reach > 1:
            put_row(c, k, z, new)
        return products(c, k, z, sums, new, cur) if sums else sums

    def products(c, k, z, sums, new, cur):
        names = names_of(c, k)
        at = z + DEEP
        have = {"new": new, "cur": cur}
        if any("other" in n for n in names):
            have["other"] = X[0, k, at]
        if any("ahead" in n for n in names):
            have["ahead"] = X[0, k + 1, at]
        if any("start" in n for n in names):
            have["start"] = X[0, 0, at]
        return tuple(s + folded(have[l] * have[r]) for s, (_, l, r) in zip(sums, names))

    def all_products(c, k):
        def body(z, sums):
            return products(c, k, z, sums, X[c, k, z + DEEP], X[c, k - 1, z + DEEP])
        return lax.fori_loop(0, tall, body, zero_sums(c, k), unroll=4)

    def put_rows(c, k, z, new):
        put_row(c, k, z, new)
        at = pl.ds(z, 1)
        for i in range(deep(c, k)):
            stage[c, min(k, 1), 0, i, at, :] = new[i:i + 1]
            stage[c, min(k, 1), 1, i, at, :] = new[rows - 1 - i:rows - i]

    def zero_sums(c, k):
        return tuple(jnp.zeros((8, LANES), jnp.float32) for _ in names_of(c, k))

    def keep(c, k, sums):
        for s, (slot, _, _) in zip(sums, names_of(c, k)):
            accs[slot] = s

    def ends(c, k, width_of, sums, reach):
        def body(i, sums):
            return plane(c, k, i + (i // width_of) * (tall - 2 * width_of), sums, reach)
        return lax.fori_loop(0, 2 * width_of, body, sums, unroll=True)

    def middle(c, k, width_of, sums, reach):
        length = tall - 2 * width_of
        unroll = max(u for u in range(1, UNROLL + 1) if length % u == 0)
        return lax.fori_loop(width_of, tall - width_of, lambda z, s: plane(c, k, z, s, reach), sums, unroll=unroll)

    def chain_round(c, k):
        d = deep(c, k)
        outer = c == 1 and k == 0 and 2 * (d + 1) < tall
        receive_rows(c, k)
        inner = middle(c, k + 1, 1, () if outer else zero_sums(c, k + 1), d - 1)
        if outer:
            for m in range(2, d + 1):
                extend_rows(c, k + m - 1, d - m + 1)
                middle(c, k + m, m, (), d - m)
        receive_planes(c, k)
        settle(c, k)
        sums = []
        for m in range(1, d + 1):
            n, reach = k + m, d - m
            if reach:
                extend_rows(c, n, reach)
                extend_planes(c, n, reach)
            if m == 1:
                sums.append(ends(c, n, 1, inner, reach))
            elif outer:
                ends(c, n, min(m, 2 + reach), (), reach)
            else:
                sums.append(middle(c, n, 0, zero_sums(c, n), reach))
        if sent(c, k + d):
            send_z(c, k + d)
            if outer:
                send_edges(c, k + d)
        if outer:
            for m in range(2, d + 1):
                n, reach = k + m, d - m
                for z in range(2 + reach, m):
                    plane(c, n, z, (), reach)
                    plane(c, n, tall - 1 - z, (), reach)
        if sent(c, k + d):
            send_rows(c, k + d)
            if not outer:
                send_edges(c, k + d)
        for m in range(1, d + 1):
            keep(c, k + m, all_products(c, k + m) if outer else sums[m - 1])

    def arrive(c):
        own_in(c).wait()
        others = held.at[c, :, pl.ds(0, width - rows), :]
        pltpu.make_async_copy(others, others, in_recv.at[c]).wait()
        send_z(c, 0)

        def copy_rows(z, carry):
            put_rows(c, 0, z, X[c, 0, z + DEEP])
            return carry
        lax.fori_loop(0, tall, copy_rows, 0, unroll=4)
        send_edges(c, 0)
        send_rows(c, 0)

    arrive(0)
    arrive(1)
    for h in range(2):
        for c in range(2):
            chain_round(c, h * FIRST[c])

    lanes = lax.broadcasted_iota(jnp.int32, (8, LANES), 1)
    packed = jnp.zeros((8, LANES), jnp.float32)
    for t in range(COUNT // 8):
        part = jnp.sum(jnp.sum(accs[8 * t:8 * t + 8], axis=1), axis=1, keepdims=True)
        packed = packed + jnp.where(lanes == t, part, 0.0)
    red[me] = jnp.sum(pltpu.roll(packed, 0, 1, stride=8, stride_axis=0), axis=0, keepdims=True)

    far = 2 * ((2 * g) // groups) - 1

    def moments_to(j):
        t = (me + far * j + count) % count
        return pltpu.make_async_remote_copy(
            src_ref=red.at[me], dst_ref=red.at[me], send_sem=a_send.at[0], recv_sem=a_recv.at[0],
            device_id=(t // ga, t % ga), device_id_type=MESH)

    def start_moments(j, carry):
        moments_to(j).start()
        return carry

    lax.fori_loop(1, count, start_moments, 0, unroll=count <= 64)
    drained(held.at[:, :, pl.ds(0, width - rows), :], in_send.at[0])
    for up in range(2):
        @pl.when(z_there[up])
        def _():
            drained(X.at[0, pl.ds(0, 5), pl.ds(0, 3)], z_send.at[up])

        @pl.when(r_there[up])
        def _():
            drained(halo.at[0, pl.ds(0, 3), 0, pl.ds(0, 5), pl.ds(8, tall)], r_send.at[up])

        for side in range(2):
            @pl.when(z_there[up] & r_there[side])
            def _():
                for c, k in exchanges:
                    edge_left(c, k, up, side)
    others = red.at[pl.ds(0, count - 1)]
    drained(others, a_recv.at[0])
    total = jnp.sum(red[...], axis=0)

    loads[2].wait()
    gram = jnp.zeros((SIDE, LANES), jnp.float32)
    moved = jnp.zeros((SIDE, LANES), jnp.float32)
    for e in range(COUNT):
        at = 8 * (e % 8) + e // 8
        value = total[0:1, at:at + 1]
        gram = gram + value * table[e]
        moved = moved + value * table[COUNT + e]
    change, change_t = table[2 * COUNT], table[2 * COUNT + 1]

    def unit(axis, at):
        ids = lax.broadcasted_iota(jnp.int32, (SIDE, LANES), axis)
        return jnp.where(ids == at, 1.0, 0.0).astype(jnp.float32)

    def down(x):
        return jnp.sum(x, axis=0, keepdims=True)

    def across(x):
        return jnp.sum(x, axis=1, keepdims=True)

    def advance(state):
        qc, qr, wc, wr, it, uc, rho = state
        mc = across(change * qr)
        gc = across(moved * qr)
        mr = down(change_t * qc)
        alpha = rho / down(qc * gc)
        it = it + alpha * qc
        wc = wc - alpha * mc
        wr = wr - alpha * mr
        uc = uc - alpha * gc
        rho_new = down(wc * uc)
        return wc, wr, it, uc, rho_new, rho_new / rho

    def inner(_, state):
        wc, wr, it, uc, rho, beta = advance(state)
        return wc + beta * state[0], wr + beta * state[1], wc, wr, it, uc, rho

    wc, wr = unit(0, S + 1), unit(1, S + 1)
    start = across(gram * wr) + jnp.zeros((SIDE, LANES), jnp.float32)
    state = (unit(0, 0), unit(1, 0), wc, wr, jnp.zeros((SIDE, LANES), jnp.float32), start, down(wc * start))
    state = lax.fori_loop(0, S - 1, inner, state)
    _, _, it, _, _, beta = advance(state)
    coef[0] = it
    coef[1] = state[0]
    beta_ref[...] = jnp.zeros((8, LANES), jnp.float32) + beta

    tile = 16 if rows % 16 == 0 else 8

    def combine(o, start, out, height):
        def strip(s, carry):
            i, part = s // (rows // tile), s % (rows // tile)
            at = pl.ds(pl.multiple_of(part * tile, tile), tile)
            total = None
            for v in range(2 * S - 1):
                c, k = (0, v) if v < S else (1, v - S)
                row = v if v < S else v + 1
                f = coef[o, row:row + 1, :]
                f = jnp.concatenate([f] * (depth // LANES), axis=1)
                term = f * X[c, k, start + i, at, :]
                total = term if total is None else total + term
            out[i, at, :] = total
            return carry
        lax.fori_loop(0, height * (rows // tile), strip, 0, unroll=2)

    def combine_dx(q):
        combine(0, planes * q + DEEP - 1 + q % 2, out_dx.at[q], planes + 1)

    def combine_q(q):
        combine(1, planes * q + DEEP, out_q.at[q], planes)

    odd = p % 2

    def outgoing_dx(j):
        q = flipped(p, j, group)
        return pltpu.make_async_remote_copy(
            src_ref=out_dx.at[q], dst_ref=dx.at[pl.ds(q % 2, planes + 1), block_rows(b), :],
            send_sem=o_send.at[0], recv_sem=o_recv.at[j],
            device_id=device(g, q), device_id_type=MESH)

    def outgoing_q(j):
        q = flipped(p, j, group)
        return pltpu.make_async_remote_copy(
            src_ref=out_q.at[q], dst_ref=last.at[:, block_rows(b), :],
            send_sem=q_send.at[0], recv_sem=q_recv.at[0],
            device_id=device(g, q), device_id_type=MESH)

    def source_of(j):
        return flipped(p, j, group) if group & (group - 1) == 0 else (p + group - j) % group

    def dx_from(j):
        at = block_rows(place(source_of(j)))
        return pltpu.make_async_remote_copy(
            src_ref=out_dx.at[p], dst_ref=dx.at[pl.ds(odd, planes + 1), at, :],
            send_sem=o_send.at[0], recv_sem=o_recv.at[j],
            device_id=device(g, source_of(j)), device_id_type=MESH)

    mate = p + 1 - 2 * odd

    def forward_of(block):
        at = block_rows(block)
        return pltpu.make_async_remote_copy(
            src_ref=dx.at[planes - odd * (planes - 1), at, :],
            dst_ref=dx.at[odd * (planes + 1), at, :],
            send_sem=f_send.at[0], recv_sem=f_recv.at[0],
            device_id=device(g, mate), device_id_type=MESH)

    for j in order:
        combine_dx(flipped(p, j, group))
        outgoing_dx(j).start()
    combine_dx(p)
    own = pltpu.make_async_copy(out_dx.at[p], dx.at[pl.ds(odd, planes + 1), block_rows(b), :], own_sem.at[2])
    own.start()
    for j in order:
        combine_q(flipped(p, j, group))
        outgoing_q(j).start()
    combine_q(p)
    own_q = pltpu.make_async_copy(out_q.at[p], last.at[:, block_rows(b), :], own_sem.at[3])
    own_q.start()
    own.wait()
    forward_of(b).start()
    for j in [order[-1]] + order[:-1]:
        dx_from(j).wait_recv()
        forward_of(place(source_of(j))).start()
    own_q.wait()
    drained(dx.at[0], f_recv.at[0])
    drained(others, a_send.at[0])
    drained(out_dx.at[pl.ds(0, group - 1)], o_send.at[0])
    drained(dx.at[0], f_send.at[0])
    loads[3].wait()

    piece = width // PIECES
    for i in range(planes):
        for t in range(PIECES):
            at = pl.ds(t * piece, piece)
            cur = dx[i + 1, at, :]
            none = jnp.zeros((1, depth), jnp.float32)
            low = dx[i + 1, t * piece - 1:t * piece, :] if t else none
            high = dx[i + 1, (t + 1) * piece:(t + 1) * piece + 1, :] if t < PIECES - 1 else none
            total = neighbours(cur, dx[i, at, :] + dx[i + 2, at, :], low, high)
            sol_out[i, at, :] = sol_in[i, at, :] + cur
            res_out[i, at, :] = held[1, i, at, :] - (6.0 * cur - total)
    drained(last.at[:, pl.ds(0, width - rows), :], q_recv.at[0])
    drained(last.at[:, pl.ds(0, width - rows), :], q_send.at[0])


def finish(sol, res, last, beta, sol_out, res_out, dir_out, buf, sem):
    planes, width, depth = sol.shape
    piece = width // PIECES
    factor = jnp.concatenate([beta[0:1, :]] * (depth // LANES), axis=1)
    copies = [pltpu.make_async_copy(source, target, sem.at[i])
              for i, (source, target) in enumerate(((sol, sol_out), (res, res_out)))]
    for copy in copies:
        copy.start()
    for i in range(planes):
        for s in range(PIECES):
            at = pl.ds(s * piece, piece)
            buf[i, at, :] = res[i, at, :] + factor * last[i, at, :]
        copies.append(pltpu.make_async_copy(buf.at[i], dir_out.at[i], sem.at[2 + i]))
        copies[-1].start()
    for copy in copies:
        copy.wait()


def on_device(gz_count, ga, sol, res, direction):
    planes, width, depth = sol.shape
    group, groups = 2 * ga, gz_count // 2
    tall, rows = planes * group, width // group
    table = jnp.asarray(np.concatenate(gram_tables()))
    vmem = pl.BlockSpec(memory_space=pltpu.VMEM)
    dma = pltpu.SemaphoreType.DMA
    anywhere = pl.BlockSpec(memory_space=pltpu.HBM)
    f32 = jnp.float32
    outs = pl.pallas_call(
        functools.partial(kernel, gz_count, ga),
        out_shape=[pltpu.VMEM(sol.shape, f32)] * 3 + [pltpu.VMEM((8, LANES), f32)],
        in_specs=[anywhere] * 4,
        out_specs=[vmem] * 4,
        scratch_shapes=[
            pltpu.VMEM((2, S + 1, tall + 2 * DEEP, rows, depth), f32),
            pltpu.VMEM((2, S, 2, DEEP + 1, tall + 16, depth), f32),
            pltpu.VMEM((2, 2, 2, DEEP, tall, depth), f32),
            pltpu.VMEM((2, 2, FIRST[1] - 1, 4, depth), f32),
            pltpu.VMEM((2, 2, FIRST[1] - 1, 4, depth), f32),
            pltpu.VMEM((2, 2, FIRST[0] - 2, 4, depth), f32),
            pltpu.VMEM((2, 2, FIRST[0] - 2, 4, depth), f32),
            pltpu.VMEM((2, 2, 2, 1, 1, depth), f32),
            pltpu.VMEM((2, 2, 2, 1, 1, depth), f32),
            pltpu.VMEM((COUNT, 8, LANES), f32),
            pltpu.VMEM((gz_count * ga, 1, LANES), f32),
            pltpu.VMEM((2, SIDE, LANES), f32),
            pltpu.VMEM((planes + 2, width, depth), f32),
            pltpu.VMEM((group, planes + 1, rows, depth), f32),
            pltpu.VMEM((group, planes, rows, depth), f32),
            pltpu.VMEM((2, planes, width, depth), f32),
            pltpu.VMEM(sol.shape, f32),
            pltpu.VMEM((2 * COUNT + 2, SIDE, LANES), f32),
            dma((1,)), dma((2,)), dma((4,)),
            dma((2,)), dma((2, 2, 2)), dma((2,)), dma((2, 2, 2)),
            dma((2, 2, 2, 2)), dma((2, 2, 2, 2)),
            dma((1,)), dma((1,)),
            dma((1,)), dma((group,)), dma((1,)), dma((1,)), dma((1,)), dma((1,)),
            dma((4,)),
        ],
        compiler_params=pltpu.CompilerParams(collective_id=0, has_side_effects=True, vmem_limit_bytes=VMEM_LIMIT),
    )(*(pltpu.with_memory_space_constraint(x, pltpu.HBM) for x in (res, direction, table, sol)))
    shape = jax.ShapeDtypeStruct(sol.shape, f32)
    return pl.pallas_call(
        finish,
        out_shape=[shape] * 3,
        in_specs=[vmem] * 4,
        out_specs=[anywhere] * 3,
        scratch_shapes=[pltpu.VMEM(sol.shape, f32), dma((2 + planes,))],
        compiler_params=pltpu.CompilerParams(vmem_limit_bytes=8 * 2 ** 20),
    )(*outs)


def solution(mesh):
    spec = P(("gz", "ga"), None, None)
    return jax.shard_map(
        functools.partial(on_device, mesh.shape["gz"], mesh.shape["ga"]),
        mesh=mesh, in_specs=(spec, spec, spec), out_specs=(spec, spec, spec), check_vma=False,
    )
```
